128 devices in a mesh: group: 2 (over z_hi), tensoror: 4 (over x), seq: 16 (over y, z_lo, core).
Axes of the slice: x: 4, y: 4, z: 4 (z_hi: 2, z_lo: 2; z = z_hi * 2 + z_lo), core: 2. Of those that a mesh axis runs over, the one named last changes fastest.
Arguments:
- visual_hidden: bfloat16 [16, 512, 5120], P('group', 'seq', 'tensoror'), may hold values from -6 to 6
- projector_weight: bfloat16 [5120, 5120], P('tensoror'), may hold values from -0.078125 to 0.078125
- text_embeddings: bfloat16 [16, 2048, 5120], P(('group', 'tensoror'), 'seq'), may hold values from -6 to 6
- tile_counts: int32 [16], replicated, may hold values from 1 to 2, 24 in all
- image_start: int32 [16], replicated, may hold values from 0 to 1536
- norm_gain: float32 [5120], replicated, may hold values from 0.5 to 1.5
- query_weight: bfloat16 [5120, 2560], P('tensoror'), may hold values from -3 to 3
- keyvalue_weight: bfloat16 [5120, 1024], P('tensoror'), may hold values from -0.08385255 to 0.08385255
Outputs:
- context: bfloat16 [16, 2048, 2560], P(('group', 'tensoror'), 'seq')
The draws below stay inside these ranges and needn't reach their ends.
Inputs may be any that keep to these rules, and one draw needn't show every extreme that they name: `tile_counts`: the counts of all sequences sum to 24.
All inputs are finite; a program needn't handle non-finite values.
Results may differ from the reference program's by a relative error of at most 0.0061.
Values may be sent and summed in bfloat16 or wider, within the bound.
A program may use at most 128 MiB of HBM per device.

```python
import math
import jax
import jax.numpy as jnp
import numpy as np
from jax import lax

MODEL_WIDTH = 5120
QUERY_HEADS = 20
KEY_VALUE_HEADS = 4
HEAD_SIZE = 128
SEQUENCE_LENGTH = 2048
TILE = 256
MAXT = 2
SEQUENCE_COUNT = 16
MAXV = 512
TILES = 24


def weight_draws(key):
    bound = 6.0 / math.sqrt(MODEL_WIDTH)
    starting_query = jax.random.normal(jax.random.fold_in(key, 101), (MODEL_WIDTH, QUERY_HEADS * HEAD_SIZE), jnp.float32) / math.sqrt(MODEL_WIDTH)
    starting_pair = jax.random.normal(jax.random.fold_in(key, 202), (MODEL_WIDTH, 2 * KEY_VALUE_HEADS * HEAD_SIZE), jnp.float32) / math.sqrt(MODEL_WIDTH)
    return (jnp.clip(starting_query, -bound, bound), jnp.clip(starting_pair, -bound, bound))


def draw_query_weight(key, part):
    starting_query, starting_pair = weight_draws(key)
    return starting_query.astype(jnp.bfloat16)


def draw_keyvalue_weight(key, part):
    starting_query, starting_pair = weight_draws(key)
    return starting_pair.astype(jnp.bfloat16)


def place_ends(array, key, smallest, top_value):
    longest = array.shape.index(max(array.shape))
    spots = []
    for shift in (0, 1):
        where = [jax.random.randint(jax.random.fold_in(key, axis), (), 0, length) for axis, length in enumerate(array.shape)]
        where[longest] = (where[longest] + shift) % array.shape[longest]
        spots.append(tuple(where))
    return array.at[spots[0]].set(smallest).at[spots[1]].set(top_value)


def steps_of(key, extent, shards, smallest, largest):
    factor_of = 1.0
    for axis_at, shards_of in shards:
        heights = jax.random.uniform(jax.random.fold_in(jax.random.fold_in(key, 6), axis_at), (shards_of,), jnp.float32, smallest / len(shards), largest / len(shards))
        factor_of = factor_of * jnp.repeat(jnp.exp(heights), extent[axis_at] // shards_of).reshape((-1,) + (1,) * (len(extent) - 1 - axis_at))
    return factor_of


def length_profile(number_of, total, limit, slope):
    loads = [(1 << 20) // math.isqrt(grade ** slope) + 1 for grade in range(2, number_of + 1)]
    surplus, holding = total - limit - (number_of - 1), [1] * (number_of - 1)
    while surplus > 0:
        free = [i for i in range(number_of - 1) if holding[i] < limit]
        pool, remaining = sum([loads[i] for i in free]), surplus
        for i in free:
            addition = min(limit - holding[i], max(1, remaining * loads[i] // pool), surplus)
            holding[i] = holding[i] + addition
            surplus = surplus - addition
    return np.array([limit] + holding)


def uneven(key, amount, total, limit, skew):
    if amount == 2:
        one = jax.random.randint(key, (), max(1, total - limit), min(limit, total - 1) + 1)
        return jnp.stack([one, total - one])
    sizes = jnp.asarray(length_profile(amount, total, limit, skew), jnp.int32)
    couples = (amount - 1) // 2
    source_of, receiver = sizes[1:1 + 2 * couples:2], sizes[2:2 + 2 * couples:2]
    room = jnp.minimum(source_of - 1, limit - receiver)
    moved = jax.random.randint(jax.random.fold_in(key, 1), (couples,), 0, 1 << 20) % (room + 1)
    sizes = sizes.at[1:1 + 2 * couples:2].set(source_of - moved).at[2:2 + 2 * couples:2].set(receiver + moved)
    return sizes[jax.random.permutation(jax.random.fold_in(key, 2), amount)]


def normal_values(stream_key, extent, scale, most, shards=(), held_as=jnp.bfloat16):
    result = jax.random.normal(stream_key, extent, jnp.float32) * scale
    if len(shards) > 0:
        result = steps_of(stream_key, extent, shards, -0.22, 0.18) * result
    return jnp.clip(result, min=-most, max=most).astype(held_as)


def setup_inputs(seed: int = 0) -> dict:
    arg_keys = jax.random.split(jax.random.key(seed), 9)
    return {
        "visual_hidden": normal_values(arg_keys[0], (SEQUENCE_COUNT, MAXV, MODEL_WIDTH), 1.0, 6.0, ((0, 2), (1, 16), (2, 4))),
        "projector_weight": normal_values(arg_keys[1], (MODEL_WIDTH, MODEL_WIDTH), MODEL_WIDTH ** -0.5, 0.078125, ((0, 4),)),
        "text_embeddings": normal_values(arg_keys[2], (SEQUENCE_COUNT, SEQUENCE_LENGTH, MODEL_WIDTH), 1.0, 6.0, ((0, 8), (1, 16))),
        "tile_counts": uneven(arg_keys[3], SEQUENCE_COUNT, TILES, MAXT, 2).astype(jnp.int32),
        "image_start": place_ends(jax.random.randint(arg_keys[4], (SEQUENCE_COUNT,), 0, SEQUENCE_LENGTH - MAXV + 1), jax.random.fold_in(arg_keys[4], 1), 0, SEQUENCE_LENGTH - MAXV).astype(jnp.int32),
        "norm_gain": jnp.clip(1.0 + 0.1 * jax.random.normal(arg_keys[5], (MODEL_WIDTH,), jnp.float32), 0.5, 1.5),
        "query_weight": draw_query_weight(jax.random.fold_in(arg_keys[8], 71), 0),
        "keyvalue_weight": draw_keyvalue_weight(jax.random.fold_in(arg_keys[8], 71), 0),
    }


epsilon = 1e-06
masked_score = -1e+30

def attend_block(block_queries, first_row, keys, values):
    rows = block_queries.shape[0]
    scale = 1.0 / HEAD_SIZE ** 0.5
    scores = jnp.einsum('qkgd,rkd->kgqr', block_queries.astype(jnp.float32), keys.astype(jnp.float32)) * scale
    query_pos = first_row + jnp.arange(rows, dtype=jnp.int32)
    key_pos = jnp.arange(SEQUENCE_LENGTH, dtype=jnp.int32)
    causal_mask = key_pos[None, :] <= query_pos[:, None]
    scores = jnp.where(causal_mask, scores, masked_score)
    row_max = lax.optimization_barrier(jnp.max(scores, axis=-1, keepdims=True))
    expo = jnp.where(causal_mask, jnp.exp(scores - row_max), 0.0)
    denominator = lax.optimization_barrier(jnp.sum(expo, axis=-1))
    rounded = expo.astype(jnp.bfloat16)
    summed = jnp.einsum('kgqr,rkd->qkgd', rounded.astype(jnp.float32), values.astype(jnp.float32))
    summed = summed / jnp.transpose(denominator, (2, 0, 1))[..., None]
    return summed.astype(jnp.bfloat16).reshape(rows, QUERY_HEADS * HEAD_SIZE)

def reference(visual_hidden, projector_weight, text_embeddings, tile_counts, image_start, norm_gain, query_weight, keyvalue_weight):
    query_groups = QUERY_HEADS // KEY_VALUE_HEADS
    activated = jax.nn.gelu(visual_hidden.astype(jnp.float32), approximate=False).astype(jnp.bfloat16)
    visual = jnp.dot(activated, projector_weight, preferred_element_type=jnp.float32).astype(jnp.bfloat16)
    positions = jnp.arange(SEQUENCE_LENGTH, dtype=jnp.int32)
    slot_index = positions[None, :] - image_start[:, None].astype(jnp.int32)
    inside = (slot_index >= 0) & (slot_index < TILE * tile_counts[:, None].astype(jnp.int32))
    clipped = jnp.clip(slot_index, 0, MAXV - 1).astype(jnp.int32)
    placed = jnp.take_along_axis(visual, clipped[:, :, None], axis=1)
    mixed = jnp.where(inside[:, :, None], placed, text_embeddings)
    widened = mixed.astype(jnp.float32)
    mean_square = lax.optimization_barrier(jnp.mean(widened * widened, axis=-1, keepdims=True))
    normed = (widened * lax.rsqrt(mean_square + epsilon) * norm_gain).astype(jnp.bfloat16)
    flat = normed.reshape(SEQUENCE_COUNT * SEQUENCE_LENGTH, MODEL_WIDTH)
    query_rows = jnp.dot(flat, query_weight, preferred_element_type=jnp.float32).astype(jnp.bfloat16)
    key_value_rows = jnp.dot(flat, keyvalue_weight, preferred_element_type=jnp.float32).astype(jnp.bfloat16)
    query_rows = query_rows.reshape(SEQUENCE_COUNT, SEQUENCE_LENGTH, KEY_VALUE_HEADS, query_groups, HEAD_SIZE)
    key_value_rows = key_value_rows.reshape(SEQUENCE_COUNT, SEQUENCE_LENGTH, 2, KEY_VALUE_HEADS, HEAD_SIZE)
    block_current = min(512, SEQUENCE_LENGTH)

    def one_sequence(operands):
        sequence_query_rows, seq_keyvalues = operands
        keys = seq_keyvalues[:, 0]
        values = seq_keyvalues[:, 1]
        block_split = sequence_query_rows.reshape(SEQUENCE_LENGTH // block_current, block_current, KEY_VALUE_HEADS, query_groups, HEAD_SIZE)
        starts = jnp.arange(SEQUENCE_LENGTH // block_current, dtype=jnp.int32) * block_current
        return lax.map(lambda item: attend_block(item[0], item[1], keys, values), (block_split, starts)).reshape(SEQUENCE_LENGTH, QUERY_HEADS * HEAD_SIZE)
    return lax.map(one_sequence, (query_rows, key_value_rows))
```

```python
import functools
import math

import jax
import jax.numpy as jnp
from jax import lax
from jax.experimental import pallas as pl
from jax.experimental.pallas import tpu as pltpu
from jax.sharding import PartitionSpec as P

QUERY_HEADS = 20
KEY_VALUE_HEADS = 4
HEAD_SIZE = 128
TILE = 256
GROUP_HEADS = QUERY_HEADS // KEY_VALUE_HEADS
MESH = pl.DeviceIdType.MESH

epsilon = 1e-06
masked_score = -1e30
VMEM = 60 * 1024 * 1024


def neighbours():
    count = lax.axis_size("tensoror")
    me = lax.axis_index("tensoror")
    return me, lax.rem(me + 1, count), lax.rem(me + 2, count), lax.rem(me + 3, count)


def greet(peers):
    barrier = pltpu.get_barrier_semaphore()
    for peer in peers:
        pl.semaphore_signal(
            barrier, inc=1, device_id={"tensoror": peer}, device_id_type=MESH
        )
    pl.semaphore_wait(barrier, len(peers))


TO_RIGHT = (False, True, True, False, False, True)


def piece(kind, c, send, recv, send_sem, recv_sem):
    me, right, opposite, left = neighbours()
    return pltpu.make_async_remote_copy(
        src_ref=send.at[kind, c],
        dst_ref=recv.at[kind, c],
        send_sem=send_sem.at[kind, c],
        recv_sem=recv_sem.at[kind, c],
        device_id={"tensoror": right if TO_RIGHT[kind] else left},
        device_id_type=MESH,
    )


def first_pieces(c, part, send, keep, own, copy):
    me, right, opposite, left = neighbours()
    half = send.shape[3]
    sums = part(2, opposite)
    send[0, c] = sums[:, :half].astype(jnp.bfloat16)
    send[1, c] = sums[:, half:].astype(jnp.bfloat16)
    copy(0, c).start()
    copy(1, c).start()
    sums = part(1, right)
    send[2, c] = sums[:, :half].astype(jnp.bfloat16)
    keep[1, c] = sums[:, half:]
    copy(2, c).start()
    sums = part(3, left)
    send[3, c] = sums[:, half:].astype(jnp.bfloat16)
    keep[0, c] = sums[:, :half]
    copy(3, c).start()
    own[c] = part(0, me)


def pass_on(c, send, recv, keep, copy):
    for side in (0, 1):
        copy(side, c).wait_recv()
        send[4 + side, c] = (keep[side, c] + recv[side, c].astype(jnp.float32)).astype(
            jnp.bfloat16
        )
        copy(4 + side, c).start()


def last_sum(c, recv, own, copy):
    for kind in (2, 3, 4, 5):
        copy(kind, c).wait_recv()
    half = recv.shape[3]
    first = own[c, :, :half] + recv[2, c].astype(jnp.float32) + recv[4, c].astype(jnp.float32)
    second = own[c, :, half:] + recv[3, c].astype(jnp.float32) + recv[5, c].astype(jnp.float32)
    return first, second


def each(start, stop, body):
    lax.fori_loop(start, stop, lambda c, _: (body(c), 0)[1], 0)


def all_sent(chunks, copy):
    def wait(c):
        for kind in range(6):
            copy(kind, c).wait_send()

    each(0, chunks, wait)


def piece_scratch(chunks, rows, half):
    return [
        pltpu.VMEM((6, chunks, rows, half), jnp.bfloat16),
        pltpu.VMEM((6, chunks, rows, half), jnp.bfloat16),
        pltpu.VMEM((2, chunks, rows, half), jnp.float32),
        pltpu.VMEM((chunks, rows, 2 * half), jnp.float32),
        pltpu.SemaphoreType.DMA((6, chunks)),
        pltpu.SemaphoreType.DMA((6, chunks)),
    ]


def project_kernel(
    act_ref, w_ref, out_ref, weights, weight_sem, send, recv, keep, own, send_sem, recv_sem
):
    me, right, opposite, left = neighbours()
    chunks, rows, wide = own.shape
    half = wide // 2

    def load(k, dest, c):
        column = pl.multiple_of(dest * (chunks * wide) + c * wide, 128)
        return pltpu.make_async_copy(
            w_ref.at[:, pl.ds(column, wide)], weights.at[k, c], weight_sem.at[k, c]
        )

    for c in range(chunks):
        for k, dest in ((2, opposite), (1, right), (3, left), (0, me)):
            load(k, dest, c).start()
    greet((left, right))

    def copy(kind, c):
        return piece(kind, c, send, recv, send_sem, recv_sem)

    def first(c):
        def part(k, dest):
            load(k, dest, c).wait()
            return jnp.dot(act_ref[...], weights[k, c], preferred_element_type=jnp.float32)

        first_pieces(c, part, send, keep, own, copy)

    def last(c):
        low, high = last_sum(c, recv, own, copy)
        column = pl.multiple_of(c * wide, 128)
        out_ref[:, pl.ds(column, half)] = low.astype(jnp.bfloat16)
        out_ref[:, pl.ds(pl.multiple_of(column + half, 128), half)] = high.astype(jnp.bfloat16)

    each(0, chunks, first)
    each(0, chunks, lambda c: pass_on(c, send, recv, keep, copy))
    each(0, chunks, last)
    all_sent(chunks, copy)


def project(activated, weight):
    rows, depth = activated.shape
    width = weight.shape[1] // lax.axis_size("tensoror")
    wide = 256
    chunks = width // wide
    return pl.pallas_call(
        project_kernel,
        in_specs=[
            pl.BlockSpec(memory_space=pltpu.VMEM),
            pl.BlockSpec(memory_space=pl.ANY),
        ],
        out_specs=pl.BlockSpec(memory_space=pltpu.VMEM),
        out_shape=jax.ShapeDtypeStruct((rows, width), jnp.bfloat16),
        scratch_shapes=[
            pltpu.VMEM((4, chunks, depth, wide), jnp.bfloat16),
            pltpu.SemaphoreType.DMA((4, chunks)),
        ]
        + piece_scratch(chunks, rows, wide // 2),
        compiler_params=pltpu.CompilerParams(
            collective_id=1, has_side_effects=True, vmem_limit_bytes=VMEM
        ),
        cost_estimate=pl.CostEstimate(
            flops=8 * rows * depth * width, bytes_accessed=2 * weight.size, transcendentals=0
        ),
    )(activated, weight)


def heads_kernel(
    x_ref,
    square_ref,
    wkv_ref,
    wq_ref,
    kv_ref,
    q_ref,
    weights,
    squares,
    total,
    scale,
    weight_sem,
    square_send,
    square_recv,
    send,
    recv,
    keep,
    own,
    send_sem,
    recv_sem,
    *,
    width,
):
    me, right, opposite, left = neighbours()
    chunks, rows, wide = own.shape
    half = wide // 2
    extent = square_ref.shape[1]
    local = rows // extent
    kv_chunks = kv_ref.shape[1] // wide
    for c in range(chunks):
        source = wkv_ref if c < kv_chunks else wq_ref
        column = (c if c < kv_chunks else c - kv_chunks) * wide
        pltpu.make_async_copy(
            source.at[:, pl.ds(column, wide)], weights.at[c], weight_sem.at[c]
        ).start()
    greet((right, opposite, left))

    def square_copy(k, peer):
        return pltpu.make_async_remote_copy(
            src_ref=square_ref,
            dst_ref=squares.at[k],
            send_sem=square_send.at[k],
            recv_sem=square_recv.at[k],
            device_id={"tensoror": peer},
            device_id_type=MESH,
        )

    peers = ((1, right), (2, opposite), (3, left))
    for k, peer in peers:
        square_copy(k, peer).start()

    def copy(kind, c):
        return piece(kind, c, send, recv, send_sem, recv_sem)

    def first(c):
        pltpu.make_async_copy(
            wkv_ref.at[:, pl.ds(0, wide)], weights.at[c], weight_sem.at[c]
        ).wait()

        def part(k, dest):
            return jnp.dot(
                x_ref[pl.ds(pl.multiple_of(dest * rows, rows), rows), :],
                weights[c],
                preferred_element_type=jnp.float32,
            )

        first_pieces(c, part, send, keep, own, copy)

    each(0, chunks, first)
    for k, peer in peers:
        square_copy(k, peer).wait()
    total[...] = square_ref[...] + squares[1] + squares[2] + squares[3]
    diagonal = lax.broadcasted_iota(jnp.int32, (extent, extent), 0) == lax.broadcasted_iota(
        jnp.int32, (extent, extent), 1
    )
    for b in range(local):
        row = jnp.broadcast_to(total[pl.ds(me * local + b, 1), :], (extent, extent))
        column = jnp.sum(jnp.where(diagonal, row, 0.0), axis=1, keepdims=True)
        scale[pl.ds(b * extent, extent), :] = lax.rsqrt(column / width + epsilon)
    each(0, chunks, lambda c: pass_on(c, send, recv, keep, copy))

    def last(c, out_ref, base):
        low, high = last_sum(c, recv, own, copy)
        column = pl.multiple_of((c - base) * wide, 128)
        out_ref[:, pl.ds(column, half)] = (low * scale[...]).astype(jnp.bfloat16)
        out_ref[:, pl.ds(pl.multiple_of(column + half, 128), half)] = (
            high * scale[...]
        ).astype(jnp.bfloat16)

    each(0, kv_chunks, lambda c: last(c, kv_ref, 0))
    each(kv_chunks, chunks, lambda c: last(c, q_ref, kv_chunks))
    all_sent(chunks, copy)


def heads(mixed, squares, kv_weight, q_weight, full_width):
    count = lax.axis_size("tensoror")
    total, width = mixed.shape
    rows = total // count
    kv_cols = kv_weight.shape[1]
    q_cols = q_weight.shape[1]
    wide = 512
    chunks = (kv_cols + q_cols) // wide
    return pl.pallas_call(
        functools.partial(heads_kernel, width=full_width),
        in_specs=[
            pl.BlockSpec(memory_space=pltpu.VMEM),
            pl.BlockSpec(memory_space=pltpu.VMEM),
            pl.BlockSpec(memory_space=pl.ANY),
            pl.BlockSpec(memory_space=pl.ANY),
        ],
        out_specs=[pl.BlockSpec(memory_space=pltpu.VMEM)] * 2,
        out_shape=[
            jax.ShapeDtypeStruct((rows, kv_cols), jnp.bfloat16),
            jax.ShapeDtypeStruct((rows, q_cols), jnp.bfloat16),
        ],
        scratch_shapes=[
            pltpu.VMEM((chunks, width, wide), jnp.bfloat16),
            pltpu.VMEM((count,) + squares.shape, jnp.float32),
            pltpu.VMEM(squares.shape, jnp.float32),
            pltpu.VMEM((rows, 1), jnp.float32),
            pltpu.SemaphoreType.DMA((chunks,)),
            pltpu.SemaphoreType.DMA((count,)),
            pltpu.SemaphoreType.DMA((count,)),
        ]
        + piece_scratch(chunks, rows, wide // 2),
        compiler_params=pltpu.CompilerParams(
            collective_id=2, has_side_effects=True, vmem_limit_bytes=VMEM
        ),
        cost_estimate=pl.CostEstimate(
            flops=2 * total * width * (kv_cols + q_cols),
            bytes_accessed=2 * width * (kv_cols + q_cols),
            transcendentals=0,
        ),
    )(mixed, squares, kv_weight, q_weight)


def exchange_kernel(text_ref, after_ref, out_ref, buffer, send_sem, recv_sem, own_sem):
    count = lax.axis_size("tensoror")
    me = lax.axis_index("tensoror")
    local = text_ref.shape[0]
    depth = out_ref.shape[2]
    barrier = pltpu.get_barrier_semaphore()
    for k in range(1, count):
        pl.semaphore_signal(
            barrier,
            inc=1,
            device_id={"tensoror": lax.rem(me + k, count)},
            device_id_type=MESH,
        )
    pl.semaphore_wait(barrier, count - 1)
    copies = []
    for k in (2, 1, 3):
        peer = lax.rem(me + k, count)
        copies.append(
            pltpu.make_async_remote_copy(
                src_ref=text_ref.at[:, :, pl.ds(pl.multiple_of(peer * depth, 128), depth)],
                dst_ref=out_ref.at[pl.ds(me * local, local)],
                send_sem=send_sem.at[k],
                recv_sem=recv_sem.at[k],
                device_id={"tensoror": peer},
                device_id_type=MESH,
            )
        )
    for copy in copies:
        copy.start()
    own = pltpu.make_async_copy(
        text_ref.at[:, :, pl.ds(pl.multiple_of(me * depth, 128), depth)], buffer, own_sem.at[0]
    )
    own.start()
    own.wait()
    back = pltpu.make_async_copy(buffer, out_ref.at[pl.ds(me * local, local)], own_sem.at[1])
    back.start()
    back.wait()
    for copy in copies:
        copy.wait()


def exchange(text, after):
    count = lax.axis_size("tensoror")
    local, rows, width = text.shape
    depth = width // count
    return pl.pallas_call(
        exchange_kernel,
        in_specs=[pl.BlockSpec(memory_space=pl.ANY)] * 2,
        out_specs=pl.BlockSpec(memory_space=pl.ANY),
        out_shape=jax.ShapeDtypeStruct((local * count, rows, depth), text.dtype),
        scratch_shapes=[
            pltpu.VMEM((local, rows, depth), text.dtype),
            pltpu.SemaphoreType.DMA((4,)),
            pltpu.SemaphoreType.DMA((4,)),
            pltpu.SemaphoreType.DMA((2,)),
        ],
        compiler_params=pltpu.CompilerParams(
            collective_id=0, has_side_effects=True, vmem_limit_bytes=VMEM
        ),
        cost_estimate=pl.CostEstimate(
            flops=30_000_000_000, bytes_accessed=text.size * 4, transcendentals=0
        ),
    )(text, after)


def mix_kernel(
    start_ref, count_ref, visual_ref, text_ref, gain_ref, out_ref, square_ref, *, sequences
):
    step = pl.program_id(0)
    rows = text_ref.shape[1]
    width = text_ref.shape[2]
    group = lax.axis_index("group")
    place = lax.axis_index("seq")
    index = group * sequences + step
    start = start_ref[index]
    slots = TILE * count_ref[index]
    visual = visual_ref[...].reshape(-1, width)
    total = visual.shape[0]
    shift = place * rows - start
    slot = shift + lax.broadcasted_iota(jnp.int32, (rows, total), 0)
    column = lax.broadcasted_iota(jnp.int32, (rows, total), 1)
    pick = ((slot == column) & (column < slots)).astype(jnp.float32).astype(jnp.bfloat16)
    placed = jnp.dot(pick, visual, preferred_element_type=jnp.float32)
    own = shift + lax.broadcasted_iota(jnp.int32, (rows, width), 0)
    inside = (own >= 0) & (own < slots)
    mixed = jnp.where(inside, placed, text_ref[0].astype(jnp.float32))
    summed = lax.dot_general(
        jnp.ones((8, width), jnp.float32),
        mixed * mixed,
        (((1,), (1,)), ((), ())),
        precision=lax.Precision.HIGHEST,
        preferred_element_type=jnp.float32,
    )
    square_ref[pl.ds(step, 1), :] = summed[0:1]
    out_ref[...] = (mixed * gain_ref[...]).astype(jnp.bfloat16)


def mix(starts, counts, visual, text, gain):
    devices, sequences, part, width = visual.shape
    rows = text.shape[1]
    return pl.pallas_call(
        functools.partial(mix_kernel, sequences=sequences),
        grid_spec=pltpu.PrefetchScalarGridSpec(
            num_scalar_prefetch=2,
            grid=(sequences,),
            in_specs=[
                pl.BlockSpec((devices, 1, part, width), lambda j, *_: (0, j, 0, 0)),
                pl.BlockSpec((1, rows, width), lambda j, *_: (j, 0, 0)),
                pl.BlockSpec((1, width), lambda j, *_: (0, lax.axis_index("tensoror"))),
            ],
            out_specs=[
                pl.BlockSpec((rows, width), lambda j, *_: (j, 0)),
                pl.BlockSpec((sequences, rows), lambda j, *_: (0, 0)),
            ],
        ),
        out_shape=[
            jax.ShapeDtypeStruct((sequences * rows, width), jnp.bfloat16),
            jax.ShapeDtypeStruct((sequences, rows), jnp.float32),
        ],
        compiler_params=pltpu.CompilerParams(vmem_limit_bytes=VMEM),
        cost_estimate=pl.CostEstimate(
            flops=2 * devices * part * rows * width * sequences,
            bytes_accessed=2 * (visual.size + 2 * text.size),
            transcendentals=0,
        ),
    )(starts, counts, visual, text, gain)


def attend_kernel(q_ref, k_ref, v_ref, out_ref, stacked, top, low, total):
    rows = q_ref.shape[1]
    chunk = 512
    blocks = chunk // rows
    place = lax.axis_index("seq")
    factor = math.log2(math.e) / math.sqrt(HEAD_SIZE)
    for j in range(GROUP_HEADS):
        stacked[j * rows : (j + 1) * rows, :] = q_ref[0, :, j * HEAD_SIZE : (j + 1) * HEAD_SIZE]
    top[...] = jnp.full_like(top, masked_score)
    low[...] = jnp.zeros_like(low)
    total[...] = jnp.zeros_like(total)

    def absorb(c, masked):
        keys = k_ref[pl.ds(c * blocks, blocks)].reshape(chunk, HEAD_SIZE)
        values = v_ref[pl.ds(c * blocks, blocks)].reshape(chunk, HEAD_SIZE)
        scores = lax.dot_general(
            stacked[...], keys, (((1,), (1,)), ((), ())), preferred_element_type=jnp.float32
        )
        if masked:
            row = lax.rem(lax.broadcasted_iota(jnp.int32, scores.shape, 0), rows) + place * rows
            column = lax.broadcasted_iota(jnp.int32, scores.shape, 1) + c * chunk
            scores = jnp.where(column <= row, scores, masked_score)
        old = top[...]
        new = jnp.maximum(old, jnp.max(scores, axis=1, keepdims=True))
        expo = jnp.exp2((scores - new) * factor)
        keep = jnp.exp2((old - new) * factor)
        low[...] = low[...] * keep + jnp.sum(expo, axis=1, keepdims=True)
        total[...] = total[...] * keep + jnp.dot(
            expo.astype(jnp.bfloat16), values, preferred_element_type=jnp.float32
        )
        top[...] = new

    last = lax.div(place, blocks)
    lax.fori_loop(0, last, lambda c, _: (absorb(c, False), 0)[1], 0)
    absorb(last, True)
    result = total[...] / low[...]
    for j in range(GROUP_HEADS):
        out_ref[0, :, j * HEAD_SIZE : (j + 1) * HEAD_SIZE] = result[
            j * rows : (j + 1) * rows
        ].astype(jnp.bfloat16)


def attend(queries, keyvalues):
    local, rows, q_cols = queries.shape
    devices = keyvalues.shape[0]
    wide = GROUP_HEADS * HEAD_SIZE
    heads = KEY_VALUE_HEADS
    stack = GROUP_HEADS * rows
    return pl.pallas_call(
        attend_kernel,
        grid=(local, heads),
        in_specs=[
            pl.BlockSpec((1, rows, wide), lambda b, h: (b, 0, h)),
            pl.BlockSpec((devices, 1, rows, HEAD_SIZE), lambda b, h: (0, b, 0, h)),
            pl.BlockSpec((devices, 1, rows, HEAD_SIZE), lambda b, h: (0, b, 0, h + heads)),
        ],
        out_specs=pl.BlockSpec((1, rows, wide), lambda b, h: (b, 0, h)),
        out_shape=jax.ShapeDtypeStruct((local, rows, q_cols), jnp.bfloat16),
        scratch_shapes=[
            pltpu.VMEM((stack, HEAD_SIZE), jnp.bfloat16),
            pltpu.VMEM((stack, 1), jnp.float32),
            pltpu.VMEM((stack, 1), jnp.float32),
            pltpu.VMEM((stack, HEAD_SIZE), jnp.float32),
        ],
        compiler_params=pltpu.CompilerParams(vmem_limit_bytes=VMEM),
        cost_estimate=pl.CostEstimate(
            flops=4 * local * rows * q_cols * rows * devices,
            bytes_accessed=2 * keyvalues.size,
            transcendentals=0,
        ),
    )(queries, keyvalues, keyvalues)


def shards(
    visual_hidden,
    projector_weight,
    text_embeddings,
    tile_counts,
    image_start,
    norm_gain,
    query_weight,
    keyvalue_weight,
):
    sequence_local, extent_rows, width = text_embeddings.shape
    sequences, slot_rows, depth = visual_hidden.shape
    activated = jax.nn.gelu(visual_hidden.astype(jnp.float32), approximate=False).astype(
        jnp.bfloat16
    )
    visual = project(activated.reshape(sequences * slot_rows, depth), projector_weight)
    spread = lax.all_gather(visual, "seq", axis=0, tiled=False)
    spread = spread.reshape(-1, sequences, slot_rows, depth)
    text = exchange(text_embeddings, visual)
    mixed, squares = mix(image_start, tile_counts, spread, text, norm_gain.reshape(1, width))
    keyvalues, queries = heads(mixed, squares, keyvalue_weight, query_weight, width)
    gathered = lax.all_gather(
        keyvalues.reshape(sequence_local, extent_rows, -1), "seq", axis=0, tiled=False
    )
    return attend(queries.reshape(sequence_local, extent_rows, -1), gathered)


def solution(mesh):
    in_specs = (
        P("group", "seq", "tensoror"),
        P("tensoror", None),
        P(("group", "tensoror"), "seq", None),
        P(),
        P(),
        P(),
        P("tensoror", None),
        P("tensoror", None),
    )
    out_specs = P(("group", "tensoror"), "seq", None)
    return jax.shard_map(shards, mesh=mesh, in_specs=in_specs, out_specs=out_specs, check_vma=False)
```

```python
import functools
import math

import jax
import jax.numpy as jnp
from jax import lax
from jax.experimental import pallas as pl
from jax.experimental.pallas import tpu as pltpu
from jax.sharding import PartitionSpec as P

QUERY_HEADS = 20
KEY_VALUE_HEADS = 4
HEAD_SIZE = 128
TILE = 256
GROUP_HEADS = QUERY_HEADS // KEY_VALUE_HEADS
MESH = pl.DeviceIdType.MESH

epsilon = 1e-06
masked_score = -1e30
VMEM = 60 * 1024 * 1024


def neighbours():
    count = lax.axis_size("tensoror")
    me = lax.axis_index("tensoror")
    return me, lax.rem(me + 1, count), lax.rem(me + 2, count), lax.rem(me + 3, count)


def greet(peers):
    barrier = pltpu.get_barrier_semaphore()
    for peer in peers:
        pl.semaphore_signal(
            barrier, inc=1, device_id=peer, device_id_type=MESH
        )
    pl.semaphore_wait(barrier, len(peers))


TO_RIGHT = (False, True, True, False, False, True)


def piece(kind, c, send, recv, send_sem, recv_sem):
    me, right, opposite, left = neighbours()
    return pltpu.make_async_remote_copy(
        src_ref=send.at[kind, c],
        dst_ref=recv.at[kind, c],
        send_sem=send_sem.at[kind, c],
        recv_sem=recv_sem.at[kind, c],
        device_id={"tensoror": right if TO_RIGHT[kind] else left},
        device_id_type=MESH,
    )


def first_pieces(c, part, send, keep, own, copy):
    me, right, opposite, left = neighbours()
    half = send.shape[3]
    sums = part(2, opposite)
    send[0, c] = sums[:, :half].astype(jnp.bfloat16)
    send[1, c] = sums[:, half:].astype(jnp.bfloat16)
    copy(0, c).start()
    copy(1, c).start()
    sums = part(1, right)
    send[2, c] = sums[:, :half].astype(jnp.bfloat16)
    keep[1, c] = sums[:, half:]
    copy(2, c).start()
    sums = part(3, left)
    send[3, c] = sums[:, half:].astype(jnp.bfloat16)
    keep[0, c] = sums[:, :half]
    copy(3, c).start()
    own[c] = part(0, me)


def pass_on(c, send, recv, keep, copy):
    for side in (0, 1):
        copy(side, c).wait_recv()
        send[4 + side, c] = (keep[side, c] + recv[side, c].astype(jnp.float32)).astype(
            jnp.bfloat16
        )
        copy(4 + side, c).start()


def last_sum(c, recv, own, copy):
    for kind in (2, 3, 4, 5):
        copy(kind, c).wait_recv()
    half = recv.shape[3]
    first = own[c, :, :half] + recv[2, c].astype(jnp.float32) + recv[4, c].astype(jnp.float32)
    second = own[c, :, half:] + recv[3, c].astype(jnp.float32) + recv[5, c].astype(jnp.float32)
    return first, second


def each(start, stop, body):
    lax.fori_loop(start, stop, lambda c, _: (body(c), 0)[1], 0)


def all_sent(chunks, copy):
    def wait(c):
        for kind in range(6):
            copy(kind, c).wait_send()

    each(0, chunks, wait)


def piece_scratch(chunks, rows, half):
    return [
        pltpu.VMEM((6, chunks, rows, half), jnp.bfloat16),
        pltpu.VMEM((6, chunks, rows, half), jnp.bfloat16),
        pltpu.VMEM((2, chunks, rows, half), jnp.float32),
        pltpu.VMEM((chunks, rows, 2 * half), jnp.float32),
        pltpu.SemaphoreType.DMA((6, chunks)),
        pltpu.SemaphoreType.DMA((6, chunks)),
    ]


def project_kernel(
    act_ref, w_ref, out_ref, weights, weight_sem, send, recv, keep, own, send_sem, recv_sem
):
    me, right, opposite, left = neighbours()
    chunks, rows, wide = own.shape
    half = wide // 2

    def load(k, dest, c):
        column = pl.multiple_of(dest * (chunks * wide) + c * wide, 128)
        return pltpu.make_async_copy(
            w_ref.at[:, pl.ds(column, wide)], weights.at[k, c], weight_sem.at[k, c]
        )

    for c in range(chunks):
        for k, dest in ((2, opposite), (1, right), (3, left), (0, me)):
            load(k, dest, c).start()
    greet([{"tensoror": peer} for peer in (left, right)])

    def copy(kind, c):
        return piece(kind, c, send, recv, send_sem, recv_sem)

    def first(c):
        def part(k, dest):
            load(k, dest, c).wait()
            return jnp.dot(act_ref[...], weights[k, c], preferred_element_type=jnp.float32)

        first_pieces(c, part, send, keep, own, copy)

    def last(c):
        low, high = last_sum(c, recv, own, copy)
        column = pl.multiple_of(c * wide, 128)
        out_ref[:, pl.ds(column, half)] = low.astype(jnp.bfloat16)
        out_ref[:, pl.ds(pl.multiple_of(column + half, 128), half)] = high.astype(jnp.bfloat16)

    each(0, chunks, first)
    each(0, chunks, lambda c: pass_on(c, send, recv, keep, copy))
    each(0, chunks, last)
    all_sent(chunks, copy)


def project(activated, weight):
    rows, depth = activated.shape
    width = weight.shape[1] // lax.axis_size("tensoror")
    wide = 256
    chunks = width // wide
    return pl.pallas_call(
        project_kernel,
        in_specs=[
            pl.BlockSpec(memory_space=pltpu.VMEM),
            pl.BlockSpec(memory_space=pl.ANY),
        ],
        out_specs=pl.BlockSpec(memory_space=pltpu.VMEM),
        out_shape=jax.ShapeDtypeStruct((rows, width), jnp.bfloat16),
        scratch_shapes=[
            pltpu.VMEM((4, chunks, depth, wide), jnp.bfloat16),
            pltpu.SemaphoreType.DMA((4, chunks)),
        ]
        + piece_scratch(chunks, rows, wide // 2),
        compiler_params=pltpu.CompilerParams(
            collective_id=1, has_side_effects=True, vmem_limit_bytes=VMEM
        ),
        cost_estimate=pl.CostEstimate(
            flops=8 * rows * depth * width, bytes_accessed=2 * weight.size, transcendentals=0
        ),
    )(activated, weight)


def heads_kernel(
    x_ref,
    square_ref,
    wkv_ref,
    wq_ref,
    kv_ref,
    q_ref,
    weights,
    squares,
    total,
    scale,
    weight_sem,
    square_send,
    square_recv,
    send,
    recv,
    keep,
    own,
    send_sem,
    recv_sem,
    *,
    width,
):
    me, right, opposite, left = neighbours()
    chunks, rows, wide = own.shape
    half = wide // 2
    extent = square_ref.shape[1]
    local = rows // extent
    kv_chunks = kv_ref.shape[1] // wide
    for c in range(chunks):
        source = wkv_ref if c < kv_chunks else wq_ref
        column = (c if c < kv_chunks else c - kv_chunks) * wide
        pltpu.make_async_copy(
            source.at[:, pl.ds(column, wide)], weights.at[c], weight_sem.at[c]
        ).start()
    greet([{"tensoror": peer} for peer in (right, opposite, left)])

    def square_copy(k, peer):
        return pltpu.make_async_remote_copy(
            src_ref=square_ref,
            dst_ref=squares.at[k],
            send_sem=square_send.at[k],
            recv_sem=square_recv.at[k],
            device_id={"tensoror": peer},
            device_id_type=MESH,
        )

    peers = ((1, right), (2, opposite), (3, left))
    for k, peer in peers:
        square_copy(k, peer).start()

    def copy(kind, c):
        return piece(kind, c, send, recv, send_sem, recv_sem)

    def first(c):
        pltpu.make_async_copy(
            wkv_ref.at[:, pl.ds(0, wide)], weights.at[c], weight_sem.at[c]
        ).wait()

        def part(k, dest):
            return jnp.dot(
                x_ref[pl.ds(pl.multiple_of(dest * rows, rows), rows), :],
                weights[c],
                preferred_element_type=jnp.float32,
            )

        first_pieces(c, part, send, keep, own, copy)

    each(0, chunks, first)
    for k, peer in peers:
        square_copy(k, peer).wait()
    total[...] = square_ref[...] + squares[1] + squares[2] + squares[3]
    diagonal = lax.broadcasted_iota(jnp.int32, (extent, extent), 0) == lax.broadcasted_iota(
        jnp.int32, (extent, extent), 1
    )
    for b in range(local):
        row = jnp.broadcast_to(total[pl.ds(me * local + b, 1), :], (extent, extent))
        column = jnp.sum(jnp.where(diagonal, row, 0.0), axis=1, keepdims=True)
        scale[pl.ds(b * extent, extent), :] = lax.rsqrt(column / width + epsilon)
    each(0, chunks, lambda c: pass_on(c, send, recv, keep, copy))

    def last(c, out_ref, base):
        low, high = last_sum(c, recv, own, copy)
        column = pl.multiple_of((c - base) * wide, 128)
        out_ref[:, pl.ds(column, half)] = (low * scale[...]).astype(jnp.bfloat16)
        out_ref[:, pl.ds(pl.multiple_of(column + half, 128), half)] = (
            high * scale[...]
        ).astype(jnp.bfloat16)

    each(0, kv_chunks, lambda c: last(c, kv_ref, 0))
    each(kv_chunks, chunks, lambda c: last(c, q_ref, kv_chunks))
    all_sent(chunks, copy)


def heads(mixed, squares, kv_weight, q_weight, full_width):
    count = lax.axis_size("tensoror")
    total, width = mixed.shape
    rows = total // count
    kv_cols = kv_weight.shape[1]
    q_cols = q_weight.shape[1]
    wide = 512
    chunks = (kv_cols + q_cols) // wide
    return pl.pallas_call(
        functools.partial(heads_kernel, width=full_width),
        in_specs=[
            pl.BlockSpec(memory_space=pltpu.VMEM),
            pl.BlockSpec(memory_space=pltpu.VMEM),
            pl.BlockSpec(memory_space=pl.ANY),
            pl.BlockSpec(memory_space=pl.ANY),
        ],
        out_specs=[pl.BlockSpec(memory_space=pltpu.VMEM)] * 2,
        out_shape=[
            jax.ShapeDtypeStruct((rows, kv_cols), jnp.bfloat16),
            jax.ShapeDtypeStruct((rows, q_cols), jnp.bfloat16),
        ],
        scratch_shapes=[
            pltpu.VMEM((chunks, width, wide), jnp.bfloat16),
            pltpu.VMEM((count,) + squares.shape, jnp.float32),
            pltpu.VMEM(squares.shape, jnp.float32),
            pltpu.VMEM((rows, 1), jnp.float32),
            pltpu.SemaphoreType.DMA((chunks,)),
            pltpu.SemaphoreType.DMA((count,)),
            pltpu.SemaphoreType.DMA((count,)),
        ]
        + piece_scratch(chunks, rows, wide // 2),
        compiler_params=pltpu.CompilerParams(
            collective_id=2, has_side_effects=True, vmem_limit_bytes=VMEM
        ),
        cost_estimate=pl.CostEstimate(
            flops=2 * total * width * (kv_cols + q_cols),
            bytes_accessed=2 * width * (kv_cols + q_cols),
            transcendentals=0,
        ),
    )(mixed, squares, kv_weight, q_weight)


OWN, NEXT, PREV, ACROSS, PARTNER = (0, 0, 0), (1, 0, 0), (3, 0, 0), (0, 1, 0), (0, 0, 1)
FAR = (2, 0, 0)
KINDS = {
    "next": (OWN, PREV, None),
    "prev": (OWN, NEXT, None),
    "across": (OWN, ACROSS, None),
    "partner": (OWN, PARTNER, None),
    "far0": (NEXT, PREV, 0),
    "far1": (PREV, NEXT, 1),
    "next_across": (ACROSS, PREV, None),
    "prev_across": (ACROSS, NEXT, None),
    "far_across0": (FAR, ACROSS, 0),
    "far_across1": (FAR, ACROSS, 1),
}
GOT = {
    "next": NEXT,
    "prev": PREV,
    "across": ACROSS,
    "partner": PARTNER,
    "far0": FAR,
    "far1": FAR,
    "next_across": (1, 1, 0),
    "prev_across": (3, 1, 0),
    "far_across0": (2, 1, 0),
    "far_across1": (2, 1, 0),
}
for name in list(GOT):
    if name != "partner":
        KINDS["twin_" + name] = (GOT[name], PARTNER, KINDS[name][2])
        GOT["twin_" + name] = GOT[name][:2] + (1,)
ORDER = {name: k for k, name in enumerate(KINDS)}


def seq_at(offset):
    place = lax.axis_index("seq")
    y = lax.rem(lax.div(place, 4) + offset[0], 4)
    z = lax.rem(lax.div(place, 2) + offset[1], 2)
    core = lax.rem(place + offset[2], 2)
    return y * 4 + z * 2 + core


class Gather:
    def __init__(self, own_ref, blocks, send_sem, recv_sem):
        self.refs = own_ref, blocks, send_sem, recv_sem

    def copy(self, name, arrival):
        own_ref, blocks, send_sem, recv_sem = self.refs
        block, target, half = KINDS[name]
        rows = blocks.shape[1]
        cut = pl.ds(0, rows) if half is None else pl.ds(half * (rows // 2), rows // 2)
        where = blocks.at[seq_at(GOT[name] if arrival else block), cut]
        source = own_ref if block == OWN and not arrival else where
        k = ORDER[name]
        return pltpu.make_async_remote_copy(
            src_ref=source,
            dst_ref=where,
            send_sem=send_sem.at[k],
            recv_sem=recv_sem.at[k],
            device_id={"seq": seq_at(target)},
            device_id_type=MESH,
        )

    def start(self, *names):
        for name in names:
            self.copy(name, False).start()

    def arrived(self, *names):
        for name in names:
            self.copy(name, True).wait_recv()

    def finish(self):
        for name in KINDS:
            self.copy(name, False).wait_send()


def seq_peers():
    return [{"seq": seq_at(offset)} for offset in (NEXT, PREV, ACROSS, PARTNER)]


GATHER_SEMAPHORES = [
    pltpu.SemaphoreType.DMA((len(KINDS),)),
    pltpu.SemaphoreType.DMA((len(KINDS),)),
]


def mix_kernel(
    start_ref,
    count_ref,
    visual_ref,
    text_ref,
    gain_ref,
    out_ref,
    square_ref,
    blocks,
    text,
    text_send,
    text_recv,
    own_sem,
    send_sem,
    recv_sem,
):
    me, right, opposite, left = neighbours()
    group = lax.axis_index("group")
    place = lax.axis_index("seq")
    local = text_ref.shape[0]
    sequences, rows, width = text.shape
    part = blocks.shape[1] // sequences
    gather = Gather(visual_ref, blocks, send_sem, recv_sem)

    def columns(peer):
        return text_ref.at[:, :, pl.ds(pl.multiple_of(peer * width, 128), width)]

    own_text = pltpu.make_async_copy(columns(me), text.at[pl.ds(me * local, local)], own_sem)
    own_text.start()
    greet([{"tensoror": peer} for peer in (right, opposite, left)] + seq_peers())
    gather.start("next", "prev", "across", "partner")
    exchanges = []
    for k, peer in ((2, opposite), (1, right), (3, left)):
        exchanges.append(
            pltpu.make_async_remote_copy(
                src_ref=columns(peer),
                dst_ref=text.at[pl.ds(me * local, local)],
                send_sem=text_send.at[k],
                recv_sem=text_recv.at[k],
                device_id={"tensoror": peer},
                device_id_type=MESH,
            )
        )
    for exchange in exchanges:
        exchange.start()
    blocks[place] = visual_ref[...]
    gather.arrived("next")
    gather.start("far0", "twin_next")
    gather.arrived("prev")
    gather.start("far1", "twin_prev")
    gather.arrived("across")
    gather.start("next_across", "prev_across", "twin_across")
    gather.arrived("far0")
    gather.start("far_across0", "twin_far0")
    gather.arrived("far1")
    gather.start("far_across1", "twin_far1")
    gather.arrived("next_across")
    gather.start("twin_next_across")
    gather.arrived("prev_across")
    gather.start("twin_prev_across")
    gather.arrived("far_across0")
    gather.start("twin_far_across0")
    gather.arrived("far_across1")
    gather.start("twin_far_across1")
    gather.arrived("partner", *[name for name in KINDS if name.startswith("twin_")])
    own_text.wait()
    for exchange in exchanges:
        exchange.wait()
    diagonal = lax.broadcasted_iota(jnp.int32, (rows, rows), 0) == lax.broadcasted_iota(
        jnp.int32, (rows, rows), 1
    )

    def one(i):
        start = start_ref[group * sequences + i]
        slots = TILE * count_ref[group * sequences + i]
        visual = blocks[:, pl.ds(pl.multiple_of(i * part, part), part), :].reshape(-1, width)
        total = visual.shape[0]
        shift = place * rows - start
        slot = shift + lax.broadcasted_iota(jnp.int32, (rows, total), 0)
        column = lax.broadcasted_iota(jnp.int32, (rows, total), 1)
        pick = jnp.where((slot == column) & (column < slots), 1.0, 0.0).astype(jnp.bfloat16)
        placed = jnp.dot(pick, visual, preferred_element_type=jnp.float32)
        own = shift + lax.broadcasted_iota(jnp.int32, (rows, width), 0)
        inside = (own >= 0) & (own < slots)
        mixed = jnp.where(inside, placed, text[i].astype(jnp.float32))
        squares = jnp.sum(mixed * mixed, axis=1, keepdims=True)
        square_ref[pl.ds(i, 1), :] = jnp.sum(
            jnp.where(diagonal, squares, 0.0), axis=0, keepdims=True
        )
        out_ref[pl.ds(pl.multiple_of(i * rows, rows), rows), :] = (mixed * gain_ref[...]).astype(
            jnp.bfloat16
        )

    each(0, sequences, one)
    gather.finish()


def mix(starts, counts, visual, text, gain):
    devices = lax.axis_size("seq")
    count = lax.axis_size("tensoror")
    local, rows, full = text.shape
    width = full // count
    sequences = local * count
    smem = pl.BlockSpec(memory_space=pltpu.SMEM)
    vmem = pl.BlockSpec(memory_space=pltpu.VMEM)
    return pl.pallas_call(
        mix_kernel,
        in_specs=[smem, smem, vmem, pl.BlockSpec(memory_space=pl.ANY), vmem],
        out_specs=[vmem, vmem],
        out_shape=[
            jax.ShapeDtypeStruct((sequences * rows, width), jnp.bfloat16),
            jax.ShapeDtypeStruct((sequences, rows), jnp.float32),
        ],
        scratch_shapes=[
            pltpu.VMEM((devices,) + visual.shape, jnp.bfloat16),
            pltpu.VMEM((sequences, rows, width), jnp.bfloat16),
            pltpu.SemaphoreType.DMA((4,)),
            pltpu.SemaphoreType.DMA((4,)),
            pltpu.SemaphoreType.DMA,
        ]
        + GATHER_SEMAPHORES,
        compiler_params=pltpu.CompilerParams(
            collective_id=0, has_side_effects=True, vmem_limit_bytes=VMEM
        ),
    )(starts, counts, visual, text, gain)


def attend_kernel(
    q_ref, kv_ref, out_ref, blocks, queries, top, low, total, send_sem, recv_sem
):
    place = lax.axis_index("seq")
    rows = HEAD_SIZE
    units = queries.shape[0]
    factor = math.log2(math.e) / math.sqrt(HEAD_SIZE)
    gather = Gather(kv_ref, blocks, send_sem, recv_sem)
    greet(seq_peers())
    gather.start("next", "prev", "across", "partner")
    blocks[place] = kv_ref[...]
    for u in range(units):
        b, h = divmod(u, KEY_VALUE_HEADS)
        for j in range(GROUP_HEADS):
            column = (h * GROUP_HEADS + j) * HEAD_SIZE
            queries[u, j * rows : (j + 1) * rows, :] = q_ref[
                b * rows : (b + 1) * rows, column : column + HEAD_SIZE
            ]
    top[...] = jnp.full_like(top, masked_score)
    low[...] = jnp.zeros_like(low)
    total[...] = jnp.zeros_like(total)

    def absorb(u, chip, masked):
        b = pl.ds(pl.multiple_of(lax.div(u, KEY_VALUE_HEADS) * rows, rows), rows)
        h = lax.rem(u, KEY_VALUE_HEADS) * HEAD_SIZE
        pair = pl.ds(2 * chip, 2)
        keys = blocks[pair, b, pl.ds(pl.multiple_of(h, 128), HEAD_SIZE)]
        values = blocks[
            pair, b, pl.ds(pl.multiple_of(h + KEY_VALUE_HEADS * HEAD_SIZE, 128), HEAD_SIZE)
        ]
        scores = lax.dot_general(
            keys.reshape(2 * rows, HEAD_SIZE),
            queries[u],
            (((1,), (1,)), ((), ())),
            preferred_element_type=jnp.float32,
        )
        if masked:
            key = lax.broadcasted_iota(jnp.int32, scores.shape, 0)
            query = (
                lax.rem(lax.broadcasted_iota(jnp.int32, scores.shape, 1), rows)
                + lax.rem(place, 2) * rows
            )
            scores = jnp.where(key <= query, scores, masked_score)
        old = top[u]
        new = jnp.maximum(old, jnp.max(scores, axis=0, keepdims=True))
        expo = jnp.exp2((scores - new) * factor)
        keep = jnp.exp2((old - new) * factor)
        low[u] = low[u] * keep + jnp.sum(expo, axis=0, keepdims=True)
        total[u] = total[u] * keep + lax.dot_general(
            values.reshape(2 * rows, HEAD_SIZE),
            expo.astype(jnp.bfloat16),
            (((0,), (0,)), ((), ())),
            preferred_element_type=jnp.float32,
        )
        top[u] = new

    chip = lax.div(place, 2)

    def absorb_all(offset):
        other = lax.div(seq_at(offset), 2)

        @pl.when(other < chip)
        def _():
            each(0, units, lambda u: absorb(u, other, False))

    gather.arrived("partner")
    each(0, units, lambda u: absorb(u, chip, True))
    gather.arrived("next")
    gather.start("far0", "twin_next")
    gather.arrived("prev")
    gather.start("far1", "twin_prev")
    gather.arrived("across")
    gather.start("next_across", "prev_across", "twin_across")
    gather.arrived("twin_next")
    absorb_all(NEXT)
    gather.arrived("far0")
    gather.start("far_across0", "twin_far0")
    gather.arrived("far1")
    gather.start("far_across1", "twin_far1")
    gather.arrived("twin_prev")
    absorb_all(PREV)
    gather.arrived("twin_across")
    absorb_all(ACROSS)
    gather.arrived("twin_far0", "twin_far1")
    absorb_all(FAR)
    gather.arrived("next_across")
    gather.start("twin_next_across")
    gather.arrived("prev_across")
    gather.start("twin_prev_across")
    gather.arrived("far_across0")
    gather.start("twin_far_across0")
    gather.arrived("far_across1")
    gather.start("twin_far_across1")
    gather.arrived("twin_next_across")
    absorb_all((1, 1, 0))
    gather.arrived("twin_prev_across")
    absorb_all((3, 1, 0))
    gather.arrived("twin_far_across0", "twin_far_across1")
    absorb_all((2, 1, 0))

    for u in range(units):
        b, h = divmod(u, KEY_VALUE_HEADS)
        result = total[u] / low[u]
        for j in range(GROUP_HEADS):
            column = (h * GROUP_HEADS + j) * HEAD_SIZE
            out_ref[b * rows : (b + 1) * rows, column : column + HEAD_SIZE] = jnp.transpose(
                result[:, j * rows : (j + 1) * rows]
            ).astype(jnp.bfloat16)
    gather.finish()


def attend(queries, keyvalues):
    devices = lax.axis_size("seq")
    rows, q_cols = queries.shape
    units = rows // HEAD_SIZE * KEY_VALUE_HEADS
    stack = GROUP_HEADS * HEAD_SIZE
    vmem = pl.BlockSpec(memory_space=pltpu.VMEM)
    return pl.pallas_call(
        attend_kernel,
        in_specs=[vmem, vmem],
        out_specs=vmem,
        out_shape=jax.ShapeDtypeStruct((rows, q_cols), jnp.bfloat16),
        scratch_shapes=[
            pltpu.VMEM((devices,) + keyvalues.shape, jnp.bfloat16),
            pltpu.VMEM((units, stack, HEAD_SIZE), jnp.bfloat16),
            pltpu.VMEM((units, 1, stack), jnp.float32),
            pltpu.VMEM((units, 1, stack), jnp.float32),
            pltpu.VMEM((units, HEAD_SIZE, stack), jnp.float32),
        ]
        + GATHER_SEMAPHORES,
        compiler_params=pltpu.CompilerParams(
            collective_id=3, has_side_effects=True, vmem_limit_bytes=VMEM
        ),
    )(queries, keyvalues)


def shards(
    visual_hidden,
    projector_weight,
    text_embeddings,
    tile_counts,
    image_start,
    norm_gain,
    query_weight,
    keyvalue_weight,
):
    sequence_local, extent_rows, width = text_embeddings.shape
    sequences, slot_rows, depth = visual_hidden.shape
    activated = jax.nn.gelu(visual_hidden.astype(jnp.float32), approximate=False).astype(
        jnp.bfloat16
    )
    visual = project(activated.reshape(sequences * slot_rows, depth), projector_weight)
    gain = lax.dynamic_slice_in_dim(norm_gain, lax.axis_index("tensoror") * depth, depth)
    mixed, squares = mix(image_start, tile_counts, visual, text_embeddings, gain.reshape(1, depth))
    keyvalues, queries = heads(mixed, squares, keyvalue_weight, query_weight, width)
    return attend(queries, keyvalues).reshape(sequence_local, extent_rows, -1)


def solution(mesh):
    in_specs = (
        P("group", "seq", "tensoror"),
        P("tensoror", None),
        P(("group", "tensoror"), "seq", None),
        P(),
        P(),
        P(),
        P("tensoror", None),
        P("tensoror", None),
    )
    out_specs = P(("group", "tensoror"), "seq", None)
    return jax.shard_map(shards, mesh=mesh, in_specs=in_specs, out_specs=out_specs, check_vma=False)
```

```python
import functools
import math

import jax
import jax.numpy as jnp
from jax import lax
from jax.experimental import pallas as pl
from jax.experimental.pallas import tpu as pltpu
from jax.sharding import PartitionSpec as P

QUERY_HEADS = 20
KEY_VALUE_HEADS = 4
HEAD_SIZE = 128
TILE = 256
GROUP_HEADS = QUERY_HEADS // KEY_VALUE_HEADS
MESH = pl.DeviceIdType.MESH

epsilon = 1e-06
masked_score = -1e30
VMEM = 60 * 1024 * 1024


def neighbours():
    count = lax.axis_size("tensoror")
    me = lax.axis_index("tensoror")
    return me, lax.rem(me + 1, count), lax.rem(me + 2, count), lax.rem(me + 3, count)


def greet(peers):
    barrier = pltpu.get_barrier_semaphore()
    for peer in peers:
        pl.semaphore_signal(
            barrier, inc=1, device_id=peer, device_id_type=MESH
        )
    pl.semaphore_wait(barrier, len(peers))


TO_RIGHT = (False, True, True, False, False, True)


class Pieces:
    def __init__(self, send, recv, keep, own, send_sem, recv_sem):
        self.send, self.recv, self.keep, self.own = send, recv, keep, own
        self.send_sem, self.recv_sem = send_sem, recv_sem
        self.chunks, self.rows, self.wide = own.shape

    def copy(self, kind, c):
        me, right, opposite, left = neighbours()
        return pltpu.make_async_remote_copy(
            src_ref=self.send.at[kind, c],
            dst_ref=self.recv.at[kind, c],
            send_sem=self.send_sem.at[kind, c],
            recv_sem=self.recv_sem.at[kind, c],
            device_id={"tensoror": right if TO_RIGHT[kind] else left},
            device_id_type=MESH,
        )

    def first(self, c, part):
        me, right, opposite, left = neighbours()
        send, keep = self.send, self.keep
        half = self.rows // 2
        sums = part(2, opposite)
        send[0, c] = sums[:half].astype(jnp.bfloat16)
        send[1, c] = sums[half:].astype(jnp.bfloat16)
        self.copy(0, c).start()
        self.copy(1, c).start()
        sums = part(1, right)
        send[2, c] = sums[:half].astype(jnp.bfloat16)
        keep[1, c] = sums[half:]
        self.copy(2, c).start()
        sums = part(3, left)
        send[3, c] = sums[half:].astype(jnp.bfloat16)
        keep[0, c] = sums[:half]
        self.copy(3, c).start()
        self.own[c] = part(0, me)

    def pass_on(self, c):
        for side in (0, 1):
            self.copy(side, c).wait_recv()
            self.send[4 + side, c] = (
                self.keep[side, c] + self.recv[side, c].astype(jnp.float32)
            ).astype(jnp.bfloat16)
            self.copy(4 + side, c).start()

    def last(self, c):
        for kind in (2, 3, 4, 5):
            self.copy(kind, c).wait_recv()
        half = self.rows // 2
        own, recv = self.own, self.recv
        return [
            own[c, side * half : (side + 1) * half]
            + recv[2 + side, c].astype(jnp.float32)
            + recv[4 + side, c].astype(jnp.float32)
            for side in (0, 1)
        ]

    def finish(self):
        def wait(c):
            for kind in range(6):
                self.copy(kind, c).wait_send()

        each(0, self.chunks, wait)


def each(start, stop, body):
    lax.fori_loop(start, stop, lambda c, _: (body(c), 0)[1], 0)


def piece_scratch(chunks, rows, wide):
    return [
        pltpu.VMEM((6, chunks, rows // 2, wide), jnp.bfloat16),
        pltpu.VMEM((6, chunks, rows // 2, wide), jnp.bfloat16),
        pltpu.VMEM((2, chunks, rows // 2, wide), jnp.float32),
        pltpu.VMEM((chunks, rows, wide), jnp.float32),
        pltpu.SemaphoreType.DMA((6, chunks)),
        pltpu.SemaphoreType.DMA((6, chunks)),
    ]


def project_kernel(act_ref, w_ref, out_ref, weights, weight_sem, *scratch):
    me, right, opposite, left = neighbours()
    pieces = Pieces(*scratch)
    chunks, rows, wide = pieces.own.shape

    def load(k, dest, c):
        column = pl.multiple_of(dest * (chunks * wide) + c * wide, 128)
        return pltpu.make_async_copy(
            w_ref.at[:, pl.ds(column, wide)], weights.at[k, c], weight_sem.at[k, c]
        )

    for c in range(chunks):
        for k, dest in ((2, opposite), (1, right), (3, left), (0, me)):
            load(k, dest, c).start()
    greet([{"tensoror": peer} for peer in (left, right)])

    def first(c):
        def part(k, dest):
            load(k, dest, c).wait()
            return jnp.dot(act_ref[...], weights[k, c], preferred_element_type=jnp.float32)

        pieces.first(c, part)

    def last(c):
        column = pl.ds(pl.multiple_of(c * wide, 128), wide)
        for side, sums in enumerate(pieces.last(c)):
            half = rows // 2
            out_ref[side * half : (side + 1) * half, column] = sums.astype(jnp.bfloat16)

    each(0, chunks, first)
    each(0, chunks, pieces.pass_on)
    each(0, chunks, last)
    pieces.finish()


def project(activated, weight):
    rows, depth = activated.shape
    width = weight.shape[1] // lax.axis_size("tensoror")
    wide = 256
    chunks = width // wide
    return pl.pallas_call(
        project_kernel,
        in_specs=[
            pl.BlockSpec(memory_space=pltpu.VMEM),
            pl.BlockSpec(memory_space=pl.ANY),
        ],
        out_specs=pl.BlockSpec(memory_space=pltpu.VMEM),
        out_shape=jax.ShapeDtypeStruct((rows, width), jnp.bfloat16),
        scratch_shapes=[
            pltpu.VMEM((4, chunks, depth, wide), jnp.bfloat16),
            pltpu.SemaphoreType.DMA((4, chunks)),
        ]
        + piece_scratch(chunks, rows, wide),
        compiler_params=pltpu.CompilerParams(
            collective_id=1, has_side_effects=True, vmem_limit_bytes=VMEM
        ),
    )(activated, weight)


OWN, NEXT, PREV, ACROSS, PARTNER = (0, 0, 0), (1, 0, 0), (3, 0, 0), (0, 1, 0), (0, 0, 1)
FAR = (2, 0, 0)
KINDS = {
    "next": (OWN, PREV, None),
    "prev": (OWN, NEXT, None),
    "across": (OWN, ACROSS, None),
    "partner": (OWN, PARTNER, None),
    "far0": (NEXT, PREV, 0),
    "far1": (PREV, NEXT, 1),
    "next_across": (ACROSS, PREV, None),
    "prev_across": (ACROSS, NEXT, None),
    "far_across0": (FAR, ACROSS, 0),
    "far_across1": (FAR, ACROSS, 1),
}
GOT = {
    "next": NEXT,
    "prev": PREV,
    "across": ACROSS,
    "partner": PARTNER,
    "far0": FAR,
    "far1": FAR,
    "next_across": (1, 1, 0),
    "prev_across": (3, 1, 0),
    "far_across0": (2, 1, 0),
    "far_across1": (2, 1, 0),
}
for name in list(GOT):
    if name != "partner":
        KINDS["twin_" + name] = (GOT[name], PARTNER, KINDS[name][2])
        GOT["twin_" + name] = GOT[name][:2] + (1,)
ORDER = {name: k for k, name in enumerate(KINDS)}


def seq_at(offset):
    place = lax.axis_index("seq")
    y = lax.rem(lax.div(place, 4) + offset[0], 4)
    z = lax.rem(lax.div(place, 2) + offset[1], 2)
    core = lax.rem(place + offset[2], 2)
    return y * 4 + z * 2 + core


class Gather:
    def __init__(self, own_ref, blocks, send_sem, recv_sem):
        self.refs = own_ref, blocks, send_sem, recv_sem

    def copy(self, name, arrival):
        own_ref, blocks, send_sem, recv_sem = self.refs
        block, target, half = KINDS[name]
        rows = blocks.shape[1]
        cut = pl.ds(0, rows) if half is None else pl.ds(half * (rows // 2), rows // 2)
        where = blocks.at[seq_at(GOT[name] if arrival else block), cut]
        source = own_ref if block == OWN and not arrival and own_ref is not None else where
        k = ORDER[name]
        return pltpu.make_async_remote_copy(
            src_ref=source,
            dst_ref=where,
            send_sem=send_sem.at[k],
            recv_sem=recv_sem.at[k],
            device_id={"seq": seq_at(target)},
            device_id_type=MESH,
        )

    def start(self, *names):
        for name in names:
            self.copy(name, False).start()

    def arrived(self, *names):
        for name in names:
            self.copy(name, True).wait_recv()

    def finish(self):
        for name in KINDS:
            self.copy(name, False).wait_send()


def seq_peers():
    return [{"seq": seq_at(offset)} for offset in (NEXT, PREV, ACROSS, PARTNER)]


GATHER_SEMAPHORES = [
    pltpu.SemaphoreType.DMA((len(KINDS),)),
    pltpu.SemaphoreType.DMA((len(KINDS),)),
]


def mix_kernel(
    start_ref,
    count_ref,
    visual_ref,
    text_ref,
    gain_ref,
    out_ref,
    square_ref,
    blocks,
    text,
    text_send,
    text_recv,
    own_sem,
    send_sem,
    recv_sem,
):
    me, right, opposite, left = neighbours()
    group = lax.axis_index("group")
    place = lax.axis_index("seq")
    local = text_ref.shape[0]
    sequences, rows, width = text.shape
    part = blocks.shape[1] // sequences
    gather = Gather(visual_ref, blocks, send_sem, recv_sem)

    def columns(peer):
        return text_ref.at[:, :, pl.ds(pl.multiple_of(peer * width, 128), width)]

    own_text = pltpu.make_async_copy(columns(me), text.at[pl.ds(me * local, local)], own_sem)
    own_text.start()
    greet([{"tensoror": peer} for peer in (right, opposite, left)] + seq_peers())
    gather.start("next", "prev", "across", "partner")
    exchanges = []
    for k, peer in ((2, opposite), (1, right), (3, left)):
        exchanges.append(
            pltpu.make_async_remote_copy(
                src_ref=columns(peer),
                dst_ref=text.at[pl.ds(me * local, local)],
                send_sem=text_send.at[k],
                recv_sem=text_recv.at[k],
                device_id={"tensoror": peer},
                device_id_type=MESH,
            )
        )
    for exchange in exchanges:
        exchange.start()
    blocks[place] = visual_ref[...]
    gather.arrived("next")
    gather.start("far0", "twin_next")
    gather.arrived("prev")
    gather.start("far1", "twin_prev")
    gather.arrived("across")
    gather.start("next_across", "prev_across", "twin_across")
    gather.arrived("far0")
    gather.start("far_across0", "twin_far0")
    gather.arrived("far1")
    gather.start("far_across1", "twin_far1")
    gather.arrived("next_across")
    gather.start("twin_next_across")
    gather.arrived("prev_across")
    gather.start("twin_prev_across")
    gather.arrived("far_across0")
    gather.start("twin_far_across0")
    gather.arrived("far_across1")
    gather.start("twin_far_across1")
    gather.arrived("partner", *[name for name in KINDS if name.startswith("twin_")])
    own_text.wait()
    for exchange in exchanges:
        exchange.wait()
    diagonal = lax.broadcasted_iota(jnp.int32, (rows, rows), 0) == lax.broadcasted_iota(
        jnp.int32, (rows, rows), 1
    )

    def one(i):
        start = start_ref[group * sequences + i]
        slots = TILE * count_ref[group * sequences + i]
        visual = blocks[:, pl.ds(pl.multiple_of(i * part, part), part), :].reshape(-1, width)
        total = visual.shape[0]
        shift = place * rows - start
        slot = shift + lax.broadcasted_iota(jnp.int32, (rows, total), 0)
        column = lax.broadcasted_iota(jnp.int32, (rows, total), 1)
        pick = jnp.where((slot == column) & (column < slots), 1.0, 0.0).astype(jnp.bfloat16)
        placed = jnp.dot(pick, visual, preferred_element_type=jnp.float32)
        own = shift + lax.broadcasted_iota(jnp.int32, (rows, width), 0)
        inside = (own >= 0) & (own < slots)
        mixed = jnp.where(inside, placed, text[i].astype(jnp.float32))
        squares = jnp.sum(mixed * mixed, axis=1, keepdims=True)
        square_ref[pl.ds(i, 1), :] = jnp.sum(
            jnp.where(diagonal, squares, 0.0), axis=0, keepdims=True
        )
        out_ref[pl.ds(pl.multiple_of(i * rows, rows), rows), :] = (mixed * gain_ref[...]).astype(
            jnp.bfloat16
        )

    each(0, sequences, one)
    gather.finish()


def mix(starts, counts, visual, text, gain):
    devices = lax.axis_size("seq")
    count = lax.axis_size("tensoror")
    local, rows, full = text.shape
    width = full // count
    sequences = local * count
    smem = pl.BlockSpec(memory_space=pltpu.SMEM)
    vmem = pl.BlockSpec(memory_space=pltpu.VMEM)
    return pl.pallas_call(
        mix_kernel,
        in_specs=[smem, smem, vmem, pl.BlockSpec(memory_space=pl.ANY), vmem],
        out_specs=[vmem, vmem],
        out_shape=[
            jax.ShapeDtypeStruct((sequences * rows, width), jnp.bfloat16),
            jax.ShapeDtypeStruct((sequences, rows), jnp.float32),
        ],
        scratch_shapes=[
            pltpu.VMEM((devices,) + visual.shape, jnp.bfloat16),
            pltpu.VMEM((sequences, rows, width), jnp.bfloat16),
            pltpu.SemaphoreType.DMA((4,)),
            pltpu.SemaphoreType.DMA((4,)),
            pltpu.SemaphoreType.DMA,
        ]
        + GATHER_SEMAPHORES,
        compiler_params=pltpu.CompilerParams(
            collective_id=0, has_side_effects=True, vmem_limit_bytes=VMEM
        ),
    )(starts, counts, visual, text, gain)


def attend_kernel(
    x_ref,
    square_ref,
    wkv_ref,
    wq_ref,
    out_ref,
    kv_weights,
    q_weights,
    squares,
    total_squares,
    scale,
    blocks,
    queries,
    totals,
    kv_weight_sem,
    q_weight_sem,
    square_send,
    square_recv,
    gather_send,
    gather_recv,
    *scratch,
    width,
):
    me, right, opposite, left = neighbours()
    place = lax.axis_index("seq")
    chip = lax.div(place, 2)
    kv_pieces, q_pieces = Pieces(*scratch[:6]), Pieces(*scratch[6:])
    rows = HEAD_SIZE
    local = kv_pieces.rows // rows
    factor = math.log2(math.e) / math.sqrt(HEAD_SIZE)
    gather = Gather(None, blocks, gather_send, gather_recv)

    def weight_copy(source, c, wide, weights, sem):
        column = pl.ds(pl.multiple_of(c * wide, 128), wide)
        return pltpu.make_async_copy(source.at[:, column], weights.at[c], sem.at[c])

    def kv_copy(c):
        return weight_copy(wkv_ref, c, kv_pieces.wide, kv_weights, kv_weight_sem)

    def q_copy(c):
        return weight_copy(wq_ref, c, q_pieces.wide, q_weights, q_weight_sem)

    for c in range(kv_pieces.chunks):
        kv_copy(c).start()
    for c in range(q_pieces.chunks):
        q_copy(c).start()
    greet([{"tensoror": peer} for peer in (right, opposite, left)] + seq_peers())

    def square_copy(k, peer):
        return pltpu.make_async_remote_copy(
            src_ref=square_ref,
            dst_ref=squares.at[k],
            send_sem=square_send.at[k],
            recv_sem=square_recv.at[k],
            device_id={"tensoror": peer},
            device_id_type=MESH,
        )

    peers = ((1, right), (2, opposite), (3, left))
    for k, peer in peers:
        square_copy(k, peer).start()

    def part_of(weights, c):
        def part(k, dest):
            span = pl.ds(pl.multiple_of(dest * local * rows, rows), local * rows)
            return jnp.dot(x_ref[span, :], weights[c], preferred_element_type=jnp.float32)

        return part

    def first_kv(c):
        kv_copy(c).wait()
        kv_pieces.first(c, part_of(kv_weights, c))

    def first_q(c):
        q_copy(c).wait()
        q_pieces.first(c, part_of(q_weights, c))

    each(0, kv_pieces.chunks, first_kv)
    for k, peer in peers:
        square_copy(k, peer).wait()
    total_squares[...] = square_ref[...] + squares[1] + squares[2] + squares[3]
    diagonal = lax.broadcasted_iota(jnp.int32, (rows, rows), 0) == lax.broadcasted_iota(
        jnp.int32, (rows, rows), 1
    )
    for b in range(local):
        row = jnp.broadcast_to(total_squares[pl.ds(me * local + b, 1), :], (rows, rows))
        column = jnp.sum(jnp.where(diagonal, row, 0.0), axis=1, keepdims=True)
        scale[b * rows : (b + 1) * rows, :] = lax.rsqrt(column / width + epsilon)
    each(0, kv_pieces.chunks, kv_pieces.pass_on)
    each(0, 2, first_q)

    def last_kv(c):
        column = pl.ds(pl.multiple_of(c * kv_pieces.wide, 128), kv_pieces.wide)
        for b, sums in enumerate(kv_pieces.last(c)):
            span = slice(b * rows, (b + 1) * rows)
            blocks[place, span, column] = (sums * scale[span, :]).astype(jnp.bfloat16)

    each(0, kv_pieces.chunks, last_kv)
    gather.start("next", "prev", "across", "partner")

    def second_q(c):
        first_q(c)
        q_pieces.pass_on(c - 2)

    each(2, q_pieces.chunks, second_q)
    gather.arrived("next")
    gather.start("far0", "twin_next")
    gather.arrived("prev")
    gather.start("far1", "twin_prev")
    gather.arrived("across")
    gather.start("next_across", "prev_across", "twin_across")
    gather.arrived("far0")
    gather.start("far_across0", "twin_far0")
    gather.arrived("far1")
    gather.start("far_across1", "twin_far1")
    q_pieces.pass_on(2)
    gather.arrived("next_across")
    gather.start("twin_next_across")
    gather.arrived("prev_across")
    gather.start("twin_prev_across")
    gather.arrived("far_across0")
    gather.start("twin_far_across0")
    gather.arrived("far_across1")
    gather.start("twin_far_across1")
    q_pieces.pass_on(3)
    gather.arrived("partner", *[name for name in KINDS if name.startswith("twin_")])

    def absorb(b, h, other, state, masked):
        top, low = state
        span = slice(b * rows, (b + 1) * rows)
        pair = pl.ds(2 * other, 2)
        key_column = pl.multiple_of(h * HEAD_SIZE, 128)
        value_column = pl.multiple_of((h + KEY_VALUE_HEADS) * HEAD_SIZE, 128)
        keys = blocks[pair, span, pl.ds(key_column, HEAD_SIZE)]
        values = blocks[pair, span, pl.ds(value_column, HEAD_SIZE)]
        scores = lax.dot_general(
            keys.reshape(2 * rows, HEAD_SIZE),
            queries[b],
            (((1,), (1,)), ((), ())),
            preferred_element_type=jnp.float32,
        )
        if masked:
            key = lax.broadcasted_iota(jnp.int32, scores.shape, 0)
            query = (
                lax.rem(lax.broadcasted_iota(jnp.int32, scores.shape, 1), rows)
                + lax.rem(place, 2) * rows
            )
            scores = jnp.where(key <= query, scores, masked_score)
        best = jnp.max(scores, axis=0, keepdims=True)
        new = best if masked else jnp.maximum(top, best)
        expo = jnp.exp2((scores - new) * factor)
        summed = jnp.sum(expo, axis=0, keepdims=True)
        added = lax.dot_general(
            values.reshape(2 * rows, HEAD_SIZE),
            expo.astype(jnp.bfloat16),
            (((0,), (0,)), ((), ())),
            preferred_element_type=jnp.float32,
        )
        if masked:
            totals[b] = added
            return new, summed
        keep = jnp.exp2((top - new) * factor)
        totals[b] = totals[b] * keep + added
        return new, low * keep + summed

    def one_group(h):
        for b, sums in enumerate(q_pieces.last(h)):
            scaled = (sums * scale[b * rows : (b + 1) * rows, :]).astype(jnp.bfloat16)
            for j in range(GROUP_HEADS):
                queries[b, j * rows : (j + 1) * rows, :] = scaled[
                    :, j * HEAD_SIZE : (j + 1) * HEAD_SIZE
                ]
        states = tuple(absorb(b, h, chip, (None, None), True) for b in range(local))
        states = lax.fori_loop(
            0,
            chip,
            lambda other, now: tuple(absorb(b, h, other, now[b], False) for b in range(local)),
            states,
        )
        for b in range(local):
            result = totals[b] / states[b][1]
            for j in range(GROUP_HEADS):
                column = pl.multiple_of((h * GROUP_HEADS + j) * HEAD_SIZE, 128)
                out_ref[b * rows : (b + 1) * rows, pl.ds(column, HEAD_SIZE)] = jnp.transpose(
                    result[:, j * rows : (j + 1) * rows]
                ).astype(jnp.bfloat16)

    each(0, KEY_VALUE_HEADS, one_group)
    gather.finish()
    kv_pieces.finish()
    q_pieces.finish()


def attend(mixed, squares, kv_weight, q_weight, full_width):
    count = lax.axis_size("tensoror")
    devices = lax.axis_size("seq")
    total, width = mixed.shape
    rows = total // count
    kv_cols = kv_weight.shape[1]
    q_cols = q_weight.shape[1]
    kv_wide, q_wide = 512, GROUP_HEADS * HEAD_SIZE
    kv_chunks, q_chunks = kv_cols // kv_wide, q_cols // q_wide
    local = rows // HEAD_SIZE
    vmem = pl.BlockSpec(memory_space=pltpu.VMEM)
    hbm = pl.BlockSpec(memory_space=pl.ANY)
    return pl.pallas_call(
        functools.partial(attend_kernel, width=full_width),
        in_specs=[vmem, vmem, hbm, hbm],
        out_specs=vmem,
        out_shape=jax.ShapeDtypeStruct((rows, q_cols), jnp.bfloat16),
        scratch_shapes=[
            pltpu.VMEM((kv_chunks, width, kv_wide), jnp.bfloat16),
            pltpu.VMEM((q_chunks, width, q_wide), jnp.bfloat16),
            pltpu.VMEM((count,) + squares.shape, jnp.float32),
            pltpu.VMEM(squares.shape, jnp.float32),
            pltpu.VMEM((rows, 1), jnp.float32),
            pltpu.VMEM((devices, rows, kv_cols), jnp.bfloat16),
            pltpu.VMEM((local, q_wide, HEAD_SIZE), jnp.bfloat16),
            pltpu.VMEM((local, HEAD_SIZE, q_wide), jnp.float32),
            pltpu.SemaphoreType.DMA((kv_chunks,)),
            pltpu.SemaphoreType.DMA((q_chunks,)),
            pltpu.SemaphoreType.DMA((count,)),
            pltpu.SemaphoreType.DMA((count,)),
        ]
        + GATHER_SEMAPHORES
        + piece_scratch(kv_chunks, rows, kv_wide)
        + piece_scratch(q_chunks, rows, q_wide),
        compiler_params=pltpu.CompilerParams(
            collective_id=2, has_side_effects=True, vmem_limit_bytes=VMEM
        ),
    )(mixed, squares, kv_weight, q_weight)


def shards(
    visual_hidden,
    projector_weight,
    text_embeddings,
    tile_counts,
    image_start,
    norm_gain,
    query_weight,
    keyvalue_weight,
):
    sequence_local, extent_rows, width = text_embeddings.shape
    sequences, slot_rows, depth = visual_hidden.shape
    activated = jax.nn.gelu(visual_hidden.astype(jnp.float32), approximate=False).astype(
        jnp.bfloat16
    )
    visual = project(activated.reshape(sequences * slot_rows, depth), projector_weight)
    gain = lax.dynamic_slice_in_dim(norm_gain, lax.axis_index("tensoror") * depth, depth)
    mixed, squares = mix(image_start, tile_counts, visual, text_embeddings, gain.reshape(1, depth))
    context = attend(mixed, squares, keyvalue_weight, query_weight, width)
    return context.reshape(sequence_local, extent_rows, -1)


def solution(mesh):
    in_specs = (
        P("group", "seq", "tensoror"),
        P("tensoror", None),
        P(("group", "tensoror"), "seq", None),
        P(),
        P(),
        P(),
        P("tensoror", None),
        P("tensoror", None),
    )
    out_specs = P(("group", "tensoror"), "seq", None)
    return jax.shard_map(shards, mesh=mesh, in_specs=in_specs, out_specs=out_specs, check_vma=False)
```

```python
import functools
import math

import jax
import jax.numpy as jnp
from jax import lax
from jax.experimental import pallas as pl
from jax.experimental.pallas import tpu as pltpu
from jax.sharding import PartitionSpec as P

QUERY_HEADS = 20
KEY_VALUE_HEADS = 4
HEAD_SIZE = 128
TILE = 256
GROUP_HEADS = QUERY_HEADS // KEY_VALUE_HEADS
MESH = pl.DeviceIdType.MESH

epsilon = 1e-06
masked_score = -1e30
VMEM = 60 * 1024 * 1024


def neighbours():
    count = lax.axis_size("tensoror")
    me = lax.axis_index("tensoror")
    return me, lax.rem(me + 1, count), lax.rem(me + 2, count), lax.rem(me + 3, count)


def greet(peers):
    barrier = pltpu.get_barrier_semaphore()
    for peer in peers:
        pl.semaphore_signal(
            barrier, inc=1, device_id=peer, device_id_type=MESH
        )
    pl.semaphore_wait(barrier, len(peers))


TO_RIGHT = (False, True, True, False, False, True)


class Pieces:
    def __init__(self, send, recv, keep, own, send_sem, recv_sem):
        self.send, self.recv, self.keep, self.own = send, recv, keep, own
        self.send_sem, self.recv_sem = send_sem, recv_sem
        self.chunks, self.rows, self.wide = own.shape

    def copy(self, kind, c):
        me, right, opposite, left = neighbours()
        return pltpu.make_async_remote_copy(
            src_ref=self.send.at[kind, c],
            dst_ref=self.recv.at[kind, c],
            send_sem=self.send_sem.at[kind, c],
            recv_sem=self.recv_sem.at[kind, c],
            device_id={"tensoror": right if TO_RIGHT[kind] else left},
            device_id_type=MESH,
        )

    def first(self, c, part):
        me, right, opposite, left = neighbours()
        send, keep = self.send, self.keep
        half = self.rows // 2
        sums = part(2, opposite)
        send[0, c] = sums[:half].astype(jnp.bfloat16)
        send[1, c] = sums[half:].astype(jnp.bfloat16)
        self.copy(0, c).start()
        self.copy(1, c).start()
        sums = part(1, right)
        send[2, c] = sums[:half].astype(jnp.bfloat16)
        keep[1, c] = sums[half:]
        self.copy(2, c).start()
        sums = part(3, left)
        send[3, c] = sums[half:].astype(jnp.bfloat16)
        keep[0, c] = sums[:half]
        self.copy(3, c).start()
        self.own[c] = part(0, me)

    def pass_on(self, c):
        for side in (0, 1):
            self.copy(side, c).wait_recv()
            self.send[4 + side, c] = (
                self.keep[side, c] + self.recv[side, c].astype(jnp.float32)
            ).astype(jnp.bfloat16)
            self.copy(4 + side, c).start()

    def last(self, c):
        for kind in (2, 3, 4, 5):
            self.copy(kind, c).wait_recv()
        half = self.rows // 2
        own, recv = self.own, self.recv
        return [
            own[c, side * half : (side + 1) * half]
            + recv[2 + side, c].astype(jnp.float32)
            + recv[4 + side, c].astype(jnp.float32)
            for side in (0, 1)
        ]

    def finish(self):
        def wait(c):
            for kind in range(6):
                self.copy(kind, c).wait_send()

        each(0, self.chunks, wait)


def each(start, stop, body):
    lax.fori_loop(start, stop, lambda c, _: (body(c), 0)[1], 0)


def piece_scratch(chunks, rows, wide):
    return [
        pltpu.VMEM((6, chunks, rows // 2, wide), jnp.bfloat16),
        pltpu.VMEM((6, chunks, rows // 2, wide), jnp.bfloat16),
        pltpu.VMEM((2, chunks, rows // 2, wide), jnp.float32),
        pltpu.VMEM((chunks, rows, wide), jnp.float32),
        pltpu.SemaphoreType.DMA((6, chunks)),
        pltpu.SemaphoreType.DMA((6, chunks)),
    ]


OWN, NEXT, PREV, ACROSS, PARTNER = (0, 0, 0), (1, 0, 0), (3, 0, 0), (0, 1, 0), (0, 0, 1)
FAR = (2, 0, 0)
KINDS = {
    "next": (OWN, PREV, None),
    "prev": (OWN, NEXT, None),
    "across": (OWN, ACROSS, None),
    "partner": (OWN, PARTNER, None),
    "far0": (NEXT, PREV, 0),
    "far1": (PREV, NEXT, 1),
    "next_across": (ACROSS, PREV, None),
    "prev_across": (ACROSS, NEXT, None),
    "far_across0": (FAR, ACROSS, 0),
    "far_across1": (FAR, ACROSS, 1),
}
GOT = {
    "next": NEXT,
    "prev": PREV,
    "across": ACROSS,
    "partner": PARTNER,
    "far0": FAR,
    "far1": FAR,
    "next_across": (1, 1, 0),
    "prev_across": (3, 1, 0),
    "far_across0": (2, 1, 0),
    "far_across1": (2, 1, 0),
}
for name in list(GOT):
    if name != "partner":
        KINDS["twin_" + name] = (GOT[name], PARTNER, KINDS[name][2])
        GOT["twin_" + name] = GOT[name][:2] + (1,)
ORDER = {name: k for k, name in enumerate(KINDS)}


def seq_at(offset):
    place = lax.axis_index("seq")
    y = lax.rem(lax.div(place, 4) + offset[0], 4)
    z = lax.rem(lax.div(place, 2) + offset[1], 2)
    core = lax.rem(place + offset[2], 2)
    return y * 4 + z * 2 + core


class Gather:
    def __init__(self, blocks, send_sem, recv_sem, first=0, last=None):
        self.refs = blocks, send_sem, recv_sem
        self.first, self.size = first, (last or blocks.shape[2]) - first

    def copy(self, name, arrival):
        blocks, send_sem, recv_sem = self.refs
        block, target, half = KINDS[name]
        rows = blocks.shape[1]
        cut = pl.ds(0, rows) if half is None else pl.ds(half * (rows // 2), rows // 2)
        where = blocks.at[
            seq_at(GOT[name] if arrival else block), cut, pl.ds(self.first, self.size)
        ]
        k = ORDER[name]
        return pltpu.make_async_remote_copy(
            src_ref=where,
            dst_ref=where,
            send_sem=send_sem.at[k],
            recv_sem=recv_sem.at[k],
            device_id={"seq": seq_at(target)},
            device_id_type=MESH,
        )

    def start(self, *names):
        for name in names:
            self.copy(name, False).start()

    def arrived(self, *names):
        for name in names:
            self.copy(name, True).wait_recv()

    def finish(self):
        for name in KINDS:
            self.copy(name, False).wait_send()


def seq_peers():
    return [{"seq": seq_at(offset)} for offset in (NEXT, PREV, ACROSS, PARTNER)]


GATHER_SEMAPHORES = [
    pltpu.SemaphoreType.DMA((len(KINDS),)),
    pltpu.SemaphoreType.DMA((len(KINDS),)),
]


SPLIT = 512


def mix_kernel(
    start_ref,
    count_ref,
    hidden_ref,
    w_ref,
    text_ref,
    gain_ref,
    out_ref,
    square_ref,
    act,
    weights,
    blocks,
    text,
    weight_sem,
    text_send,
    text_recv,
    own_sem,
    first_send,
    first_recv,
    second_send,
    second_recv,
    *scratch,
):
    me, right, opposite, left = neighbours()
    group = lax.axis_index("group")
    place = lax.axis_index("seq")
    pieces = Pieces(*scratch)
    chunks, wide = pieces.chunks, pieces.wide
    local = text_ref.shape[0]
    sequences, rows, width = text.shape
    part_rows = blocks.shape[1] // sequences
    early = SPLIT // wide
    spans = ((0, SPLIT), (SPLIT, width))
    gathers = (
        Gather(blocks, first_send, first_recv, *spans[0]),
        Gather(blocks, second_send, second_recv, *spans[1]),
    )

    def load(k, dest, c):
        column = pl.multiple_of(dest * width + c * wide, 128)
        return pltpu.make_async_copy(
            w_ref.at[:, pl.ds(column, wide)], weights.at[k, c], weight_sem.at[k, c]
        )

    for c in range(chunks):
        for k, dest in ((2, opposite), (1, right), (3, left), (0, me)):
            load(k, dest, c).start()
    own_text = pltpu.make_async_copy(
        text_ref.at[:, :, pl.ds(pl.multiple_of(me * width, 128), width)],
        text.at[pl.ds(me * local, local)],
        own_sem,
    )
    own_text.start()
    greet([{"tensoror": peer} for peer in (right, opposite, left)] + seq_peers())

    def exchange(k, peer, b, p):
        first, last = spans[p]
        source = pl.ds(pl.multiple_of(peer * width + first, 128), last - first)
        return pltpu.make_async_remote_copy(
            src_ref=text_ref.at[b, :, source],
            dst_ref=text.at[me * local + b, :, pl.ds(first, last - first)],
            send_sem=text_send.at[k, b, p],
            recv_sem=text_recv.at[k, b, p],
            device_id={"tensoror": peer},
            device_id_type=MESH,
        )

    peers = ((2, opposite), (1, right), (3, left))
    for k, peer in peers:
        exchange(k, peer, 0, 0).start()
    hidden = hidden_ref[...].astype(jnp.float32)
    act[...] = (0.5 * hidden * (1.0 + lax.erf(hidden * math.sqrt(0.5)))).astype(jnp.bfloat16)

    def first(c):
        def part(k, dest):
            load(k, dest, c).wait()
            return jnp.dot(act[...], weights[k, c], preferred_element_type=jnp.float32)

        pieces.first(c, part)

    def last(c):
        column = pl.ds(pl.multiple_of(c * wide, 128), wide)
        half = pieces.rows // 2
        for side, sums in enumerate(pieces.last(c)):
            blocks[place, side * half : (side + 1) * half, column] = sums.astype(jnp.bfloat16)

    def forward_near(gather):
        gather.arrived("next")
        gather.start("far0", "twin_next")
        gather.arrived("prev")
        gather.start("far1", "twin_prev")
        gather.arrived("across")
        gather.start("next_across", "prev_across", "twin_across")

    def forward_far(gather):
        gather.arrived("far0")
        gather.start("far_across0", "twin_far0")
        gather.arrived("far1")
        gather.start("far_across1", "twin_far1")

    def forward_last(gather):
        gather.arrived("next_across")
        gather.start("twin_next_across")
        gather.arrived("prev_across")
        gather.start("twin_prev_across")
        gather.arrived("far_across0")
        gather.start("twin_far_across0")
        gather.arrived("far_across1")
        gather.start("twin_far_across1")

    def all_here(gather):
        gather.arrived("partner", *[name for name in KINDS if name.startswith("twin_")])

    diagonal = lax.broadcasted_iota(jnp.int32, (rows, rows), 0) == lax.broadcasted_iota(
        jnp.int32, (rows, rows), 1
    )

    def mix_columns(p):
        low, high = spans[p]
        gain = gain_ref[:, pl.ds(pl.multiple_of(me * width + low, 128), high - low)]

        def one(i):
            start = start_ref[group * sequences + i]
            slots = TILE * count_ref[group * sequences + i]
            visual = blocks[
                :, pl.ds(pl.multiple_of(i * part_rows, part_rows), part_rows), low:high
            ].reshape(-1, high - low)
            total = visual.shape[0]
            shift = place * rows - start
            slot = shift + lax.broadcasted_iota(jnp.int32, (rows, total), 0)
            column = lax.broadcasted_iota(jnp.int32, (rows, total), 1)
            pick = jnp.where((slot == column) & (column < slots), 1.0, 0.0).astype(jnp.bfloat16)
            placed = jnp.dot(pick, visual, preferred_element_type=jnp.float32)
            own = shift + lax.broadcasted_iota(jnp.int32, placed.shape, 0)
            inside = (own >= 0) & (own < slots)
            mixed = jnp.where(inside, placed, text[i, :, low:high].astype(jnp.float32))
            squares = jnp.sum(mixed * mixed, axis=1, keepdims=True)
            line = jnp.sum(jnp.where(diagonal, squares, 0.0), axis=0, keepdims=True)
            if p == 0:
                square_ref[pl.ds(i, 1), :] = line
            else:
                square_ref[pl.ds(i, 1), :] += line
            out_ref[pl.ds(pl.multiple_of(i * rows, rows), rows), low:high] = (
                mixed * gain
            ).astype(jnp.bfloat16)

        each(0, sequences, one)

    each(0, early, first)
    each(0, early, pieces.pass_on)
    each(early, chunks - 1, first)
    each(0, early, last)
    gathers[0].start("next", "prev", "across", "partner")
    each(chunks - 1, chunks, first)
    each(early, chunks, pieces.pass_on)
    for b, p in ((1, 0), (0, 1), (1, 1)):
        for k, peer in peers:
            exchange(k, peer, b, p).start()
    forward_near(gathers[0])
    each(early, chunks, last)
    gathers[1].start("next", "prev", "across", "partner")
    forward_far(gathers[0])
    forward_last(gathers[0])
    all_here(gathers[0])
    own_text.wait()
    for b in range(local):
        for k, peer in peers:
            exchange(k, peer, b, 0).wait()
    mix_columns(0)
    forward_near(gathers[1])
    forward_far(gathers[1])
    forward_last(gathers[1])
    for b in range(local):
        for k, peer in peers:
            exchange(k, peer, b, 1).wait()
    all_here(gathers[1])
    mix_columns(1)
    for gather in gathers:
        gather.finish()
    pieces.finish()


def mix(starts, counts, hidden, weight, text, gain):
    devices = lax.axis_size("seq")
    count = lax.axis_size("tensoror")
    local, rows, full = text.shape
    width = full // count
    sequences = local * count
    wide = 256
    chunks = width // wide
    smem = pl.BlockSpec(memory_space=pltpu.SMEM)
    vmem = pl.BlockSpec(memory_space=pltpu.VMEM)
    hbm = pl.BlockSpec(memory_space=pl.ANY)
    return pl.pallas_call(
        mix_kernel,
        in_specs=[smem, smem, vmem, hbm, hbm, vmem],
        out_specs=[vmem, vmem],
        out_shape=[
            jax.ShapeDtypeStruct((sequences * rows, width), jnp.bfloat16),
            jax.ShapeDtypeStruct((sequences, rows), jnp.float32),
        ],
        scratch_shapes=[
            pltpu.VMEM(hidden.shape, jnp.bfloat16),
            pltpu.VMEM((count, chunks, width, wide), jnp.bfloat16),
            pltpu.VMEM((devices, hidden.shape[0], width), jnp.bfloat16),
            pltpu.VMEM((sequences, rows, width), jnp.bfloat16),
            pltpu.SemaphoreType.DMA((count, chunks)),
            pltpu.SemaphoreType.DMA((count, local, 2)),
            pltpu.SemaphoreType.DMA((count, local, 2)),
            pltpu.SemaphoreType.DMA,
        ]
        + GATHER_SEMAPHORES
        + GATHER_SEMAPHORES
        + piece_scratch(chunks, hidden.shape[0], wide),
        compiler_params=pltpu.CompilerParams(
            collective_id=0, has_side_effects=True, vmem_limit_bytes=VMEM
        ),
    )(starts, counts, hidden, weight, text, gain)


def attend_kernel(
    x_ref,
    square_ref,
    wkv_ref,
    wq_ref,
    out_ref,
    kv_weights,
    q_weights,
    squares,
    total_squares,
    scale,
    blocks,
    queries,
    totals,
    kv_weight_sem,
    q_weight_sem,
    square_send,
    square_recv,
    gather_send,
    gather_recv,
    *scratch,
    width,
):
    me, right, opposite, left = neighbours()
    place = lax.axis_index("seq")
    chip = lax.div(place, 2)
    kv_pieces, q_pieces = Pieces(*scratch[:6]), Pieces(*scratch[6:])
    rows = HEAD_SIZE
    local = kv_pieces.rows // rows
    factor = math.log2(math.e) / math.sqrt(HEAD_SIZE)
    gather = Gather(blocks, gather_send, gather_recv)

    def weight_copy(source, c, wide, weights, sem):
        column = pl.ds(pl.multiple_of(c * wide, 128), wide)
        return pltpu.make_async_copy(source.at[:, column], weights.at[c], sem.at[c])

    def kv_copy(c):
        return weight_copy(wkv_ref, c, kv_pieces.wide, kv_weights, kv_weight_sem)

    def q_copy(c):
        return weight_copy(wq_ref, c, q_pieces.wide, q_weights, q_weight_sem)

    for c in range(kv_pieces.chunks):
        kv_copy(c).start()
    for c in range(q_pieces.chunks):
        q_copy(c).start()
    greet([{"tensoror": peer} for peer in (right, opposite, left)] + seq_peers())

    def square_copy(k, peer):
        return pltpu.make_async_remote_copy(
            src_ref=square_ref,
            dst_ref=squares.at[k],
            send_sem=square_send.at[k],
            recv_sem=square_recv.at[k],
            device_id={"tensoror": peer},
            device_id_type=MESH,
        )

    peers = ((1, right), (2, opposite), (3, left))
    for k, peer in peers:
        square_copy(k, peer).start()

    def part_of(weights, c):
        def part(k, dest):
            span = pl.ds(pl.multiple_of(dest * local * rows, rows), local * rows)
            return jnp.dot(x_ref[span, :], weights[c], preferred_element_type=jnp.float32)

        return part

    def first_kv(c):
        kv_copy(c).wait()
        kv_pieces.first(c, part_of(kv_weights, c))

    def first_q(c):
        q_copy(c).wait()
        q_pieces.first(c, part_of(q_weights, c))

    each(0, kv_pieces.chunks, first_kv)
    for k, peer in peers:
        square_copy(k, peer).wait()
    total_squares[...] = square_ref[...] + squares[1] + squares[2] + squares[3]
    diagonal = lax.broadcasted_iota(jnp.int32, (rows, rows), 0) == lax.broadcasted_iota(
        jnp.int32, (rows, rows), 1
    )
    for b in range(local):
        row = jnp.broadcast_to(total_squares[pl.ds(me * local + b, 1), :], (rows, rows))
        column = jnp.sum(jnp.where(diagonal, row, 0.0), axis=1, keepdims=True)
        scale[b * rows : (b + 1) * rows, :] = lax.rsqrt(column / width + epsilon)
    each(0, kv_pieces.chunks, kv_pieces.pass_on)
    each(0, 2, first_q)

    def last_kv(c):
        column = pl.ds(pl.multiple_of(c * kv_pieces.wide, 128), kv_pieces.wide)
        for b, sums in enumerate(kv_pieces.last(c)):
            span = slice(b * rows, (b + 1) * rows)
            blocks[place, span, column] = (sums * scale[span, :]).astype(jnp.bfloat16)

    each(0, kv_pieces.chunks, last_kv)
    gather.start("next", "prev", "across", "partner")

    def second_q(c):
        first_q(c)
        q_pieces.pass_on(c - 2)

    each(2, q_pieces.chunks, second_q)
    gather.arrived("next")
    gather.start("far0", "twin_next")
    gather.arrived("prev")
    gather.start("far1", "twin_prev")
    gather.arrived("across")
    gather.start("next_across", "prev_across", "twin_across")
    gather.arrived("far0")
    gather.start("far_across0", "twin_far0")
    gather.arrived("far1")
    gather.start("far_across1", "twin_far1")
    q_pieces.pass_on(2)
    gather.arrived("next_across")
    gather.start("twin_next_across")
    gather.arrived("prev_across")
    gather.start("twin_prev_across")
    gather.arrived("far_across0")
    gather.start("twin_far_across0")
    gather.arrived("far_across1")
    gather.start("twin_far_across1")
    q_pieces.pass_on(3)
    gather.arrived("partner", *[name for name in KINDS if name.startswith("twin_")])

    def absorb(b, h, other, state, masked):
        top, low = state
        span = slice(b * rows, (b + 1) * rows)
        pair = pl.ds(2 * other, 2)
        key_column = pl.multiple_of(h * HEAD_SIZE, 128)
        value_column = pl.multiple_of((h + KEY_VALUE_HEADS) * HEAD_SIZE, 128)
        keys = blocks[pair, span, pl.ds(key_column, HEAD_SIZE)]
        values = blocks[pair, span, pl.ds(value_column, HEAD_SIZE)]
        scores = lax.dot_general(
            keys.reshape(2 * rows, HEAD_SIZE),
            queries[b],
            (((1,), (1,)), ((), ())),
            preferred_element_type=jnp.float32,
        )
        if masked:
            key = lax.broadcasted_iota(jnp.int32, scores.shape, 0)
            query = (
                lax.rem(lax.broadcasted_iota(jnp.int32, scores.shape, 1), rows)
                + lax.rem(place, 2) * rows
            )
            scores = jnp.where(key <= query, scores, masked_score)
        best = jnp.max(scores, axis=0, keepdims=True)
        new = best if masked else jnp.maximum(top, best)
        expo = jnp.exp2((scores - new) * factor)
        summed = jnp.sum(expo, axis=0, keepdims=True)
        added = lax.dot_general(
            values.reshape(2 * rows, HEAD_SIZE),
            expo.astype(jnp.bfloat16),
            (((0,), (0,)), ((), ())),
            preferred_element_type=jnp.float32,
        )
        if masked:
            totals[b] = added
            return new, summed
        keep = jnp.exp2((top - new) * factor)
        totals[b] = totals[b] * keep + added
        return new, low * keep + summed

    def one_group(h):
        for b, sums in enumerate(q_pieces.last(h)):
            scaled = (sums * scale[b * rows : (b + 1) * rows, :]).astype(jnp.bfloat16)
            for j in range(GROUP_HEADS):
                queries[b, j * rows : (j + 1) * rows, :] = scaled[
                    :, j * HEAD_SIZE : (j + 1) * HEAD_SIZE
                ]
        states = tuple(absorb(b, h, chip, (None, None), True) for b in range(local))
        states = lax.fori_loop(
            0,
            chip,
            lambda other, now: tuple(absorb(b, h, other, now[b], False) for b in range(local)),
            states,
        )
        for b in range(local):
            result = totals[b] / states[b][1]
            for j in range(GROUP_HEADS):
                column = pl.multiple_of((h * GROUP_HEADS + j) * HEAD_SIZE, 128)
                out_ref[b * rows : (b + 1) * rows, pl.ds(column, HEAD_SIZE)] = jnp.transpose(
                    result[:, j * rows : (j + 1) * rows]
                ).astype(jnp.bfloat16)

    each(0, KEY_VALUE_HEADS, one_group)
    gather.finish()
    kv_pieces.finish()
    q_pieces.finish()


def attend(mixed, squares, kv_weight, q_weight, full_width):
    count = lax.axis_size("tensoror")
    devices = lax.axis_size("seq")
    total, width = mixed.shape
    rows = total // count
    kv_cols = kv_weight.shape[1]
    q_cols = q_weight.shape[1]
    kv_wide, q_wide = 512, GROUP_HEADS * HEAD_SIZE
    kv_chunks, q_chunks = kv_cols // kv_wide, q_cols // q_wide
    local = rows // HEAD_SIZE
    vmem = pl.BlockSpec(memory_space=pltpu.VMEM)
    hbm = pl.BlockSpec(memory_space=pl.ANY)
    return pl.pallas_call(
        functools.partial(attend_kernel, width=full_width),
        in_specs=[vmem, vmem, hbm, hbm],
        out_specs=vmem,
        out_shape=jax.ShapeDtypeStruct((rows, q_cols), jnp.bfloat16),
        scratch_shapes=[
            pltpu.VMEM((kv_chunks, width, kv_wide), jnp.bfloat16),
            pltpu.VMEM((q_chunks, width, q_wide), jnp.bfloat16),
            pltpu.VMEM((count,) + squares.shape, jnp.float32),
            pltpu.VMEM(squares.shape, jnp.float32),
            pltpu.VMEM((rows, 1), jnp.float32),
            pltpu.VMEM((devices, rows, kv_cols), jnp.bfloat16),
            pltpu.VMEM((local, q_wide, HEAD_SIZE), jnp.bfloat16),
            pltpu.VMEM((local, HEAD_SIZE, q_wide), jnp.float32),
            pltpu.SemaphoreType.DMA((kv_chunks,)),
            pltpu.SemaphoreType.DMA((q_chunks,)),
            pltpu.SemaphoreType.DMA((count,)),
            pltpu.SemaphoreType.DMA((count,)),
        ]
        + GATHER_SEMAPHORES
        + piece_scratch(kv_chunks, rows, kv_wide)
        + piece_scratch(q_chunks, rows, q_wide),
        compiler_params=pltpu.CompilerParams(
            collective_id=2, has_side_effects=True, vmem_limit_bytes=VMEM
        ),
    )(mixed, squares, kv_weight, q_weight)


def shards(
    visual_hidden,
    projector_weight,
    text_embeddings,
    tile_counts,
    image_start,
    norm_gain,
    query_weight,
    keyvalue_weight,
):
    sequence_local, extent_rows, width = text_embeddings.shape
    sequences, slot_rows, depth = visual_hidden.shape
    mixed, squares = mix(
        image_start,
        tile_counts,
        visual_hidden.reshape(sequences * slot_rows, depth),
        projector_weight,
        text_embeddings,
        norm_gain.reshape(1, width),
    )
    context = attend(mixed, squares, keyvalue_weight, query_weight, width)
    return context.reshape(sequence_local, extent_rows, -1)


def solution(mesh):
    in_specs = (
        P("group", "seq", "tensoror"),
        P("tensoror", None),
        P(("group", "tensoror"), "seq", None),
        P(),
        P(),
        P(),
        P("tensoror", None),
        P("tensoror", None),
    )
    out_specs = P(("group", "tensoror"), "seq", None)
    return jax.shard_map(shards, mesh=mesh, in_specs=in_specs, out_specs=out_specs, check_vma=False)
```

```python
import functools
import math

import jax
import jax.numpy as jnp
from jax import lax
from jax.experimental import pallas as pl
from jax.experimental.pallas import tpu as pltpu
from jax.sharding import PartitionSpec as P

QUERY_HEADS = 20
KEY_VALUE_HEADS = 4
HEAD_SIZE = 128
TILE = 256
GROUP_HEADS = QUERY_HEADS // KEY_VALUE_HEADS
MESH = pl.DeviceIdType.MESH

epsilon = 1e-06
masked_score = -1e30
VMEM = 60 * 1024 * 1024


def neighbours():
    count = lax.axis_size("tensoror")
    me = lax.axis_index("tensoror")
    return me, lax.rem(me + 1, count), lax.rem(me + 2, count), lax.rem(me + 3, count)


def greet(peers):
    barrier = pltpu.get_barrier_semaphore()
    for peer in peers:
        pl.semaphore_signal(
            barrier, inc=1, device_id=peer, device_id_type=MESH
        )
    pl.semaphore_wait(barrier, len(peers))


TO_RIGHT = (False, True, True, False, False, True)


class Pieces:
    def __init__(self, send, recv, keep, own, send_sem, recv_sem):
        self.send, self.recv, self.keep, self.own = send, recv, keep, own
        self.send_sem, self.recv_sem = send_sem, recv_sem
        self.chunks, self.rows, self.wide = own.shape

    def copy(self, kind, c):
        me, right, opposite, left = neighbours()
        return pltpu.make_async_remote_copy(
            src_ref=self.send.at[kind, c],
            dst_ref=self.recv.at[kind, c],
            send_sem=self.send_sem.at[kind, c],
            recv_sem=self.recv_sem.at[kind, c],
            device_id={"tensoror": right if TO_RIGHT[kind] else left},
            device_id_type=MESH,
        )

    def first(self, c, part):
        me, right, opposite, left = neighbours()
        send, keep = self.send, self.keep
        half = self.rows // 2
        sums = part(2, opposite)
        send[0, c] = sums[:half].astype(jnp.bfloat16)
        send[1, c] = sums[half:].astype(jnp.bfloat16)
        self.copy(0, c).start()
        self.copy(1, c).start()
        sums = part(1, right)
        send[2, c] = sums[:half].astype(jnp.bfloat16)
        keep[1, c] = sums[half:]
        self.copy(2, c).start()
        sums = part(3, left)
        send[3, c] = sums[half:].astype(jnp.bfloat16)
        keep[0, c] = sums[:half]
        self.copy(3, c).start()
        self.own[c] = part(0, me)

    def pass_on(self, c):
        for side in (0, 1):
            self.copy(side, c).wait_recv()
            self.send[4 + side, c] = (
                self.keep[side, c] + self.recv[side, c].astype(jnp.float32)
            ).astype(jnp.bfloat16)
            self.copy(4 + side, c).start()

    def last(self, c):
        for kind in (2, 3, 4, 5):
            self.copy(kind, c).wait_recv()
        half = self.rows // 2
        own, recv = self.own, self.recv
        return [
            own[c, side * half : (side + 1) * half]
            + recv[2 + side, c].astype(jnp.float32)
            + recv[4 + side, c].astype(jnp.float32)
            for side in (0, 1)
        ]

    def finish(self):
        def wait(c):
            for kind in range(6):
                self.copy(kind, c).wait_send()

        each(0, self.chunks, wait)


def each(start, stop, body):
    lax.fori_loop(start, stop, lambda c, _: (body(c), 0)[1], 0)


def piece_scratch(chunks, rows, wide):
    return [
        pltpu.VMEM((6, chunks, rows // 2, wide), jnp.bfloat16),
        pltpu.VMEM((6, chunks, rows // 2, wide), jnp.bfloat16),
        pltpu.VMEM((2, chunks, rows // 2, wide), jnp.float32),
        pltpu.VMEM((chunks, rows, wide), jnp.float32),
        pltpu.SemaphoreType.DMA((6, chunks)),
        pltpu.SemaphoreType.DMA((6, chunks)),
    ]


OWN, NEXT, PREV, ACROSS, PARTNER = (0, 0, 0), (1, 0, 0), (3, 0, 0), (0, 1, 0), (0, 0, 1)
FAR = (2, 0, 0)
KINDS = {
    "next": (OWN, PREV, None),
    "prev": (OWN, NEXT, None),
    "across": (OWN, ACROSS, None),
    "partner": (OWN, PARTNER, None),
    "far0": (NEXT, PREV, 0),
    "far1": (PREV, NEXT, 1),
    "next_across": (ACROSS, PREV, None),
    "prev_across": (ACROSS, NEXT, None),
    "far_across0": (FAR, ACROSS, 0),
    "far_across1": (FAR, ACROSS, 1),
}
GOT = {
    "next": NEXT,
    "prev": PREV,
    "across": ACROSS,
    "partner": PARTNER,
    "far0": FAR,
    "far1": FAR,
    "next_across": (1, 1, 0),
    "prev_across": (3, 1, 0),
    "far_across0": (2, 1, 0),
    "far_across1": (2, 1, 0),
}
for name in list(GOT):
    if name != "partner":
        KINDS["twin_" + name] = (GOT[name], PARTNER, KINDS[name][2])
        GOT["twin_" + name] = GOT[name][:2] + (1,)
ORDER = {name: k for k, name in enumerate(KINDS)}


def seq_at(offset):
    place = lax.axis_index("seq")
    y = lax.rem(lax.div(place, 4) + offset[0], 4)
    z = lax.rem(lax.div(place, 2) + offset[1], 2)
    core = lax.rem(place + offset[2], 2)
    return y * 4 + z * 2 + core


class Gather:
    def __init__(self, blocks, send_sem, recv_sem, first=0, last=None):
        self.refs = blocks, send_sem, recv_sem
        self.first, self.size = first, (last or blocks.shape[2]) - first

    def copy(self, name, arrival):
        blocks, send_sem, recv_sem = self.refs
        block, target, half = KINDS[name]
        rows = blocks.shape[1]
        cut = pl.ds(0, rows) if half is None else pl.ds(half * (rows // 2), rows // 2)
        where = blocks.at[
            seq_at(GOT[name] if arrival else block), cut, pl.ds(self.first, self.size)
        ]
        k = ORDER[name]
        return pltpu.make_async_remote_copy(
            src_ref=where,
            dst_ref=where,
            send_sem=send_sem.at[k],
            recv_sem=recv_sem.at[k],
            device_id={"seq": seq_at(target)},
            device_id_type=MESH,
        )

    def start(self, *names):
        for name in names:
            self.copy(name, False).start()

    def arrived(self, *names):
        for name in names:
            self.copy(name, True).wait_recv()

    def finish(self):
        for name in KINDS:
            self.copy(name, False).wait_send()


def seq_peers():
    return [{"seq": seq_at(offset)} for offset in (NEXT, PREV, ACROSS, PARTNER)]


GATHER_SEMAPHORES = [
    pltpu.SemaphoreType.DMA((len(KINDS),)),
    pltpu.SemaphoreType.DMA((len(KINDS),)),
]


PASSES = (0, 1, 3, 5)


def mix_kernel(
    start_ref,
    count_ref,
    hidden_ref,
    w_ref,
    text_ref,
    gain_ref,
    out_ref,
    square_ref,
    act,
    weights,
    blocks,
    text,
    weight_sem,
    text_send,
    text_recv,
    own_sem,
    gather_send,
    gather_recv,
    *scratch,
):
    me, right, opposite, left = neighbours()
    group = lax.axis_index("group")
    place = lax.axis_index("seq")
    pieces = Pieces(*scratch)
    chunks, wide = pieces.chunks, pieces.wide
    local = text_ref.shape[0]
    sequences, rows, width = text.shape
    part_rows = blocks.shape[1] // sequences
    spans = [(a * wide, b * wide) for a, b in zip(PASSES, PASSES[1:])]
    gathers = [
        Gather(blocks, gather_send.at[p], gather_recv.at[p], *span)
        for p, span in enumerate(spans)
    ]

    def load(k, dest, c):
        column = pl.multiple_of(dest * width + c * wide, 128)
        return pltpu.make_async_copy(
            w_ref.at[:, pl.ds(column, wide)], weights.at[k, c], weight_sem.at[k, c]
        )

    for c in range(chunks):
        for k, dest in ((2, opposite), (1, right), (3, left), (0, me)):
            load(k, dest, c).start()
    own_text = pltpu.make_async_copy(
        text_ref.at[:, :, pl.ds(pl.multiple_of(me * width, 128), width)],
        text.at[pl.ds(me * local, local)],
        own_sem,
    )
    own_text.start()
    greet([{"tensoror": peer} for peer in (right, opposite, left)] + seq_peers())

    def exchange(k, peer, b, p):
        first, last = spans[p]
        source = pl.ds(pl.multiple_of(peer * width + first, 128), last - first)
        return pltpu.make_async_remote_copy(
            src_ref=text_ref.at[b, :, source],
            dst_ref=text.at[me * local + b, :, pl.ds(first, last - first)],
            send_sem=text_send.at[k, b, p],
            recv_sem=text_recv.at[k, b, p],
            device_id={"tensoror": peer},
            device_id_type=MESH,
        )

    peers = ((2, opposite), (1, right), (3, left))
    for k, peer in peers:
        exchange(k, peer, 0, 0).start()
    hidden = hidden_ref[...].astype(jnp.float32)
    act[...] = (0.5 * hidden * (1.0 + lax.erf(hidden * math.sqrt(0.5)))).astype(jnp.bfloat16)

    def first(c):
        def part(k, dest):
            load(k, dest, c).wait()
            return jnp.dot(act[...], weights[k, c], preferred_element_type=jnp.float32)

        pieces.first(c, part)

    def last(c):
        column = pl.ds(pl.multiple_of(c * wide, 128), wide)
        half = pieces.rows // 2
        for side, sums in enumerate(pieces.last(c)):
            blocks[place, side * half : (side + 1) * half, column] = sums.astype(jnp.bfloat16)

    def forward_near(gather):
        gather.arrived("next")
        gather.start("far0", "twin_next")
        gather.arrived("prev")
        gather.start("far1", "twin_prev")
        gather.arrived("across")
        gather.start("next_across", "prev_across", "twin_across")

    def forward_far(gather):
        gather.arrived("far0")
        gather.start("far_across0", "twin_far0")
        gather.arrived("far1")
        gather.start("far_across1", "twin_far1")

    def forward_last(gather):
        gather.arrived("next_across")
        gather.start("twin_next_across")
        gather.arrived("prev_across")
        gather.start("twin_prev_across")
        gather.arrived("far_across0")
        gather.start("twin_far_across0")
        gather.arrived("far_across1")
        gather.start("twin_far_across1")

    def all_here(gather):
        gather.arrived("partner", *[name for name in KINDS if name.startswith("twin_")])

    diagonal = lax.broadcasted_iota(jnp.int32, (rows, rows), 0) == lax.broadcasted_iota(
        jnp.int32, (rows, rows), 1
    )

    def mix_columns(p):
        low, high = spans[p]
        gain = gain_ref[:, pl.ds(pl.multiple_of(me * width + low, 128), high - low)]

        def one(i):
            start = start_ref[group * sequences + i]
            slots = TILE * count_ref[group * sequences + i]
            visual = blocks[
                :, pl.ds(pl.multiple_of(i * part_rows, part_rows), part_rows), low:high
            ].reshape(-1, high - low)
            total = visual.shape[0]
            shift = place * rows - start
            slot = shift + lax.broadcasted_iota(jnp.int32, (rows, total), 0)
            column = lax.broadcasted_iota(jnp.int32, (rows, total), 1)
            pick = jnp.where((slot == column) & (column < slots), 1.0, 0.0).astype(jnp.bfloat16)
            placed = jnp.dot(pick, visual, preferred_element_type=jnp.float32)
            own = shift + lax.broadcasted_iota(jnp.int32, placed.shape, 0)
            inside = (own >= 0) & (own < slots)
            mixed = jnp.where(inside, placed, text[i, :, low:high].astype(jnp.float32))
            squares = jnp.sum(mixed * mixed, axis=1, keepdims=True)
            line = jnp.sum(jnp.where(diagonal, squares, 0.0), axis=0, keepdims=True)
            if p == 0:
                square_ref[pl.ds(i, 1), :] = line
            else:
                square_ref[pl.ds(i, 1), :] += line
            out_ref[pl.ds(pl.multiple_of(i * rows, rows), rows), low:high] = (
                mixed * gain
            ).astype(jnp.bfloat16)

        each(0, sequences, one)

    def own_start(p):
        each(PASSES[p], PASSES[p + 1], last)
        gathers[p].start("next", "prev", "across", "partner")

    def text_here(p):
        for b in range(local):
            for k, peer in peers:
                exchange(k, peer, b, p).wait()

    each(0, 1, first)
    each(1, 2, first)
    each(0, 1, pieces.pass_on)
    each(2, 3, first)
    each(1, 2, pieces.pass_on)
    own_start(0)
    each(3, 4, first)
    each(2, 3, pieces.pass_on)
    each(4, 5, first)
    each(3, 4, pieces.pass_on)
    forward_near(gathers[0])
    own_start(1)
    each(4, 5, pieces.pass_on)
    for b, p in ((1, 0), (0, 1), (1, 1), (0, 2), (1, 2)):
        for k, peer in peers:
            exchange(k, peer, b, p).start()
    forward_far(gathers[0])
    forward_last(gathers[0])
    forward_near(gathers[1])
    own_start(2)
    own_text.wait()
    all_here(gathers[0])
    forward_far(gathers[1])
    text_here(0)
    mix_columns(0)
    forward_last(gathers[1])
    forward_near(gathers[2])
    all_here(gathers[1])
    forward_far(gathers[2])
    text_here(1)
    mix_columns(1)
    forward_last(gathers[2])
    text_here(2)
    all_here(gathers[2])
    mix_columns(2)
    for gather in gathers:
        gather.finish()
    pieces.finish()


def mix(starts, counts, hidden, weight, text, gain):
    devices = lax.axis_size("seq")
    count = lax.axis_size("tensoror")
    local, rows, full = text.shape
    width = full // count
    sequences = local * count
    wide = 256
    chunks = width // wide
    smem = pl.BlockSpec(memory_space=pltpu.SMEM)
    vmem = pl.BlockSpec(memory_space=pltpu.VMEM)
    hbm = pl.BlockSpec(memory_space=pl.ANY)
    return pl.pallas_call(
        mix_kernel,
        in_specs=[smem, smem, vmem, hbm, hbm, vmem],
        out_specs=[vmem, vmem],
        out_shape=[
            jax.ShapeDtypeStruct((sequences * rows, width), jnp.bfloat16),
            jax.ShapeDtypeStruct((sequences, rows), jnp.float32),
        ],
        scratch_shapes=[
            pltpu.VMEM(hidden.shape, jnp.bfloat16),
            pltpu.VMEM((count, chunks, width, wide), jnp.bfloat16),
            pltpu.VMEM((devices, hidden.shape[0], width), jnp.bfloat16),
            pltpu.VMEM((sequences, rows, width), jnp.bfloat16),
            pltpu.SemaphoreType.DMA((count, chunks)),
            pltpu.SemaphoreType.DMA((count, local, len(PASSES) - 1)),
            pltpu.SemaphoreType.DMA((count, local, len(PASSES) - 1)),
            pltpu.SemaphoreType.DMA,
            pltpu.SemaphoreType.DMA((len(PASSES) - 1, len(KINDS))),
            pltpu.SemaphoreType.DMA((len(PASSES) - 1, len(KINDS))),
        ]
        + piece_scratch(chunks, hidden.shape[0], wide),
        compiler_params=pltpu.CompilerParams(
            collective_id=0, has_side_effects=True, vmem_limit_bytes=VMEM
        ),
    )(starts, counts, hidden, weight, text, gain)


def attend_kernel(
    x_ref,
    square_ref,
    wkv_ref,
    wq_ref,
    out_ref,
    kv_weights,
    q_weights,
    squares,
    total_squares,
    scale,
    blocks,
    queries,
    totals,
    kv_weight_sem,
    q_weight_sem,
    square_send,
    square_recv,
    gather_send,
    gather_recv,
    *scratch,
    width,
):
    me, right, opposite, left = neighbours()
    place = lax.axis_index("seq")
    chip = lax.div(place, 2)
    kv_pieces, q_pieces = Pieces(*scratch[:6]), Pieces(*scratch[6:])
    rows = HEAD_SIZE
    local = kv_pieces.rows // rows
    factor = math.log2(math.e) / math.sqrt(HEAD_SIZE)
    gather = Gather(blocks, gather_send, gather_recv)

    def weight_copy(source, c, wide, weights, sem):
        column = pl.ds(pl.multiple_of(c * wide, 128), wide)
        return pltpu.make_async_copy(source.at[:, column], weights.at[c], sem.at[c])

    def kv_copy(c):
        return weight_copy(wkv_ref, c, kv_pieces.wide, kv_weights, kv_weight_sem)

    def q_copy(c):
        return weight_copy(wq_ref, c, q_pieces.wide, q_weights, q_weight_sem)

    for c in range(kv_pieces.chunks):
        kv_copy(c).start()
    for c in range(q_pieces.chunks):
        q_copy(c).start()
    greet([{"tensoror": peer} for peer in (right, opposite, left)] + seq_peers())

    def square_copy(k, peer):
        return pltpu.make_async_remote_copy(
            src_ref=square_ref,
            dst_ref=squares.at[k],
            send_sem=square_send.at[k],
            recv_sem=square_recv.at[k],
            device_id={"tensoror": peer},
            device_id_type=MESH,
        )

    peers = ((1, right), (2, opposite), (3, left))
    for k, peer in peers:
        square_copy(k, peer).start()

    def part_of(weights, c):
        def part(k, dest):
            span = pl.ds(pl.multiple_of(dest * local * rows, rows), local * rows)
            return jnp.dot(x_ref[span, :], weights[c], preferred_element_type=jnp.float32)

        return part

    def first_kv(c):
        kv_copy(c).wait()
        kv_pieces.first(c, part_of(kv_weights, c))

    def first_q(c):
        q_copy(c).wait()
        q_pieces.first(c, part_of(q_weights, c))

    each(0, kv_pieces.chunks, first_kv)
    for k, peer in peers:
        square_copy(k, peer).wait()
    total_squares[...] = square_ref[...] + squares[1] + squares[2] + squares[3]
    diagonal = lax.broadcasted_iota(jnp.int32, (rows, rows), 0) == lax.broadcasted_iota(
        jnp.int32, (rows, rows), 1
    )
    for b in range(local):
        row = jnp.broadcast_to(total_squares[pl.ds(me * local + b, 1), :], (rows, rows))
        column = jnp.sum(jnp.where(diagonal, row, 0.0), axis=1, keepdims=True)
        scale[b * rows : (b + 1) * rows, :] = lax.rsqrt(column / width + epsilon)
    each(0, kv_pieces.chunks, kv_pieces.pass_on)
    each(0, 2, first_q)

    def last_kv(c):
        column = pl.ds(pl.multiple_of(c * kv_pieces.wide, 128), kv_pieces.wide)
        for b, sums in enumerate(kv_pieces.last(c)):
            span = slice(b * rows, (b + 1) * rows)
            blocks[place, span, column] = (sums * scale[span, :]).astype(jnp.bfloat16)

    each(0, kv_pieces.chunks, last_kv)
    gather.start("next", "prev", "across", "partner")

    def second_q(c):
        first_q(c)
        q_pieces.pass_on(c - 2)

    each(2, q_pieces.chunks, second_q)
    gather.arrived("next")
    gather.start("far0", "twin_next")
    gather.arrived("prev")
    gather.start("far1", "twin_prev")
    gather.arrived("across")
    gather.start("next_across", "prev_across", "twin_across")
    gather.arrived("far0")
    gather.start("far_across0", "twin_far0")
    gather.arrived("far1")
    gather.start("far_across1", "twin_far1")
    q_pieces.pass_on(2)
    gather.arrived("next_across")
    gather.start("twin_next_across")
    gather.arrived("prev_across")
    gather.start("twin_prev_across")
    gather.arrived("far_across0")
    gather.start("twin_far_across0")
    gather.arrived("far_across1")
    gather.start("twin_far_across1")
    gather.arrived("partner", *[name for name in KINDS if name.startswith("twin_")])

    def absorb(b, h, other, state, masked):
        top, low = state
        span = slice(b * rows, (b + 1) * rows)
        pair = pl.ds(2 * other, 2)
        key_column = pl.multiple_of(h * HEAD_SIZE, 128)
        value_column = pl.multiple_of((h + KEY_VALUE_HEADS) * HEAD_SIZE, 128)
        keys = blocks[pair, span, pl.ds(key_column, HEAD_SIZE)]
        values = blocks[pair, span, pl.ds(value_column, HEAD_SIZE)]
        scores = lax.dot_general(
            keys.reshape(2 * rows, HEAD_SIZE),
            queries[b],
            (((1,), (1,)), ((), ())),
            preferred_element_type=jnp.float32,
        )
        if masked:
            key = lax.broadcasted_iota(jnp.int32, scores.shape, 0)
            query = (
                lax.rem(lax.broadcasted_iota(jnp.int32, scores.shape, 1), rows)
                + lax.rem(place, 2) * rows
            )
            scores = jnp.where(key <= query, scores, masked_score)
        best = jnp.max(scores, axis=0, keepdims=True)
        new = best if masked else jnp.maximum(top, best)
        expo = jnp.exp2((scores - new) * factor)
        summed = jnp.sum(expo, axis=0, keepdims=True)
        added = lax.dot_general(
            values.reshape(2 * rows, HEAD_SIZE),
            expo.astype(jnp.bfloat16),
            (((0,), (0,)), ((), ())),
            preferred_element_type=jnp.float32,
        )
        if masked:
            totals[b] = added
            return new, summed
        keep = jnp.exp2((top - new) * factor)
        totals[b] = totals[b] * keep + added
        return new, low * keep + summed

    def one_group(h):
        for b, sums in enumerate(q_pieces.last(h)):
            scaled = (sums * scale[b * rows : (b + 1) * rows, :]).astype(jnp.bfloat16)
            for j in range(GROUP_HEADS):
                queries[b, j * rows : (j + 1) * rows, :] = scaled[
                    :, j * HEAD_SIZE : (j + 1) * HEAD_SIZE
                ]
        states = tuple(absorb(b, h, chip, (None, None), True) for b in range(local))
        states = lax.fori_loop(
            0,
            chip,
            lambda other, now: tuple(absorb(b, h, other, now[b], False) for b in range(local)),
            states,
        )
        for b in range(local):
            result = totals[b] / states[b][1]
            for j in range(GROUP_HEADS):
                column = pl.multiple_of((h * GROUP_HEADS + j) * HEAD_SIZE, 128)
                out_ref[b * rows : (b + 1) * rows, pl.ds(column, HEAD_SIZE)] = jnp.transpose(
                    result[:, j * rows : (j + 1) * rows]
                ).astype(jnp.bfloat16)

    each(0, 1, one_group)
    q_pieces.pass_on(3)
    each(1, KEY_VALUE_HEADS, one_group)
    gather.finish()
    kv_pieces.finish()
    q_pieces.finish()


def attend(mixed, squares, kv_weight, q_weight, full_width):
    count = lax.axis_size("tensoror")
    devices = lax.axis_size("seq")
    total, width = mixed.shape
    rows = total // count
    kv_cols = kv_weight.shape[1]
    q_cols = q_weight.shape[1]
    kv_wide, q_wide = 512, GROUP_HEADS * HEAD_SIZE
    kv_chunks, q_chunks = kv_cols // kv_wide, q_cols // q_wide
    local = rows // HEAD_SIZE
    vmem = pl.BlockSpec(memory_space=pltpu.VMEM)
    hbm = pl.BlockSpec(memory_space=pl.ANY)
    return pl.pallas_call(
        functools.partial(attend_kernel, width=full_width),
        in_specs=[vmem, vmem, hbm, hbm],
        out_specs=vmem,
        out_shape=jax.ShapeDtypeStruct((rows, q_cols), jnp.bfloat16),
        scratch_shapes=[
            pltpu.VMEM((kv_chunks, width, kv_wide), jnp.bfloat16),
            pltpu.VMEM((q_chunks, width, q_wide), jnp.bfloat16),
            pltpu.VMEM((count,) + squares.shape, jnp.float32),
            pltpu.VMEM(squares.shape, jnp.float32),
            pltpu.VMEM((rows, 1), jnp.float32),
            pltpu.VMEM((devices, rows, kv_cols), jnp.bfloat16),
            pltpu.VMEM((local, q_wide, HEAD_SIZE), jnp.bfloat16),
            pltpu.VMEM((local, HEAD_SIZE, q_wide), jnp.float32),
            pltpu.SemaphoreType.DMA((kv_chunks,)),
            pltpu.SemaphoreType.DMA((q_chunks,)),
            pltpu.SemaphoreType.DMA((count,)),
            pltpu.SemaphoreType.DMA((count,)),
        ]
        + GATHER_SEMAPHORES
        + piece_scratch(kv_chunks, rows, kv_wide)
        + piece_scratch(q_chunks, rows, q_wide),
        compiler_params=pltpu.CompilerParams(
            collective_id=2, has_side_effects=True, vmem_limit_bytes=VMEM
        ),
    )(mixed, squares, kv_weight, q_weight)


def shards(
    visual_hidden,
    projector_weight,
    text_embeddings,
    tile_counts,
    image_start,
    norm_gain,
    query_weight,
    keyvalue_weight,
):
    sequence_local, extent_rows, width = text_embeddings.shape
    sequences, slot_rows, depth = visual_hidden.shape
    mixed, squares = mix(
        image_start,
        tile_counts,
        visual_hidden.reshape(sequences * slot_rows, depth),
        projector_weight,
        text_embeddings,
        norm_gain.reshape(1, width),
    )
    context = attend(mixed, squares, keyvalue_weight, query_weight, width)
    return context.reshape(sequence_local, extent_rows, -1)


def solution(mesh):
    in_specs = (
        P("group", "seq", "tensoror"),
        P("tensoror", None),
        P(("group", "tensoror"), "seq", None),
        P(),
        P(),
        P(),
        P("tensoror", None),
        P("tensoror", None),
    )
    out_specs = P(("group", "tensoror"), "seq", None)
    return jax.shard_map(shards, mesh=mesh, in_specs=in_specs, out_specs=out_specs, check_vma=False)
```

```python
import functools
import math

import jax
import jax.numpy as jnp
from jax import lax
from jax.experimental import pallas as pl
from jax.experimental.pallas import tpu as pltpu
from jax.sharding import PartitionSpec as P

QUERY_HEADS = 20
KEY_VALUE_HEADS = 4
HEAD_SIZE = 128
TILE = 256
GROUP_HEADS = QUERY_HEADS // KEY_VALUE_HEADS
MESH = pl.DeviceIdType.MESH

epsilon = 1e-06
masked_score = -1e30
VMEM = 60 * 1024 * 1024


def neighbours():
    count = lax.axis_size("tensoror")
    me = lax.axis_index("tensoror")
    return me, lax.rem(me + 1, count), lax.rem(me + 2, count), lax.rem(me + 3, count)


def greet(peers):
    barrier = pltpu.get_barrier_semaphore()
    for peer in peers:
        pl.semaphore_signal(
            barrier, inc=1, device_id=peer, device_id_type=MESH
        )
    pl.semaphore_wait(barrier, len(peers))


TO_RIGHT = (False, True, True, False, False, True)


class Pieces:
    def __init__(self, send, recv, keep, own, send_sem, recv_sem):
        self.send, self.recv, self.keep, self.own = send, recv, keep, own
        self.send_sem, self.recv_sem = send_sem, recv_sem
        self.chunks, self.rows, self.wide = own.shape

    def copy(self, kind, c):
        me, right, opposite, left = neighbours()
        return pltpu.make_async_remote_copy(
            src_ref=self.send.at[kind, c],
            dst_ref=self.recv.at[kind, c],
            send_sem=self.send_sem.at[kind, c],
            recv_sem=self.recv_sem.at[kind, c],
            device_id={"tensoror": right if TO_RIGHT[kind] else left},
            device_id_type=MESH,
        )

    def first(self, c, part):
        me, right, opposite, left = neighbours()
        send, keep = self.send, self.keep
        half = self.rows // 2
        sums = part(2, opposite)
        send[0, c] = sums[:half].astype(jnp.bfloat16)
        send[1, c] = sums[half:].astype(jnp.bfloat16)
        self.copy(0, c).start()
        self.copy(1, c).start()
        sums = part(1, right)
        send[2, c] = sums[:half].astype(jnp.bfloat16)
        keep[1, c] = sums[half:]
        self.copy(2, c).start()
        sums = part(3, left)
        send[3, c] = sums[half:].astype(jnp.bfloat16)
        keep[0, c] = sums[:half]
        self.copy(3, c).start()
        self.own[c] = part(0, me)

    def pass_on(self, c):
        for side in (0, 1):
            self.copy(side, c).wait_recv()
            self.send[4 + side, c] = (
                self.keep[side, c] + self.recv[side, c].astype(jnp.float32)
            ).astype(jnp.bfloat16)
            self.copy(4 + side, c).start()

    def last(self, c):
        for kind in (2, 3, 4, 5):
            self.copy(kind, c).wait_recv()
        half = self.rows // 2
        own, recv = self.own, self.recv
        return [
            own[c, side * half : (side + 1) * half]
            + recv[2 + side, c].astype(jnp.float32)
            + recv[4 + side, c].astype(jnp.float32)
            for side in (0, 1)
        ]

    def finish(self):
        def wait(c):
            for kind in range(6):
                self.copy(kind, c).wait_send()

        each(0, self.chunks, wait)


def each(start, stop, body):
    lax.fori_loop(start, stop, lambda c, _: (body(c), 0)[1], 0)


def piece_scratch(chunks, rows, wide):
    return [
        pltpu.VMEM((6, chunks, rows // 2, wide), jnp.bfloat16),
        pltpu.VMEM((6, chunks, rows // 2, wide), jnp.bfloat16),
        pltpu.VMEM((2, chunks, rows // 2, wide), jnp.float32),
        pltpu.VMEM((chunks, rows, wide), jnp.float32),
        pltpu.SemaphoreType.DMA((6, chunks)),
        pltpu.SemaphoreType.DMA((6, chunks)),
    ]


OWN, NEXT, PREV, ACROSS, PARTNER = (0, 0, 0), (1, 0, 0), (3, 0, 0), (0, 1, 0), (0, 0, 1)
FAR = (2, 0, 0)
KINDS = {
    "next0": (OWN, PREV, 0),
    "next1": (OWN, PREV, 1),
    "prev1": (OWN, NEXT, 1),
    "prev0": (OWN, NEXT, 0),
    "across": (OWN, ACROSS, None),
    "partner": (OWN, PARTNER, None),
    "far0": (NEXT, PREV, 0),
    "far1": (PREV, NEXT, 1),
    "next_across": (ACROSS, PREV, None),
    "prev_across": (ACROSS, NEXT, None),
    "far_across0": (FAR, ACROSS, 0),
    "far_across1": (FAR, ACROSS, 1),
}
GOT = {
    "next0": NEXT,
    "next1": NEXT,
    "prev1": PREV,
    "prev0": PREV,
    "across": ACROSS,
    "partner": PARTNER,
    "far0": FAR,
    "far1": FAR,
    "next_across": (1, 1, 0),
    "prev_across": (3, 1, 0),
    "far_across0": (2, 1, 0),
    "far_across1": (2, 1, 0),
}
for name in list(GOT):
    if name != "partner":
        KINDS["twin_" + name] = (GOT[name], PARTNER, KINDS[name][2])
        GOT["twin_" + name] = GOT[name][:2] + (1,)
ORDER = {name: k for k, name in enumerate(KINDS)}
NEAR_TWINS = [
    "twin_" + name for name in ("next0", "next1", "prev1", "prev0", "across", "far0", "far1")
]


def seq_at(offset):
    place = lax.axis_index("seq")
    y = lax.rem(lax.div(place, 4) + offset[0], 4)
    z = lax.rem(lax.div(place, 2) + offset[1], 2)
    core = lax.rem(place + offset[2], 2)
    return y * 4 + z * 2 + core


class Gather:
    def __init__(self, blocks, send_sem, recv_sem, first=0, last=None):
        self.refs = blocks, send_sem, recv_sem
        self.first, self.size = first, (last or blocks.shape[2]) - first

    def copy(self, name, arrival):
        blocks, send_sem, recv_sem = self.refs
        block, target, half = KINDS[name]
        rows = blocks.shape[1]
        cut = pl.ds(0, rows) if half is None else pl.ds(half * (rows // 2), rows // 2)
        where = blocks.at[
            seq_at(GOT[name] if arrival else block), cut, pl.ds(self.first, self.size)
        ]
        k = ORDER[name]
        return pltpu.make_async_remote_copy(
            src_ref=where,
            dst_ref=where,
            send_sem=send_sem.at[k],
            recv_sem=recv_sem.at[k],
            device_id={"seq": seq_at(target)},
            device_id_type=MESH,
        )

    def start(self, *names):
        for name in names:
            self.copy(name, False).start()

    def arrived(self, *names):
        for name in names:
            self.copy(name, True).wait_recv()

    def start_own(self):
        self.start("next0", "prev1", "across", "next1", "prev0", "partner")

    def forward_near(self):
        self.arrived("next0")
        self.start("far0", "twin_next0")
        self.arrived("prev1")
        self.start("far1", "twin_prev1")
        self.arrived("across")
        self.start("next_across", "prev_across", "twin_across")
        self.arrived("next1")
        self.start("twin_next1")
        self.arrived("prev0")
        self.start("twin_prev0")

    def forward_far(self):
        self.arrived("far0")
        self.start("far_across0", "twin_far0")
        self.arrived("far1")
        self.start("far_across1", "twin_far1")

    def forward_last(self):
        self.arrived("next_across")
        self.start("twin_next_across")
        self.arrived("prev_across")
        self.start("twin_prev_across")
        self.arrived("far_across0")
        self.start("twin_far_across0")
        self.arrived("far_across1")
        self.start("twin_far_across1")

    def near_here(self):
        self.arrived("partner", *[name for name in KINDS if name in NEAR_TWINS])

    def late_here(self):
        self.arrived(*[name for name in KINDS if name[:5] == "twin_" and name not in NEAR_TWINS])

    def finish(self):
        for name in KINDS:
            self.copy(name, False).wait_send()


def seq_peers():
    return [{"seq": seq_at(offset)} for offset in (NEXT, PREV, ACROSS, PARTNER)]


GATHER_SEMAPHORES = [
    pltpu.SemaphoreType.DMA((len(KINDS),)),
    pltpu.SemaphoreType.DMA((len(KINDS),)),
]


PASSES = (0, 1, 3, 5)


def mix_kernel(
    start_ref,
    count_ref,
    hidden_ref,
    w_ref,
    text_ref,
    gain_ref,
    out_ref,
    square_ref,
    act,
    weights,
    blocks,
    text,
    weight_sem,
    text_send,
    text_recv,
    own_sem,
    gather_send,
    gather_recv,
    *scratch,
):
    me, right, opposite, left = neighbours()
    group = lax.axis_index("group")
    place = lax.axis_index("seq")
    pieces = Pieces(*scratch)
    chunks, wide = pieces.chunks, pieces.wide
    local = text_ref.shape[0]
    sequences, rows, width = text.shape
    part_rows = blocks.shape[1] // sequences
    spans = [(a * wide, b * wide) for a, b in zip(PASSES, PASSES[1:])]
    gathers = [
        Gather(blocks, gather_send.at[p], gather_recv.at[p], *span)
        for p, span in enumerate(spans)
    ]

    def load(k, dest, c):
        column = pl.multiple_of(dest * width + c * wide, 128)
        return pltpu.make_async_copy(
            w_ref.at[:, pl.ds(column, wide)], weights.at[k, c], weight_sem.at[k, c]
        )

    for c in range(chunks):
        for k, dest in ((2, opposite), (1, right), (3, left), (0, me)):
            load(k, dest, c).start()
    own_text = pltpu.make_async_copy(
        text_ref.at[:, :, pl.ds(pl.multiple_of(me * width, 128), width)],
        text.at[pl.ds(me * local, local)],
        own_sem,
    )
    own_text.start()
    greet([{"tensoror": peer} for peer in (right, opposite, left)] + seq_peers())

    def exchange(k, peer, b, p):
        first, last = spans[p]
        source = pl.ds(pl.multiple_of(peer * width + first, 128), last - first)
        return pltpu.make_async_remote_copy(
            src_ref=text_ref.at[b, :, source],
            dst_ref=text.at[me * local + b, :, pl.ds(first, last - first)],
            send_sem=text_send.at[k, b, p],
            recv_sem=text_recv.at[k, b, p],
            device_id={"tensoror": peer},
            device_id_type=MESH,
        )

    peers = ((2, opposite), (1, right), (3, left))
    for k, peer in peers:
        exchange(k, peer, 0, 0).start()
    hidden = hidden_ref[...].astype(jnp.float32)
    act[...] = (0.5 * hidden * (1.0 + lax.erf(hidden * math.sqrt(0.5)))).astype(jnp.bfloat16)

    def first(c):
        def part(k, dest):
            load(k, dest, c).wait()
            return jnp.dot(act[...], weights[k, c], preferred_element_type=jnp.float32)

        pieces.first(c, part)

    def last(c):
        column = pl.ds(pl.multiple_of(c * wide, 128), wide)
        half = pieces.rows // 2
        for side, sums in enumerate(pieces.last(c)):
            blocks[place, side * half : (side + 1) * half, column] = sums.astype(jnp.bfloat16)

    diagonal = lax.broadcasted_iota(jnp.int32, (rows, rows), 0) == lax.broadcasted_iota(
        jnp.int32, (rows, rows), 1
    )

    def mix_columns(p):
        low, high = spans[p]
        gain = gain_ref[:, pl.ds(pl.multiple_of(me * width + low, 128), high - low)]

        def one(i):
            start = start_ref[group * sequences + i]
            slots = TILE * count_ref[group * sequences + i]
            visual = blocks[
                :, pl.ds(pl.multiple_of(i * part_rows, part_rows), part_rows), low:high
            ].reshape(-1, high - low)
            total = visual.shape[0]
            shift = place * rows - start
            slot = shift + lax.broadcasted_iota(jnp.int32, (rows, total), 0)
            column = lax.broadcasted_iota(jnp.int32, (rows, total), 1)
            pick = jnp.where((slot == column) & (column < slots), 1.0, 0.0).astype(jnp.bfloat16)
            placed = jnp.dot(pick, visual, preferred_element_type=jnp.float32)
            own = shift + lax.broadcasted_iota(jnp.int32, placed.shape, 0)
            inside = (own >= 0) & (own < slots)
            mixed = jnp.where(inside, placed, text[i, :, low:high].astype(jnp.float32))
            squares = jnp.sum(mixed * mixed, axis=1, keepdims=True)
            line = jnp.sum(jnp.where(diagonal, squares, 0.0), axis=0, keepdims=True)
            if p == 0:
                square_ref[pl.ds(i, 1), :] = line
            else:
                square_ref[pl.ds(i, 1), :] += line
            out_ref[pl.ds(pl.multiple_of(i * rows, rows), rows), low:high] = (
                mixed * gain
            ).astype(jnp.bfloat16)

        each(0, sequences, one)

    def own_start(p):
        each(PASSES[p], PASSES[p + 1], last)
        gathers[p].start_own()

    def text_here(p):
        for b in range(local):
            for k, peer in peers:
                exchange(k, peer, b, p).wait()

    each(0, 1, first)
    each(1, 2, first)
    each(0, 1, pieces.pass_on)
    each(2, 3, first)
    each(1, 2, pieces.pass_on)
    own_start(0)
    each(3, 4, first)
    each(2, 3, pieces.pass_on)
    each(4, 5, first)
    each(3, 4, pieces.pass_on)
    gathers[0].forward_near()
    own_start(1)
    each(4, 5, pieces.pass_on)
    for b, p in ((1, 0), (0, 1), (1, 1), (0, 2), (1, 2)):
        for k, peer in peers:
            exchange(k, peer, b, p).start()
    gathers[0].forward_far()
    gathers[0].forward_last()
    gathers[1].forward_near()
    own_start(2)
    own_text.wait()
    gathers[0].near_here()
    gathers[0].late_here()
    gathers[1].forward_far()
    text_here(0)
    mix_columns(0)
    gathers[1].forward_last()
    gathers[2].forward_near()
    gathers[1].near_here()
    gathers[1].late_here()
    gathers[2].forward_far()
    text_here(1)
    mix_columns(1)
    gathers[2].forward_last()
    text_here(2)
    gathers[2].near_here()
    gathers[2].late_here()
    mix_columns(2)
    for gather in gathers:
        gather.finish()
    pieces.finish()


def mix(starts, counts, hidden, weight, text, gain):
    devices = lax.axis_size("seq")
    count = lax.axis_size("tensoror")
    local, rows, full = text.shape
    width = full // count
    sequences = local * count
    wide = 256
    chunks = width // wide
    smem = pl.BlockSpec(memory_space=pltpu.SMEM)
    vmem = pl.BlockSpec(memory_space=pltpu.VMEM)
    hbm = pl.BlockSpec(memory_space=pl.ANY)
    return pl.pallas_call(
        mix_kernel,
        in_specs=[smem, smem, vmem, hbm, hbm, vmem],
        out_specs=[vmem, vmem],
        out_shape=[
            jax.ShapeDtypeStruct((sequences * rows, width), jnp.bfloat16),
            jax.ShapeDtypeStruct((sequences, rows), jnp.float32),
        ],
        scratch_shapes=[
            pltpu.VMEM(hidden.shape, jnp.bfloat16),
            pltpu.VMEM((count, chunks, width, wide), jnp.bfloat16),
            pltpu.VMEM((devices, hidden.shape[0], width), jnp.bfloat16),
            pltpu.VMEM((sequences, rows, width), jnp.bfloat16),
            pltpu.SemaphoreType.DMA((count, chunks)),
            pltpu.SemaphoreType.DMA((count, local, len(PASSES) - 1)),
            pltpu.SemaphoreType.DMA((count, local, len(PASSES) - 1)),
            pltpu.SemaphoreType.DMA,
            pltpu.SemaphoreType.DMA((len(PASSES) - 1, len(KINDS))),
            pltpu.SemaphoreType.DMA((len(PASSES) - 1, len(KINDS))),
        ]
        + piece_scratch(chunks, hidden.shape[0], wide),
        compiler_params=pltpu.CompilerParams(
            collective_id=0, has_side_effects=True, vmem_limit_bytes=VMEM
        ),
    )(starts, counts, hidden, weight, text, gain)


def attend_kernel(
    x_ref,
    square_ref,
    wkv_ref,
    wq_ref,
    out_ref,
    kv_weights,
    q_weights,
    squares,
    total_squares,
    scale,
    blocks,
    queries,
    totals,
    top,
    low,
    kv_weight_sem,
    q_weight_sem,
    square_send,
    square_recv,
    gather_send,
    gather_recv,
    *scratch,
    width,
):
    me, right, opposite, left = neighbours()
    place = lax.axis_index("seq")
    chip = lax.div(place, 2)
    kv_pieces, q_pieces = Pieces(*scratch[:6]), Pieces(*scratch[6:])
    rows = HEAD_SIZE
    local = kv_pieces.rows // rows
    factor = math.log2(math.e) / math.sqrt(HEAD_SIZE)
    gather = Gather(blocks, gather_send, gather_recv)

    def weight_copy(source, c, wide, weights, sem):
        column = pl.ds(pl.multiple_of(c * wide, 128), wide)
        return pltpu.make_async_copy(source.at[:, column], weights.at[c], sem.at[c])

    def kv_copy(c):
        return weight_copy(wkv_ref, c, kv_pieces.wide, kv_weights, kv_weight_sem)

    def q_copy(c):
        return weight_copy(wq_ref, c, q_pieces.wide, q_weights, q_weight_sem)

    for c in range(kv_pieces.chunks):
        kv_copy(c).start()
    for c in range(q_pieces.chunks):
        q_copy(c).start()
    greet([{"tensoror": peer} for peer in (right, opposite, left)] + seq_peers())

    def square_copy(k, peer):
        return pltpu.make_async_remote_copy(
            src_ref=square_ref,
            dst_ref=squares.at[k],
            send_sem=square_send.at[k],
            recv_sem=square_recv.at[k],
            device_id={"tensoror": peer},
            device_id_type=MESH,
        )

    peers = ((1, right), (2, opposite), (3, left))
    for k, peer in peers:
        square_copy(k, peer).start()

    def part_of(weights, c):
        def part(k, dest):
            span = pl.ds(pl.multiple_of(dest * local * rows, rows), local * rows)
            return jnp.dot(x_ref[span, :], weights[c], preferred_element_type=jnp.float32)

        return part

    def first_kv(c):
        kv_copy(c).wait()
        kv_pieces.first(c, part_of(kv_weights, c))

    def first_q(c):
        q_copy(c).wait()
        q_pieces.first(c, part_of(q_weights, c))

    each(0, kv_pieces.chunks, first_kv)
    for k, peer in peers:
        square_copy(k, peer).wait()
    total_squares[...] = square_ref[...] + squares[1] + squares[2] + squares[3]
    diagonal = lax.broadcasted_iota(jnp.int32, (rows, rows), 0) == lax.broadcasted_iota(
        jnp.int32, (rows, rows), 1
    )
    for b in range(local):
        row = jnp.broadcast_to(total_squares[pl.ds(me * local + b, 1), :], (rows, rows))
        column = jnp.sum(jnp.where(diagonal, row, 0.0), axis=1, keepdims=True)
        scale[b * rows : (b + 1) * rows, :] = lax.rsqrt(column / width + epsilon)
    each(0, kv_pieces.chunks, kv_pieces.pass_on)
    each(0, 2, first_q)

    def last_kv(c):
        column = pl.ds(pl.multiple_of(c * kv_pieces.wide, 128), kv_pieces.wide)
        for b, sums in enumerate(kv_pieces.last(c)):
            span = slice(b * rows, (b + 1) * rows)
            blocks[place, span, column] = (sums * scale[span, :]).astype(jnp.bfloat16)

    each(0, kv_pieces.chunks, last_kv)
    gather.start_own()

    def second_q(c):
        first_q(c)
        q_pieces.pass_on(c - 2)

    def absorb(b, h, other, masked):
        unit = b * KEY_VALUE_HEADS + h
        span = slice(b * rows, (b + 1) * rows)
        pair = pl.ds(2 * other, 2)
        key_column = pl.multiple_of(h * HEAD_SIZE, 128)
        value_column = pl.multiple_of((h + KEY_VALUE_HEADS) * HEAD_SIZE, 128)
        keys = blocks[pair, span, pl.ds(key_column, HEAD_SIZE)]
        values = blocks[pair, span, pl.ds(value_column, HEAD_SIZE)]
        scores = lax.dot_general(
            keys.reshape(2 * rows, HEAD_SIZE),
            queries[unit],
            (((1,), (1,)), ((), ())),
            preferred_element_type=jnp.float32,
        )
        if masked:
            key = lax.broadcasted_iota(jnp.int32, scores.shape, 0)
            query = (
                lax.rem(lax.broadcasted_iota(jnp.int32, scores.shape, 1), rows)
                + lax.rem(place, 2) * rows
            )
            scores = jnp.where(key <= query, scores, masked_score)
        best = jnp.max(scores, axis=0, keepdims=True)
        new = best if masked else jnp.maximum(top[unit], best)
        expo = jnp.exp2((scores - new) * factor)
        summed = jnp.sum(expo, axis=0, keepdims=True)
        added = lax.dot_general(
            values.reshape(2 * rows, HEAD_SIZE),
            expo.astype(jnp.bfloat16),
            (((0,), (0,)), ((), ())),
            preferred_element_type=jnp.float32,
        )
        if masked:
            totals[unit] = added
            low[unit] = summed
        else:
            keep = jnp.exp2((top[unit] - new) * factor)
            totals[unit] = totals[unit] * keep + added
            low[unit] = low[unit] * keep + summed
        top[unit] = new

    def absorb_other(h, steps, across):
        other = lax.div(seq_at((steps, across, 0)), 2)

        @pl.when(other < chip)
        def _():
            for b in range(local):
                absorb(b, h, other, False)

    def group_near(h):
        for b, sums in enumerate(q_pieces.last(h)):
            unit = b * KEY_VALUE_HEADS + h
            scaled = (sums * scale[b * rows : (b + 1) * rows, :]).astype(jnp.bfloat16)
            for j in range(GROUP_HEADS):
                queries[unit, j * rows : (j + 1) * rows, :] = scaled[
                    :, j * HEAD_SIZE : (j + 1) * HEAD_SIZE
                ]
        for b in range(local):
            absorb(b, h, chip, True)
        each(0, 4, lambda steps: absorb_other(h, steps, jnp.where(steps == 0, 1, 0)))

    def group_late(h):
        each(1, 4, lambda steps: absorb_other(h, steps, 1))
        for b in range(local):
            unit = b * KEY_VALUE_HEADS + h
            result = totals[unit] / low[unit]
            for j in range(GROUP_HEADS):
                column = pl.multiple_of((h * GROUP_HEADS + j) * HEAD_SIZE, 128)
                out_ref[b * rows : (b + 1) * rows, pl.ds(column, HEAD_SIZE)] = jnp.transpose(
                    result[:, j * rows : (j + 1) * rows]
                ).astype(jnp.bfloat16)

    each(2, q_pieces.chunks, second_q)
    gather.forward_near()
    gather.forward_far()
    q_pieces.pass_on(2)
    gather.near_here()
    each(0, 1, group_near)
    gather.arrived("next_across")
    gather.start("twin_next_across")
    gather.arrived("prev_across")
    gather.start("twin_prev_across")
    each(1, 2, group_near)
    gather.arrived("far_across0")
    gather.start("twin_far_across0")
    gather.arrived("far_across1")
    gather.start("twin_far_across1")
    q_pieces.pass_on(3)
    gather.late_here()
    each(0, 2, group_late)

    def whole(h):
        group_near(h)
        group_late(h)

    each(2, KEY_VALUE_HEADS, whole)
    gather.finish()
    kv_pieces.finish()
    q_pieces.finish()


def attend(mixed, squares, kv_weight, q_weight, full_width):
    count = lax.axis_size("tensoror")
    devices = lax.axis_size("seq")
    total, width = mixed.shape
    rows = total // count
    kv_cols = kv_weight.shape[1]
    q_cols = q_weight.shape[1]
    kv_wide, q_wide = 512, GROUP_HEADS * HEAD_SIZE
    kv_chunks, q_chunks = kv_cols // kv_wide, q_cols // q_wide
    local = rows // HEAD_SIZE
    vmem = pl.BlockSpec(memory_space=pltpu.VMEM)
    hbm = pl.BlockSpec(memory_space=pl.ANY)
    return pl.pallas_call(
        functools.partial(attend_kernel, width=full_width),
        in_specs=[vmem, vmem, hbm, hbm],
        out_specs=vmem,
        out_shape=jax.ShapeDtypeStruct((rows, q_cols), jnp.bfloat16),
        scratch_shapes=[
            pltpu.VMEM((kv_chunks, width, kv_wide), jnp.bfloat16),
            pltpu.VMEM((q_chunks, width, q_wide), jnp.bfloat16),
            pltpu.VMEM((count,) + squares.shape, jnp.float32),
            pltpu.VMEM(squares.shape, jnp.float32),
            pltpu.VMEM((rows, 1), jnp.float32),
            pltpu.VMEM((devices, rows, kv_cols), jnp.bfloat16),
            pltpu.VMEM((local * KEY_VALUE_HEADS, q_wide, HEAD_SIZE), jnp.bfloat16),
            pltpu.VMEM((local * KEY_VALUE_HEADS, HEAD_SIZE, q_wide), jnp.float32),
            pltpu.VMEM((local * KEY_VALUE_HEADS, 1, q_wide), jnp.float32),
            pltpu.VMEM((local * KEY_VALUE_HEADS, 1, q_wide), jnp.float32),
            pltpu.SemaphoreType.DMA((kv_chunks,)),
            pltpu.SemaphoreType.DMA((q_chunks,)),
            pltpu.SemaphoreType.DMA((count,)),
            pltpu.SemaphoreType.DMA((count,)),
        ]
        + GATHER_SEMAPHORES
        + piece_scratch(kv_chunks, rows, kv_wide)
        + piece_scratch(q_chunks, rows, q_wide),
        compiler_params=pltpu.CompilerParams(
            collective_id=2, has_side_effects=True, vmem_limit_bytes=VMEM
        ),
    )(mixed, squares, kv_weight, q_weight)


def shards(
    visual_hidden,
    projector_weight,
    text_embeddings,
    tile_counts,
    image_start,
    norm_gain,
    query_weight,
    keyvalue_weight,
):
    sequence_local, extent_rows, width = text_embeddings.shape
    sequences, slot_rows, depth = visual_hidden.shape
    mixed, squares = mix(
        image_start,
        tile_counts,
        visual_hidden.reshape(sequences * slot_rows, depth),
        projector_weight,
        text_embeddings,
        norm_gain.reshape(1, width),
    )
    context = attend(mixed, squares, keyvalue_weight, query_weight, width)
    return context.reshape(sequence_local, extent_rows, -1)


def solution(mesh):
    in_specs = (
        P("group", "seq", "tensoror"),
        P("tensoror", None),
        P(("group", "tensoror"), "seq", None),
        P(),
        P(),
        P(),
        P("tensoror", None),
        P("tensoror", None),
    )
    out_specs = P(("group", "tensoror"), "seq", None)
    return jax.shard_map(shards, mesh=mesh, in_specs=in_specs, out_specs=out_specs, check_vma=False)
```

```python
import functools
import math

import jax
import jax.numpy as jnp
from jax import lax
from jax.experimental import pallas as pl
from jax.experimental.pallas import tpu as pltpu
from jax.sharding import PartitionSpec as P

QUERY_HEADS = 20
KEY_VALUE_HEADS = 4
HEAD_SIZE = 128
TILE = 256
GROUP_HEADS = QUERY_HEADS // KEY_VALUE_HEADS
MESH = pl.DeviceIdType.MESH

epsilon = 1e-06
masked_score = -1e30
VMEM = 60 * 1024 * 1024


def neighbours():
    count = lax.axis_size("tensoror")
    me = lax.axis_index("tensoror")
    return me, lax.rem(me + 1, count), lax.rem(me + 2, count), lax.rem(me + 3, count)


def greet(peers):
    barrier = pltpu.get_barrier_semaphore()
    for peer in peers:
        pl.semaphore_signal(
            barrier, inc=1, device_id=peer, device_id_type=MESH
        )
    pl.semaphore_wait(barrier, len(peers))


TO_RIGHT = (False, True, True, False, False, True)


class Pieces:
    def __init__(self, send, recv, keep, own, send_sem, recv_sem):
        self.send, self.recv, self.keep, self.own = send, recv, keep, own
        self.send_sem, self.recv_sem = send_sem, recv_sem
        self.chunks, self.rows, self.wide = own.shape

    def copy(self, kind, c):
        me, right, opposite, left = neighbours()
        return pltpu.make_async_remote_copy(
            src_ref=self.send.at[kind, c],
            dst_ref=self.recv.at[kind, c],
            send_sem=self.send_sem.at[kind, c],
            recv_sem=self.recv_sem.at[kind, c],
            device_id={"tensoror": right if TO_RIGHT[kind] else left},
            device_id_type=MESH,
        )

    def first(self, c, part):
        me, right, opposite, left = neighbours()
        send, keep = self.send, self.keep
        half = self.rows // 2
        sums = part(2, opposite)
        send[0, c] = sums[:half].astype(jnp.bfloat16)
        send[1, c] = sums[half:].astype(jnp.bfloat16)
        self.copy(0, c).start()
        self.copy(1, c).start()
        sums = part(1, right)
        send[2, c] = sums[:half].astype(jnp.bfloat16)
        keep[1, c] = sums[half:]
        self.copy(2, c).start()
        sums = part(3, left)
        send[3, c] = sums[half:].astype(jnp.bfloat16)
        keep[0, c] = sums[:half]
        self.copy(3, c).start()
        self.own[c] = part(0, me)

    def pass_on(self, c):
        for side in (0, 1):
            self.copy(side, c).wait_recv()
            self.send[4 + side, c] = (
                self.keep[side, c] + self.recv[side, c].astype(jnp.float32)
            ).astype(jnp.bfloat16)
            self.copy(4 + side, c).start()

    def last(self, c):
        for kind in (2, 3, 4, 5):
            self.copy(kind, c).wait_recv()
        half = self.rows // 2
        own, recv = self.own, self.recv
        return [
            own[c, side * half : (side + 1) * half]
            + recv[2 + side, c].astype(jnp.float32)
            + recv[4 + side, c].astype(jnp.float32)
            for side in (0, 1)
        ]

    def finish(self):
        def wait(c):
            for kind in range(6):
                self.copy(kind, c).wait_send()

        each(0, self.chunks, wait)


def each(start, stop, body):
    lax.fori_loop(start, stop, lambda c, _: (body(c), 0)[1], 0)


def piece_scratch(chunks, rows, wide):
    return [
        pltpu.VMEM((6, chunks, rows // 2, wide), jnp.bfloat16),
        pltpu.VMEM((6, chunks, rows // 2, wide), jnp.bfloat16),
        pltpu.VMEM((2, chunks, rows // 2, wide), jnp.float32),
        pltpu.VMEM((chunks, rows, wide), jnp.float32),
        pltpu.SemaphoreType.DMA((6, chunks)),
        pltpu.SemaphoreType.DMA((6, chunks)),
    ]


OWN, NEXT, PREV, ACROSS, PARTNER = (0, 0, 0), (1, 0, 0), (3, 0, 0), (0, 1, 0), (0, 0, 1)
FAR = (2, 0, 0)
KINDS = {
    "next0": (OWN, PREV, 0),
    "next1": (OWN, PREV, 1),
    "prev1": (OWN, NEXT, 1),
    "prev0": (OWN, NEXT, 0),
    "across": (OWN, ACROSS, None),
    "partner": (OWN, PARTNER, None),
    "far0": (NEXT, PREV, 0),
    "far1": (PREV, NEXT, 1),
    "next_across": (ACROSS, PREV, None),
    "prev_across": (ACROSS, NEXT, None),
    "far_across0": (FAR, ACROSS, 0),
    "far_across1": (FAR, ACROSS, 1),
}
GOT = {
    "next0": NEXT,
    "next1": NEXT,
    "prev1": PREV,
    "prev0": PREV,
    "across": ACROSS,
    "partner": PARTNER,
    "far0": FAR,
    "far1": FAR,
    "next_across": (1, 1, 0),
    "prev_across": (3, 1, 0),
    "far_across0": (2, 1, 0),
    "far_across1": (2, 1, 0),
}
for name in list(GOT):
    if name != "partner":
        KINDS["twin_" + name] = (GOT[name], PARTNER, KINDS[name][2])
        GOT["twin_" + name] = GOT[name][:2] + (1,)
ORDER = {name: k for k, name in enumerate(KINDS)}
NEAR_TWINS = [
    "twin_" + name for name in ("next0", "next1", "prev1", "prev0", "across", "far0", "far1")
]


def seq_at(offset):
    place = lax.axis_index("seq")
    y = lax.rem(lax.div(place, 4) + offset[0], 4)
    z = lax.rem(lax.div(place, 2) + offset[1], 2)
    core = lax.rem(place + offset[2], 2)
    return y * 4 + z * 2 + core


class Gather:
    def __init__(self, blocks, send_sem, recv_sem, first=0, last=None):
        self.refs = blocks, send_sem, recv_sem
        self.first, self.size = first, (last or blocks.shape[2]) - first

    def copy(self, name, arrival):
        blocks, send_sem, recv_sem = self.refs
        block, target, half = KINDS[name]
        rows = blocks.shape[1]
        cut = pl.ds(0, rows) if half is None else pl.ds(half * (rows // 2), rows // 2)
        where = blocks.at[
            seq_at(GOT[name] if arrival else block), cut, pl.ds(self.first, self.size)
        ]
        k = ORDER[name]
        return pltpu.make_async_remote_copy(
            src_ref=where,
            dst_ref=where,
            send_sem=send_sem.at[k],
            recv_sem=recv_sem.at[k],
            device_id={"seq": seq_at(target)},
            device_id_type=MESH,
        )

    def start(self, *names):
        for name in names:
            self.copy(name, False).start()

    def arrived(self, *names):
        for name in names:
            self.copy(name, True).wait_recv()

    def start_own(self):
        self.start("next0", "prev1", "across", "next1", "prev0", "partner")

    def forward_near(self):
        self.arrived("next0")
        self.start("far0", "twin_next0")
        self.arrived("prev1")
        self.start("far1", "twin_prev1")
        self.arrived("across")
        self.start("next_across", "prev_across", "twin_across")
        self.arrived("next1")
        self.start("twin_next1")
        self.arrived("prev0")
        self.start("twin_prev0")

    def forward_far(self):
        self.arrived("far0")
        self.start("far_across0", "twin_far0")
        self.arrived("far1")
        self.start("far_across1", "twin_far1")

    def forward_beside(self):
        self.arrived("next_across")
        self.start("twin_next_across")
        self.arrived("prev_across")
        self.start("twin_prev_across")

    def forward_last(self):
        self.arrived("far_across0")
        self.start("twin_far_across0")
        self.arrived("far_across1")
        self.start("twin_far_across1")

    def near_here(self):
        self.arrived("partner", *[name for name in KINDS if name in NEAR_TWINS])

    def beside_here(self):
        self.arrived("twin_next_across", "twin_prev_across")

    def last_here(self):
        self.arrived("twin_far_across0", "twin_far_across1")

    def finish(self):
        for name in KINDS:
            self.copy(name, False).wait_send()


def seq_peers():
    return [{"seq": seq_at(offset)} for offset in (NEXT, PREV, ACROSS, PARTNER)]


GATHER_SEMAPHORES = [
    pltpu.SemaphoreType.DMA((len(KINDS),)),
    pltpu.SemaphoreType.DMA((len(KINDS),)),
]


PASSES = (0, 1, 3, 5)


def mix_kernel(
    start_ref,
    count_ref,
    hidden_ref,
    w_ref,
    text_ref,
    gain_ref,
    out_ref,
    square_ref,
    act,
    weights,
    blocks,
    text,
    weight_sem,
    text_send,
    text_recv,
    own_sem,
    gather_send,
    gather_recv,
    *scratch,
):
    me, right, opposite, left = neighbours()
    group = lax.axis_index("group")
    place = lax.axis_index("seq")
    pieces = Pieces(*scratch)
    chunks, wide = pieces.chunks, pieces.wide
    local = text_ref.shape[0]
    sequences, rows, width = text.shape
    part_rows = blocks.shape[1] // sequences
    spans = [(a * wide, b * wide) for a, b in zip(PASSES, PASSES[1:])]
    gathers = [
        Gather(blocks, gather_send.at[p], gather_recv.at[p], *span)
        for p, span in enumerate(spans)
    ]

    def load(k, dest, c):
        column = pl.multiple_of(dest * width + c * wide, 128)
        return pltpu.make_async_copy(
            w_ref.at[:, pl.ds(column, wide)], weights.at[k, c], weight_sem.at[k, c]
        )

    for c in range(chunks):
        for k, dest in ((2, opposite), (1, right), (3, left), (0, me)):
            load(k, dest, c).start()
    own_text = pltpu.make_async_copy(
        text_ref.at[:, :, pl.ds(pl.multiple_of(me * width, 128), width)],
        text.at[pl.ds(me * local, local)],
        own_sem,
    )
    own_text.start()
    greet([{"tensoror": peer} for peer in (right, opposite, left)] + seq_peers())

    def exchange(k, peer, b, p):
        first, last = spans[p]
        source = pl.ds(pl.multiple_of(peer * width + first, 128), last - first)
        return pltpu.make_async_remote_copy(
            src_ref=text_ref.at[b, :, source],
            dst_ref=text.at[me * local + b, :, pl.ds(first, last - first)],
            send_sem=text_send.at[k, b, p],
            recv_sem=text_recv.at[k, b, p],
            device_id={"tensoror": peer},
            device_id_type=MESH,
        )

    peers = ((2, opposite), (1, right), (3, left))
    for k, peer in peers:
        exchange(k, peer, 0, 0).start()
    hidden = hidden_ref[...].astype(jnp.float32)
    act[...] = (0.5 * hidden * (1.0 + lax.erf(hidden * math.sqrt(0.5)))).astype(jnp.bfloat16)

    def first(c):
        def part(k, dest):
            load(k, dest, c).wait()
            return jnp.dot(act[...], weights[k, c], preferred_element_type=jnp.float32)

        pieces.first(c, part)

    def last(c):
        column = pl.ds(pl.multiple_of(c * wide, 128), wide)
        half = pieces.rows // 2
        for side, sums in enumerate(pieces.last(c)):
            blocks[place, side * half : (side + 1) * half, column] = sums.astype(jnp.bfloat16)

    diagonal = lax.broadcasted_iota(jnp.int32, (rows, rows), 0) == lax.broadcasted_iota(
        jnp.int32, (rows, rows), 1
    )

    def mix_columns(p):
        low, high = spans[p]
        gain = gain_ref[:, pl.ds(pl.multiple_of(me * width + low, 128), high - low)]

        def one(i):
            start = start_ref[group * sequences + i]
            slots = TILE * count_ref[group * sequences + i]
            visual = blocks[
                :, pl.ds(pl.multiple_of(i * part_rows, part_rows), part_rows), low:high
            ].reshape(-1, high - low)
            total = visual.shape[0]
            shift = place * rows - start
            slot = shift + lax.broadcasted_iota(jnp.int32, (rows, total), 0)
            column = lax.broadcasted_iota(jnp.int32, (rows, total), 1)
            pick = jnp.where((slot == column) & (column < slots), 1.0, 0.0).astype(jnp.bfloat16)
            placed = jnp.dot(pick, visual, preferred_element_type=jnp.float32)
            own = shift + lax.broadcasted_iota(jnp.int32, placed.shape, 0)
            inside = (own >= 0) & (own < slots)
            mixed = jnp.where(inside, placed, text[i, :, low:high].astype(jnp.float32))
            squares = jnp.sum(mixed * mixed, axis=1, keepdims=True)
            line = jnp.sum(jnp.where(diagonal, squares, 0.0), axis=0, keepdims=True)
            if p == 0:
                square_ref[pl.ds(i, 1), :] = line
            else:
                square_ref[pl.ds(i, 1), :] += line
            out_ref[pl.ds(pl.multiple_of(i * rows, rows), rows), low:high] = (
                mixed * gain
            ).astype(jnp.bfloat16)

        each(0, sequences, one)

    def own_start(p):
        each(PASSES[p], PASSES[p + 1], last)
        gathers[p].start_own()

    def text_here(p):
        for b in range(local):
            for k, peer in peers:
                exchange(k, peer, b, p).wait()

    each(0, 1, first)
    each(1, 2, first)
    each(0, 1, pieces.pass_on)
    each(2, 3, first)
    each(1, 2, pieces.pass_on)
    own_start(0)
    each(3, 4, first)
    each(2, 3, pieces.pass_on)
    each(4, 5, first)
    each(3, 4, pieces.pass_on)
    gathers[0].forward_near()
    own_start(1)
    each(4, 5, pieces.pass_on)
    for b, p in ((1, 0), (0, 1), (1, 1), (0, 2), (1, 2)):
        for k, peer in peers:
            exchange(k, peer, b, p).start()
    gathers[0].forward_far()
    gathers[0].forward_beside()
    gathers[0].forward_last()
    gathers[1].forward_near()
    own_start(2)
    own_text.wait()
    gathers[0].near_here()
    gathers[0].beside_here()
    gathers[0].last_here()
    gathers[1].forward_far()
    text_here(0)
    mix_columns(0)
    gathers[1].forward_beside()
    gathers[1].forward_last()
    gathers[2].forward_near()
    gathers[1].near_here()
    gathers[1].beside_here()
    gathers[1].last_here()
    gathers[2].forward_far()
    text_here(1)
    mix_columns(1)
    gathers[2].forward_beside()
    gathers[2].forward_last()
    text_here(2)
    gathers[2].near_here()
    gathers[2].beside_here()
    gathers[2].last_here()
    mix_columns(2)
    for gather in gathers:
        gather.finish()
    pieces.finish()


def mix(starts, counts, hidden, weight, text, gain):
    devices = lax.axis_size("seq")
    count = lax.axis_size("tensoror")
    local, rows, full = text.shape
    width = full // count
    sequences = local * count
    wide = 256
    chunks = width // wide
    smem = pl.BlockSpec(memory_space=pltpu.SMEM)
    vmem = pl.BlockSpec(memory_space=pltpu.VMEM)
    hbm = pl.BlockSpec(memory_space=pl.ANY)
    return pl.pallas_call(
        mix_kernel,
        in_specs=[smem, smem, vmem, hbm, hbm, vmem],
        out_specs=[vmem, vmem],
        out_shape=[
            jax.ShapeDtypeStruct((sequences * rows, width), jnp.bfloat16),
            jax.ShapeDtypeStruct((sequences, rows), jnp.float32),
        ],
        scratch_shapes=[
            pltpu.VMEM(hidden.shape, jnp.bfloat16),
            pltpu.VMEM((count, chunks, width, wide), jnp.bfloat16),
            pltpu.VMEM((devices, hidden.shape[0], width), jnp.bfloat16),
            pltpu.VMEM((sequences, rows, width), jnp.bfloat16),
            pltpu.SemaphoreType.DMA((count, chunks)),
            pltpu.SemaphoreType.DMA((count, local, len(PASSES) - 1)),
            pltpu.SemaphoreType.DMA((count, local, len(PASSES) - 1)),
            pltpu.SemaphoreType.DMA,
            pltpu.SemaphoreType.DMA((len(PASSES) - 1, len(KINDS))),
            pltpu.SemaphoreType.DMA((len(PASSES) - 1, len(KINDS))),
        ]
        + piece_scratch(chunks, hidden.shape[0], wide),
        compiler_params=pltpu.CompilerParams(
            collective_id=0, has_side_effects=True, vmem_limit_bytes=VMEM
        ),
    )(starts, counts, hidden, weight, text, gain)


def attend_kernel(
    x_ref,
    square_ref,
    wkv_ref,
    wq_ref,
    out_ref,
    kv_weights,
    q_weights,
    squares,
    total_squares,
    scale,
    blocks,
    queries,
    totals,
    top,
    low,
    kv_weight_sem,
    q_weight_sem,
    square_send,
    square_recv,
    gather_send,
    gather_recv,
    *scratch,
    width,
):
    me, right, opposite, left = neighbours()
    place = lax.axis_index("seq")
    chip = lax.div(place, 2)
    kv_pieces, q_pieces = Pieces(*scratch[:6]), Pieces(*scratch[6:])
    rows = HEAD_SIZE
    local = kv_pieces.rows // rows
    factor = math.log2(math.e) / math.sqrt(HEAD_SIZE)
    gather = Gather(blocks, gather_send, gather_recv)

    def weight_copy(source, c, wide, weights, sem):
        column = pl.ds(pl.multiple_of(c * wide, 128), wide)
        return pltpu.make_async_copy(source.at[:, column], weights.at[c], sem.at[c])

    def kv_copy(c):
        return weight_copy(wkv_ref, c, kv_pieces.wide, kv_weights, kv_weight_sem)

    def q_copy(c):
        return weight_copy(wq_ref, c, q_pieces.wide, q_weights, q_weight_sem)

    for c in range(kv_pieces.chunks):
        kv_copy(c).start()
    for c in range(q_pieces.chunks):
        q_copy(c).start()
    greet([{"tensoror": peer} for peer in (right, opposite, left)] + seq_peers())

    def square_copy(k, peer):
        return pltpu.make_async_remote_copy(
            src_ref=square_ref,
            dst_ref=squares.at[k],
            send_sem=square_send.at[k],
            recv_sem=square_recv.at[k],
            device_id={"tensoror": peer},
            device_id_type=MESH,
        )

    peers = ((1, right), (2, opposite), (3, left))
    for k, peer in peers:
        square_copy(k, peer).start()

    def part_of(weights, c):
        def part(k, dest):
            span = pl.ds(pl.multiple_of(dest * local * rows, rows), local * rows)
            return jnp.dot(x_ref[span, :], weights[c], preferred_element_type=jnp.float32)

        return part

    def first_kv(c):
        kv_copy(c).wait()
        kv_pieces.first(c, part_of(kv_weights, c))

    def first_q(c):
        q_copy(c).wait()
        q_pieces.first(c, part_of(q_weights, c))

    each(0, kv_pieces.chunks, first_kv)
    for k, peer in peers:
        square_copy(k, peer).wait()
    total_squares[...] = square_ref[...] + squares[1] + squares[2] + squares[3]
    diagonal = lax.broadcasted_iota(jnp.int32, (rows, rows), 0) == lax.broadcasted_iota(
        jnp.int32, (rows, rows), 1
    )
    for b in range(local):
        row = jnp.broadcast_to(total_squares[pl.ds(me * local + b, 1), :], (rows, rows))
        column = jnp.sum(jnp.where(diagonal, row, 0.0), axis=1, keepdims=True)
        scale[b * rows : (b + 1) * rows, :] = lax.rsqrt(column / width + epsilon)
    each(0, kv_pieces.chunks, kv_pieces.pass_on)
    each(0, 2, first_q)

    def last_kv(c):
        column = pl.ds(pl.multiple_of(c * kv_pieces.wide, 128), kv_pieces.wide)
        for b, sums in enumerate(kv_pieces.last(c)):
            span = slice(b * rows, (b + 1) * rows)
            blocks[place, span, column] = (sums * scale[span, :]).astype(jnp.bfloat16)

    each(0, kv_pieces.chunks, last_kv)
    gather.start_own()

    def second_q(c):
        first_q(c)
        q_pieces.pass_on(c - 2)

    def absorb(b, h, other, masked):
        unit = b * KEY_VALUE_HEADS + h
        span = slice(b * rows, (b + 1) * rows)
        pair = pl.ds(2 * other, 2)
        key_column = pl.multiple_of(h * HEAD_SIZE, 128)
        value_column = pl.multiple_of((h + KEY_VALUE_HEADS) * HEAD_SIZE, 128)
        keys = blocks[pair, span, pl.ds(key_column, HEAD_SIZE)]
        values = blocks[pair, span, pl.ds(value_column, HEAD_SIZE)]
        scores = lax.dot_general(
            keys.reshape(2 * rows, HEAD_SIZE),
            queries[unit],
            (((1,), (1,)), ((), ())),
            preferred_element_type=jnp.float32,
        )
        if masked:
            key = lax.broadcasted_iota(jnp.int32, scores.shape, 0)
            query = (
                lax.rem(lax.broadcasted_iota(jnp.int32, scores.shape, 1), rows)
                + lax.rem(place, 2) * rows
            )
            scores = jnp.where(key <= query, scores, masked_score)
        best = jnp.max(scores, axis=0, keepdims=True)
        new = best if masked else jnp.maximum(top[unit], best)
        expo = jnp.exp2((scores - new) * factor)
        summed = jnp.sum(expo, axis=0, keepdims=True)
        added = lax.dot_general(
            values.reshape(2 * rows, HEAD_SIZE),
            expo.astype(jnp.bfloat16),
            (((0,), (0,)), ((), ())),
            preferred_element_type=jnp.float32,
        )
        if masked:
            totals[unit] = added
            low[unit] = summed
        else:
            keep = jnp.exp2((top[unit] - new) * factor)
            totals[unit] = totals[unit] * keep + added
            low[unit] = low[unit] * keep + summed
        top[unit] = new

    def absorb_other(h, steps, across):
        other = lax.div(seq_at((steps, across, 0)), 2)

        @pl.when(other < chip)
        def _():
            for b in range(local):
                absorb(b, h, other, False)

    def group_near(h):
        for b, sums in enumerate(q_pieces.last(h)):
            unit = b * KEY_VALUE_HEADS + h
            scaled = (sums * scale[b * rows : (b + 1) * rows, :]).astype(jnp.bfloat16)
            for j in range(GROUP_HEADS):
                queries[unit, j * rows : (j + 1) * rows, :] = scaled[
                    :, j * HEAD_SIZE : (j + 1) * HEAD_SIZE
                ]
        for b in range(local):
            absorb(b, h, chip, True)
        each(0, 4, lambda steps: absorb_other(h, steps, jnp.where(steps == 0, 1, 0)))

    def group_beside(h):
        each(0, 2, lambda side: absorb_other(h, 1 + 2 * side, 1))

    def group_last(h):
        absorb_other(h, 2, 1)
        for b in range(local):
            unit = b * KEY_VALUE_HEADS + h
            result = totals[unit] / low[unit]
            for j in range(GROUP_HEADS):
                column = pl.multiple_of((h * GROUP_HEADS + j) * HEAD_SIZE, 128)
                out_ref[b * rows : (b + 1) * rows, pl.ds(column, HEAD_SIZE)] = jnp.transpose(
                    result[:, j * rows : (j + 1) * rows]
                ).astype(jnp.bfloat16)

    each(2, q_pieces.chunks, second_q)
    gather.forward_near()
    gather.forward_far()
    q_pieces.pass_on(2)
    gather.near_here()
    each(0, 1, group_near)
    gather.forward_beside()
    each(1, 2, group_near)
    q_pieces.pass_on(3)
    gather.beside_here()
    each(0, 2, group_beside)
    each(2, 3, group_near)
    gather.forward_last()
    each(2, 3, group_beside)
    each(3, 4, group_near)
    each(3, 4, group_beside)
    gather.last_here()
    each(0, KEY_VALUE_HEADS, group_last)
    gather.finish()
    kv_pieces.finish()
    q_pieces.finish()


def attend(mixed, squares, kv_weight, q_weight, full_width):
    count = lax.axis_size("tensoror")
    devices = lax.axis_size("seq")
    total, width = mixed.shape
    rows = total // count
    kv_cols = kv_weight.shape[1]
    q_cols = q_weight.shape[1]
    kv_wide, q_wide = 512, GROUP_HEADS * HEAD_SIZE
    kv_chunks, q_chunks = kv_cols // kv_wide, q_cols // q_wide
    local = rows // HEAD_SIZE
    vmem = pl.BlockSpec(memory_space=pltpu.VMEM)
    hbm = pl.BlockSpec(memory_space=pl.ANY)
    return pl.pallas_call(
        functools.partial(attend_kernel, width=full_width),
        in_specs=[vmem, vmem, hbm, hbm],
        out_specs=vmem,
        out_shape=jax.ShapeDtypeStruct((rows, q_cols), jnp.bfloat16),
        scratch_shapes=[
            pltpu.VMEM((kv_chunks, width, kv_wide), jnp.bfloat16),
            pltpu.VMEM((q_chunks, width, q_wide), jnp.bfloat16),
            pltpu.VMEM((count,) + squares.shape, jnp.float32),
            pltpu.VMEM(squares.shape, jnp.float32),
            pltpu.VMEM((rows, 1), jnp.float32),
            pltpu.VMEM((devices, rows, kv_cols), jnp.bfloat16),
            pltpu.VMEM((local * KEY_VALUE_HEADS, q_wide, HEAD_SIZE), jnp.bfloat16),
            pltpu.VMEM((local * KEY_VALUE_HEADS, HEAD_SIZE, q_wide), jnp.float32),
            pltpu.VMEM((local * KEY_VALUE_HEADS, 1, q_wide), jnp.float32),
            pltpu.VMEM((local * KEY_VALUE_HEADS, 1, q_wide), jnp.float32),
            pltpu.SemaphoreType.DMA((kv_chunks,)),
            pltpu.SemaphoreType.DMA((q_chunks,)),
            pltpu.SemaphoreType.DMA((count,)),
            pltpu.SemaphoreType.DMA((count,)),
        ]
        + GATHER_SEMAPHORES
        + piece_scratch(kv_chunks, rows, kv_wide)
        + piece_scratch(q_chunks, rows, q_wide),
        compiler_params=pltpu.CompilerParams(
            collective_id=2, has_side_effects=True, vmem_limit_bytes=VMEM
        ),
    )(mixed, squares, kv_weight, q_weight)


def shards(
    visual_hidden,
    projector_weight,
    text_embeddings,
    tile_counts,
    image_start,
    norm_gain,
    query_weight,
    keyvalue_weight,
):
    sequence_local, extent_rows, width = text_embeddings.shape
    sequences, slot_rows, depth = visual_hidden.shape
    mixed, squares = mix(
        image_start,
        tile_counts,
        visual_hidden.reshape(sequences * slot_rows, depth),
        projector_weight,
        text_embeddings,
        norm_gain.reshape(1, width),
    )
    context = attend(mixed, squares, keyvalue_weight, query_weight, width)
    return context.reshape(sequence_local, extent_rows, -1)


def solution(mesh):
    in_specs = (
        P("group", "seq", "tensoror"),
        P("tensoror", None),
        P(("group", "tensoror"), "seq", None),
        P(),
        P(),
        P(),
        P("tensoror", None),
        P("tensoror", None),
    )
    out_specs = P(("group", "tensoror"), "seq", None)
    return jax.shard_map(shards, mesh=mesh, in_specs=in_specs, out_specs=out_specs, check_vma=False)
```

```python
import functools
import math

import jax
import jax.numpy as jnp
from jax import lax
from jax.experimental import pallas as pl
from jax.experimental.pallas import tpu as pltpu
from jax.sharding import PartitionSpec as P

QUERY_HEADS = 20
KEY_VALUE_HEADS = 4
HEAD_SIZE = 128
TILE = 256
GROUP_HEADS = QUERY_HEADS // KEY_VALUE_HEADS
MESH = pl.DeviceIdType.MESH

epsilon = 1e-06
masked_score = -1e30
VMEM = 60 * 1024 * 1024


def neighbours():
    count = lax.axis_size("tensoror")
    me = lax.axis_index("tensoror")
    return me, lax.rem(me + 1, count), lax.rem(me + 2, count), lax.rem(me + 3, count)


def greet(peers):
    barrier = pltpu.get_barrier_semaphore()
    for peer in peers:
        pl.semaphore_signal(
            barrier, inc=1, device_id=peer, device_id_type=MESH
        )
    pl.semaphore_wait(barrier, len(peers))


TO_RIGHT = (False, True, True, False, False, True)


class Pieces:
    def __init__(self, send, recv, keep, own, send_sem, recv_sem):
        self.send, self.recv, self.keep, self.own = send, recv, keep, own
        self.send_sem, self.recv_sem = send_sem, recv_sem
        self.chunks, self.rows, self.wide = own.shape

    def copy(self, kind, c):
        me, right, opposite, left = neighbours()
        return pltpu.make_async_remote_copy(
            src_ref=self.send.at[kind, c],
            dst_ref=self.recv.at[kind, c],
            send_sem=self.send_sem.at[kind, c],
            recv_sem=self.recv_sem.at[kind, c],
            device_id={"tensoror": right if TO_RIGHT[kind] else left},
            device_id_type=MESH,
        )

    def first(self, c, part):
        me, right, opposite, left = neighbours()
        send, keep = self.send, self.keep
        half = self.rows // 2
        sums = part(2, opposite)
        send[0, c] = sums[:half].astype(jnp.bfloat16)
        send[1, c] = sums[half:].astype(jnp.bfloat16)
        self.copy(0, c).start()
        self.copy(1, c).start()
        sums = part(1, right)
        send[2, c] = sums[:half].astype(jnp.bfloat16)
        keep[1, c] = sums[half:]
        self.copy(2, c).start()
        sums = part(3, left)
        send[3, c] = sums[half:].astype(jnp.bfloat16)
        keep[0, c] = sums[:half]
        self.copy(3, c).start()
        self.own[c] = part(0, me)

    def pass_on(self, c):
        for side in (0, 1):
            self.copy(side, c).wait_recv()
            self.send[4 + side, c] = (
                self.keep[side, c] + self.recv[side, c].astype(jnp.float32)
            ).astype(jnp.bfloat16)
            self.copy(4 + side, c).start()

    def last(self, c):
        for kind in (2, 3, 4, 5):
            self.copy(kind, c).wait_recv()
        half = self.rows // 2
        own, recv = self.own, self.recv
        return [
            own[c, side * half : (side + 1) * half]
            + recv[2 + side, c].astype(jnp.float32)
            + recv[4 + side, c].astype(jnp.float32)
            for side in (0, 1)
        ]

    def finish(self):
        def wait(c):
            for kind in range(6):
                self.copy(kind, c).wait_send()

        each(0, self.chunks, wait)


def each(start, stop, body):
    lax.fori_loop(start, stop, lambda c, _: (body(c), 0)[1], 0)


def piece_scratch(chunks, rows, wide):
    return [
        pltpu.VMEM((6, chunks, rows // 2, wide), jnp.bfloat16),
        pltpu.VMEM((6, chunks, rows // 2, wide), jnp.bfloat16),
        pltpu.VMEM((2, chunks, rows // 2, wide), jnp.float32),
        pltpu.VMEM((chunks, rows, wide), jnp.float32),
        pltpu.SemaphoreType.DMA((6, chunks)),
        pltpu.SemaphoreType.DMA((6, chunks)),
    ]


OWN, NEXT, PREV, ACROSS, PARTNER = (0, 0, 0), (1, 0, 0), (3, 0, 0), (0, 1, 0), (0, 0, 1)
FAR = (2, 0, 0)
KINDS = {
    "next0": (OWN, PREV, 0),
    "next1": (OWN, PREV, 1),
    "prev1": (OWN, NEXT, 1),
    "prev0": (OWN, NEXT, 0),
    "across": (OWN, ACROSS, None),
    "partner": (OWN, PARTNER, None),
    "far0": (NEXT, PREV, 0),
    "far1": (PREV, NEXT, 1),
    "next_across": (ACROSS, PREV, None),
    "prev_across": (ACROSS, NEXT, None),
    "far_across0": (FAR, ACROSS, 0),
    "far_across1": (FAR, ACROSS, 1),
}
GOT = {
    "next0": NEXT,
    "next1": NEXT,
    "prev1": PREV,
    "prev0": PREV,
    "across": ACROSS,
    "partner": PARTNER,
    "far0": FAR,
    "far1": FAR,
    "next_across": (1, 1, 0),
    "prev_across": (3, 1, 0),
    "far_across0": (2, 1, 0),
    "far_across1": (2, 1, 0),
}
for name in list(GOT):
    if name != "partner":
        KINDS["twin_" + name] = (GOT[name], PARTNER, KINDS[name][2])
        GOT["twin_" + name] = GOT[name][:2] + (1,)
ORDER = {name: k for k, name in enumerate(KINDS)}
NEAR_TWINS = [
    "twin_" + name for name in ("next0", "next1", "prev1", "prev0", "across", "far0", "far1")
]


def seq_at(offset):
    place = lax.axis_index("seq")
    y = lax.rem(lax.div(place, 4) + offset[0], 4)
    z = lax.rem(lax.div(place, 2) + offset[1], 2)
    core = lax.rem(place + offset[2], 2)
    return y * 4 + z * 2 + core


class Gather:
    def __init__(self, blocks, send_sem, recv_sem, first=0, last=None):
        self.refs = blocks, send_sem, recv_sem
        self.first, self.size = first, (last or blocks.shape[2]) - first

    def copy(self, name, arrival):
        blocks, send_sem, recv_sem = self.refs
        block, target, half = KINDS[name]
        rows = blocks.shape[1]
        cut = pl.ds(0, rows) if half is None else pl.ds(half * (rows // 2), rows // 2)
        where = blocks.at[
            seq_at(GOT[name] if arrival else block), cut, pl.ds(self.first, self.size)
        ]
        k = ORDER[name]
        return pltpu.make_async_remote_copy(
            src_ref=where,
            dst_ref=where,
            send_sem=send_sem.at[k],
            recv_sem=recv_sem.at[k],
            device_id={"seq": seq_at(target)},
            device_id_type=MESH,
        )

    def start(self, *names):
        for name in names:
            self.copy(name, False).start()

    def arrived(self, *names):
        for name in names:
            self.copy(name, True).wait_recv()

    def start_own(self):
        self.start("next0", "prev1", "across", "next1", "prev0", "partner")

    def forward_near(self):
        self.arrived("next0")
        self.start("far0", "twin_next0")
        self.arrived("prev1")
        self.start("far1", "twin_prev1")
        self.arrived("across")
        self.start("next_across", "prev_across", "twin_across")
        self.arrived("next1")
        self.start("twin_next1")
        self.arrived("prev0")
        self.start("twin_prev0")

    def forward_far(self):
        self.arrived("far0")
        self.start("far_across0", "twin_far0")
        self.arrived("far1")
        self.start("far_across1", "twin_far1")

    def forward_beside(self):
        self.arrived("next_across")
        self.start("twin_next_across")
        self.arrived("prev_across")
        self.start("twin_prev_across")

    def forward_last(self):
        self.arrived("far_across0")
        self.start("twin_far_across0")
        self.arrived("far_across1")
        self.start("twin_far_across1")

    def near_here(self):
        self.arrived("partner", *[name for name in KINDS if name in NEAR_TWINS])

    def beside_here(self):
        self.arrived("twin_next_across", "twin_prev_across")

    def last_here(self):
        self.arrived("twin_far_across0", "twin_far_across1")

    def finish(self):
        for name in KINDS:
            self.copy(name, False).wait_send()


def seq_peers():
    return [{"seq": seq_at(offset)} for offset in (NEXT, PREV, ACROSS, PARTNER)]


GATHER_SEMAPHORES = [
    pltpu.SemaphoreType.DMA((len(KINDS),)),
    pltpu.SemaphoreType.DMA((len(KINDS),)),
]


PASSES = (0, 1, 3, 5)


def mix_kernel(
    start_ref,
    count_ref,
    hidden_ref,
    w_ref,
    text_ref,
    gain_ref,
    out_ref,
    square_ref,
    act,
    weights,
    blocks,
    text,
    weight_sem,
    text_send,
    text_recv,
    own_sem,
    gather_send,
    gather_recv,
    *scratch,
):
    me, right, opposite, left = neighbours()
    group = lax.axis_index("group")
    place = lax.axis_index("seq")
    pieces = Pieces(*scratch)
    chunks, wide = pieces.chunks, pieces.wide
    local = text_ref.shape[0]
    sequences, rows, width = text.shape
    part_rows = blocks.shape[1] // sequences
    spans = [(a * wide, b * wide) for a, b in zip(PASSES, PASSES[1:])]
    gathers = [
        Gather(blocks, gather_send.at[p], gather_recv.at[p], *span)
        for p, span in enumerate(spans)
    ]

    def load(k, dest, c):
        column = pl.multiple_of(dest * width + c * wide, 128)
        return pltpu.make_async_copy(
            w_ref.at[:, pl.ds(column, wide)], weights.at[k, c], weight_sem.at[k, c]
        )

    for c in range(chunks):
        for k, dest in ((2, opposite), (1, right), (3, left), (0, me)):
            load(k, dest, c).start()
    own_text = pltpu.make_async_copy(
        text_ref.at[:, :, pl.ds(pl.multiple_of(me * width, 128), width)],
        text.at[pl.ds(me * local, local)],
        own_sem,
    )
    own_text.start()
    greet([{"tensoror": peer} for peer in (right, opposite, left)] + seq_peers())

    def exchange(k, peer, b, p):
        first, last = spans[p]
        source = pl.ds(pl.multiple_of(peer * width + first, 128), last - first)
        return pltpu.make_async_remote_copy(
            src_ref=text_ref.at[b, :, source],
            dst_ref=text.at[me * local + b, :, pl.ds(first, last - first)],
            send_sem=text_send.at[k, b, p],
            recv_sem=text_recv.at[k, b, p],
            device_id={"tensoror": peer},
            device_id_type=MESH,
        )

    peers = ((2, opposite), (1, right), (3, left))
    for k, peer in peers:
        exchange(k, peer, 0, 0).start()
    hidden = hidden_ref[...].astype(jnp.float32)
    act[...] = (0.5 * hidden * (1.0 + lax.erf(hidden * math.sqrt(0.5)))).astype(jnp.bfloat16)

    def first(c):
        def part(k, dest):
            load(k, dest, c).wait()
            return jnp.dot(act[...], weights[k, c], preferred_element_type=jnp.float32)

        pieces.first(c, part)

    def last(c):
        column = pl.ds(pl.multiple_of(c * wide, 128), wide)
        half = pieces.rows // 2
        for side, sums in enumerate(pieces.last(c)):
            blocks[place, side * half : (side + 1) * half, column] = sums.astype(jnp.bfloat16)

    diagonal = lax.broadcasted_iota(jnp.int32, (rows, rows), 0) == lax.broadcasted_iota(
        jnp.int32, (rows, rows), 1
    )

    def mix_columns(p):
        low, high = spans[p]
        gain = gain_ref[:, pl.ds(pl.multiple_of(me * width + low, 128), high - low)]

        def one(i):
            start = start_ref[group * sequences + i]
            slots = TILE * count_ref[group * sequences + i]
            visual = blocks[
                :, pl.ds(pl.multiple_of(i * part_rows, part_rows), part_rows), low:high
            ].reshape(-1, high - low)
            total = visual.shape[0]
            shift = place * rows - start
            slot = shift + lax.broadcasted_iota(jnp.int32, (rows, total), 0)
            column = lax.broadcasted_iota(jnp.int32, (rows, total), 1)
            pick = jnp.where((slot == column) & (column < slots), 1.0, 0.0).astype(jnp.bfloat16)
            placed = jnp.dot(pick, visual, preferred_element_type=jnp.float32)
            own = shift + lax.broadcasted_iota(jnp.int32, placed.shape, 0)
            inside = (own >= 0) & (own < slots)
            mixed = jnp.where(inside, placed, text[i, :, low:high].astype(jnp.float32))
            squares = jnp.sum(mixed * mixed, axis=1, keepdims=True)
            line = jnp.sum(jnp.where(diagonal, squares, 0.0), axis=0, keepdims=True)
            if p == 0:
                square_ref[pl.ds(i, 1), :] = line
            else:
                square_ref[pl.ds(i, 1), :] += line
            out_ref[pl.ds(pl.multiple_of(i * rows, rows), rows), low:high] = (
                mixed * gain
            ).astype(jnp.bfloat16)

        each(0, sequences, one)

    def own_start(p):
        each(PASSES[p], PASSES[p + 1], last)
        gathers[p].start_own()

    def text_here(p):
        for b in range(local):
            for k, peer in peers:
                exchange(k, peer, b, p).wait()

    each(0, 1, first)
    each(1, 2, first)
    each(0, 1, pieces.pass_on)
    each(2, 3, first)
    each(1, 2, pieces.pass_on)
    own_start(0)
    each(3, 4, first)
    each(2, 3, pieces.pass_on)
    each(4, 5, first)
    each(3, 4, pieces.pass_on)
    gathers[0].forward_near()
    own_start(1)
    each(4, 5, pieces.pass_on)
    for b, p in ((1, 0), (0, 1), (1, 1), (0, 2), (1, 2)):
        for k, peer in peers:
            exchange(k, peer, b, p).start()
    gathers[0].forward_far()
    gathers[0].forward_beside()
    gathers[0].forward_last()
    gathers[1].forward_near()
    own_start(2)
    own_text.wait()
    gathers[0].near_here()
    gathers[0].beside_here()
    gathers[0].last_here()
    gathers[1].forward_far()
    text_here(0)
    mix_columns(0)
    gathers[1].forward_beside()
    gathers[1].forward_last()
    gathers[2].forward_near()
    gathers[1].near_here()
    gathers[1].beside_here()
    gathers[1].last_here()
    gathers[2].forward_far()
    text_here(1)
    mix_columns(1)
    gathers[2].forward_beside()
    gathers[2].forward_last()
    text_here(2)
    gathers[2].near_here()
    gathers[2].beside_here()
    gathers[2].last_here()
    mix_columns(2)
    for gather in gathers:
        gather.finish()
    pieces.finish()


def mix(starts, counts, hidden, weight, text, gain):
    devices = lax.axis_size("seq")
    count = lax.axis_size("tensoror")
    local, rows, full = text.shape
    width = full // count
    sequences = local * count
    wide = 256
    chunks = width // wide
    smem = pl.BlockSpec(memory_space=pltpu.SMEM)
    vmem = pl.BlockSpec(memory_space=pltpu.VMEM)
    hbm = pl.BlockSpec(memory_space=pl.ANY)
    return pl.pallas_call(
        mix_kernel,
        in_specs=[smem, smem, vmem, hbm, hbm, vmem],
        out_specs=[vmem, vmem],
        out_shape=[
            jax.ShapeDtypeStruct((sequences * rows, width), jnp.bfloat16),
            jax.ShapeDtypeStruct((sequences, rows), jnp.float32),
        ],
        scratch_shapes=[
            pltpu.VMEM(hidden.shape, jnp.bfloat16),
            pltpu.VMEM((count, chunks, width, wide), jnp.bfloat16),
            pltpu.VMEM((devices, hidden.shape[0], width), jnp.bfloat16),
            pltpu.VMEM((sequences, rows, width), jnp.bfloat16),
            pltpu.SemaphoreType.DMA((count, chunks)),
            pltpu.SemaphoreType.DMA((count, local, len(PASSES) - 1)),
            pltpu.SemaphoreType.DMA((count, local, len(PASSES) - 1)),
            pltpu.SemaphoreType.DMA,
            pltpu.SemaphoreType.DMA((len(PASSES) - 1, len(KINDS))),
            pltpu.SemaphoreType.DMA((len(PASSES) - 1, len(KINDS))),
        ]
        + piece_scratch(chunks, hidden.shape[0], wide),
        compiler_params=pltpu.CompilerParams(
            collective_id=0, has_side_effects=True, vmem_limit_bytes=VMEM
        ),
    )(starts, counts, hidden, weight, text, gain)


def attend_kernel(
    x_ref,
    square_ref,
    wkv_ref,
    wq_ref,
    out_ref,
    kv_weights,
    q_weights,
    squares,
    total_squares,
    scale,
    blocks,
    queries,
    totals,
    top,
    low,
    kv_weight_sem,
    q_weight_sem,
    square_send,
    square_recv,
    gather_send,
    gather_recv,
    *scratch,
    width,
):
    me, right, opposite, left = neighbours()
    place = lax.axis_index("seq")
    chip = lax.div(place, 2)
    kv_pieces, q_pieces = Pieces(*scratch[:6]), Pieces(*scratch[6:])
    rows = HEAD_SIZE
    local = kv_pieces.rows // rows
    factor = math.log2(math.e) / math.sqrt(HEAD_SIZE)
    gather = Gather(blocks, gather_send, gather_recv)

    def weight_copy(source, c, wide, weights, sem):
        column = pl.ds(pl.multiple_of(c * wide, 128), wide)
        return pltpu.make_async_copy(source.at[:, column], weights.at[c], sem.at[c])

    def kv_copy(c):
        return weight_copy(wkv_ref, c, kv_pieces.wide, kv_weights, kv_weight_sem)

    def q_copy(c):
        return weight_copy(wq_ref, c, q_pieces.wide, q_weights, q_weight_sem)

    for c in range(kv_pieces.chunks):
        kv_copy(c).start()
    for c in range(q_pieces.chunks):
        q_copy(c).start()
    greet([{"tensoror": peer} for peer in (right, opposite, left)] + seq_peers())

    def square_copy(k, peer):
        return pltpu.make_async_remote_copy(
            src_ref=square_ref,
            dst_ref=squares.at[k],
            send_sem=square_send.at[k],
            recv_sem=square_recv.at[k],
            device_id={"tensoror": peer},
            device_id_type=MESH,
        )

    peers = ((1, right), (2, opposite), (3, left))
    for k, peer in peers:
        square_copy(k, peer).start()

    def part_of(weights, c):
        def part(k, dest):
            span = pl.ds(pl.multiple_of(dest * local * rows, rows), local * rows)
            return jnp.dot(x_ref[span, :], weights[c], preferred_element_type=jnp.float32)

        return part

    def first_kv(c):
        kv_copy(c).wait()
        kv_pieces.first(c, part_of(kv_weights, c))

    def first_q(c):
        q_copy(c).wait()
        q_pieces.first(c, part_of(q_weights, c))

    each(0, kv_pieces.chunks, first_kv)
    for k, peer in peers:
        square_copy(k, peer).wait()
    total_squares[...] = square_ref[...] + squares[1] + squares[2] + squares[3]
    diagonal = lax.broadcasted_iota(jnp.int32, (rows, rows), 0) == lax.broadcasted_iota(
        jnp.int32, (rows, rows), 1
    )
    for b in range(local):
        row = jnp.broadcast_to(total_squares[pl.ds(me * local + b, 1), :], (rows, rows))
        column = jnp.sum(jnp.where(diagonal, row, 0.0), axis=1, keepdims=True)
        scale[b * rows : (b + 1) * rows, :] = lax.rsqrt(column / width + epsilon)
    each(0, kv_pieces.chunks, kv_pieces.pass_on)
    each(0, 2, first_q)

    def last_kv(c):
        column = pl.ds(pl.multiple_of(c * kv_pieces.wide, 128), kv_pieces.wide)
        for b, sums in enumerate(kv_pieces.last(c)):
            span = slice(b * rows, (b + 1) * rows)
            blocks[place, span, column] = (sums * scale[span, :]).astype(jnp.bfloat16)

    each(0, kv_pieces.chunks, last_kv)
    gather.start_own()

    def second_q(c):
        first_q(c)
        q_pieces.pass_on(c - 2)

    def absorb(b, h, other, masked):
        unit = b * KEY_VALUE_HEADS + h
        span = slice(b * rows, (b + 1) * rows)
        pair = pl.ds(2 * other, 2)
        key_column = pl.multiple_of(h * HEAD_SIZE, 128)
        value_column = pl.multiple_of((h + KEY_VALUE_HEADS) * HEAD_SIZE, 128)
        keys = blocks[pair, span, pl.ds(key_column, HEAD_SIZE)]
        values = blocks[pair, span, pl.ds(value_column, HEAD_SIZE)]
        scores = lax.dot_general(
            keys.reshape(2 * rows, HEAD_SIZE),
            queries[unit],
            (((1,), (1,)), ((), ())),
            preferred_element_type=jnp.float32,
        )
        if masked:
            key = lax.broadcasted_iota(jnp.int32, scores.shape, 0)
            query = (
                lax.rem(lax.broadcasted_iota(jnp.int32, scores.shape, 1), rows)
                + lax.rem(place, 2) * rows
            )
            scores = jnp.where(key <= query, scores, masked_score)
        best = jnp.max(scores, axis=0, keepdims=True)
        new = best if masked else jnp.maximum(top[unit], best)
        expo = jnp.exp2((scores - new) * factor)
        summed = jnp.sum(expo, axis=0, keepdims=True)
        added = lax.dot_general(
            values.reshape(2 * rows, HEAD_SIZE),
            expo.astype(jnp.bfloat16),
            (((0,), (0,)), ((), ())),
            preferred_element_type=jnp.float32,
        )
        if masked:
            totals[unit] = added
            low[unit] = summed
        else:
            keep = jnp.exp2((top[unit] - new) * factor)
            totals[unit] = totals[unit] * keep + added
            low[unit] = low[unit] * keep + summed
        top[unit] = new

    def absorb_other(h, steps, across):
        other = lax.div(seq_at((steps, across, 0)), 2)

        @pl.when(other < chip)
        def _():
            for b in range(local):
                absorb(b, h, other, False)

    def group_near(h):
        for b, sums in enumerate(q_pieces.last(h)):
            unit = b * KEY_VALUE_HEADS + h
            scaled = (sums * scale[b * rows : (b + 1) * rows, :]).astype(jnp.bfloat16)
            for j in range(GROUP_HEADS):
                queries[unit, j * rows : (j + 1) * rows, :] = scaled[
                    :, j * HEAD_SIZE : (j + 1) * HEAD_SIZE
                ]
        for b in range(local):
            absorb(b, h, chip, True)
        each(0, 4, lambda steps: absorb_other(h, steps, jnp.where(steps == 0, 1, 0)))

    def group_beside(h):
        each(0, 2, lambda side: absorb_other(h, 1 + 2 * side, 1))

    def group_last(h):
        absorb_other(h, 2, 1)
        for b in range(local):
            unit = b * KEY_VALUE_HEADS + h
            result = totals[unit] / low[unit]
            for j in range(GROUP_HEADS):
                column = pl.multiple_of((h * GROUP_HEADS + j) * HEAD_SIZE, 128)
                out_ref[b * rows : (b + 1) * rows, pl.ds(column, HEAD_SIZE)] = jnp.transpose(
                    result[:, j * rows : (j + 1) * rows]
                ).astype(jnp.bfloat16)

    each(0, 2, q_pieces.pass_on)
    gather.forward_near()
    each(2, 3, first_q)
    gather.forward_far()
    each(3, 4, first_q)
    q_pieces.pass_on(2)
    gather.near_here()
    each(0, 1, group_near)
    gather.forward_beside()
    each(1, 2, group_near)
    q_pieces.pass_on(3)
    gather.beside_here()
    each(0, 2, group_beside)
    each(2, 3, group_near)
    gather.forward_last()
    each(2, 3, group_beside)
    each(3, 4, group_near)
    each(3, 4, group_beside)
    gather.last_here()
    each(0, KEY_VALUE_HEADS, group_last)
    gather.finish()
    kv_pieces.finish()
    q_pieces.finish()


def attend(mixed, squares, kv_weight, q_weight, full_width):
    count = lax.axis_size("tensoror")
    devices = lax.axis_size("seq")
    total, width = mixed.shape
    rows = total // count
    kv_cols = kv_weight.shape[1]
    q_cols = q_weight.shape[1]
    kv_wide, q_wide = 512, GROUP_HEADS * HEAD_SIZE
    kv_chunks, q_chunks = kv_cols // kv_wide, q_cols // q_wide
    local = rows // HEAD_SIZE
    vmem = pl.BlockSpec(memory_space=pltpu.VMEM)
    hbm = pl.BlockSpec(memory_space=pl.ANY)
    return pl.pallas_call(
        functools.partial(attend_kernel, width=full_width),
        in_specs=[vmem, vmem, hbm, hbm],
        out_specs=vmem,
        out_shape=jax.ShapeDtypeStruct((rows, q_cols), jnp.bfloat16),
        scratch_shapes=[
            pltpu.VMEM((kv_chunks, width, kv_wide), jnp.bfloat16),
            pltpu.VMEM((q_chunks, width, q_wide), jnp.bfloat16),
            pltpu.VMEM((count,) + squares.shape, jnp.float32),
            pltpu.VMEM(squares.shape, jnp.float32),
            pltpu.VMEM((rows, 1), jnp.float32),
            pltpu.VMEM((devices, rows, kv_cols), jnp.bfloat16),
            pltpu.VMEM((local * KEY_VALUE_HEADS, q_wide, HEAD_SIZE), jnp.bfloat16),
            pltpu.VMEM((local * KEY_VALUE_HEADS, HEAD_SIZE, q_wide), jnp.float32),
            pltpu.VMEM((local * KEY_VALUE_HEADS, 1, q_wide), jnp.float32),
            pltpu.VMEM((local * KEY_VALUE_HEADS, 1, q_wide), jnp.float32),
            pltpu.SemaphoreType.DMA((kv_chunks,)),
            pltpu.SemaphoreType.DMA((q_chunks,)),
            pltpu.SemaphoreType.DMA((count,)),
            pltpu.SemaphoreType.DMA((count,)),
        ]
        + GATHER_SEMAPHORES
        + piece_scratch(kv_chunks, rows, kv_wide)
        + piece_scratch(q_chunks, rows, q_wide),
        compiler_params=pltpu.CompilerParams(
            collective_id=2, has_side_effects=True, vmem_limit_bytes=VMEM
        ),
    )(mixed, squares, kv_weight, q_weight)


def shards(
    visual_hidden,
    projector_weight,
    text_embeddings,
    tile_counts,
    image_start,
    norm_gain,
    query_weight,
    keyvalue_weight,
):
    sequence_local, extent_rows, width = text_embeddings.shape
    sequences, slot_rows, depth = visual_hidden.shape
    mixed, squares = mix(
        image_start,
        tile_counts,
        visual_hidden.reshape(sequences * slot_rows, depth),
        projector_weight,
        text_embeddings,
        norm_gain.reshape(1, width),
    )
    context = attend(mixed, squares, keyvalue_weight, query_weight, width)
    return context.reshape(sequence_local, extent_rows, -1)


def solution(mesh):
    in_specs = (
        P("group", "seq", "tensoror"),
        P("tensoror", None),
        P(("group", "tensoror"), "seq", None),
        P(),
        P(),
        P(),
        P("tensoror", None),
        P("tensoror", None),
    )
    out_specs = P(("group", "tensoror"), "seq", None)
    return jax.shard_map(shards, mesh=mesh, in_specs=in_specs, out_specs=out_specs, check_vma=False)
```

```python
import functools
import math

import jax
import jax.numpy as jnp
from jax import lax
from jax.experimental import pallas as pl
from jax.experimental.pallas import tpu as pltpu
from jax.sharding import PartitionSpec as P

QUERY_HEADS = 20
KEY_VALUE_HEADS = 4
HEAD_SIZE = 128
TILE = 256
GROUP_HEADS = QUERY_HEADS // KEY_VALUE_HEADS
MESH = pl.DeviceIdType.MESH

epsilon = 1e-06
masked_score = -1e30
VMEM = 60 * 1024 * 1024


def neighbours():
    count = lax.axis_size("tensoror")
    me = lax.axis_index("tensoror")
    return me, lax.rem(me + 1, count), lax.rem(me + 2, count), lax.rem(me + 3, count)


def greet(peers):
    barrier = pltpu.get_barrier_semaphore()
    for peer in peers:
        pl.semaphore_signal(
            barrier, inc=1, device_id=peer, device_id_type=MESH
        )
    pl.semaphore_wait(barrier, len(peers))


TO_RIGHT = (False, True, True, False, False, True)


class Pieces:
    def __init__(self, send, recv, keep, own, send_sem, recv_sem):
        self.send, self.recv, self.keep, self.own = send, recv, keep, own
        self.send_sem, self.recv_sem = send_sem, recv_sem
        self.chunks, self.rows, self.wide = own.shape

    def copy(self, kind, c):
        me, right, opposite, left = neighbours()
        return pltpu.make_async_remote_copy(
            src_ref=self.send.at[kind, c],
            dst_ref=self.recv.at[kind, c],
            send_sem=self.send_sem.at[kind, c],
            recv_sem=self.recv_sem.at[kind, c],
            device_id={"tensoror": right if TO_RIGHT[kind] else left},
            device_id_type=MESH,
        )

    def first(self, c, part):
        me, right, opposite, left = neighbours()
        send, keep = self.send, self.keep
        half = self.rows // 2
        sums = part(2, opposite)
        send[0, c] = sums[:half].astype(jnp.bfloat16)
        send[1, c] = sums[half:].astype(jnp.bfloat16)
        self.copy(0, c).start()
        self.copy(1, c).start()
        sums = part(1, right)
        send[2, c] = sums[:half].astype(jnp.bfloat16)
        keep[1, c] = sums[half:]
        self.copy(2, c).start()
        sums = part(3, left)
        send[3, c] = sums[half:].astype(jnp.bfloat16)
        keep[0, c] = sums[:half]
        self.copy(3, c).start()
        self.own[c] = part(0, me)

    def pass_on(self, c):
        for side in (0, 1):
            self.copy(side, c).wait_recv()
            self.send[4 + side, c] = (
                self.keep[side, c] + self.recv[side, c].astype(jnp.float32)
            ).astype(jnp.bfloat16)
            self.copy(4 + side, c).start()

    def last(self, c):
        for kind in (2, 3, 4, 5):
            self.copy(kind, c).wait_recv()
        half = self.rows // 2
        own, recv = self.own, self.recv
        return [
            own[c, side * half : (side + 1) * half]
            + recv[2 + side, c].astype(jnp.float32)
            + recv[4 + side, c].astype(jnp.float32)
            for side in (0, 1)
        ]

    def finish(self):
        def wait(c):
            for kind in range(6):
                self.copy(kind, c).wait_send()

        each(0, self.chunks, wait)


def each(start, stop, body):
    lax.fori_loop(start, stop, lambda c, _: (body(c), 0)[1], 0)


def piece_scratch(chunks, rows, wide):
    return [
        pltpu.VMEM((6, chunks, rows // 2, wide), jnp.bfloat16),
        pltpu.VMEM((6, chunks, rows // 2, wide), jnp.bfloat16),
        pltpu.VMEM((2, chunks, rows // 2, wide), jnp.float32),
        pltpu.VMEM((chunks, rows, wide), jnp.float32),
        pltpu.SemaphoreType.DMA((6, chunks)),
        pltpu.SemaphoreType.DMA((6, chunks)),
    ]


OWN, NEXT, PREV, ACROSS, PARTNER = (0, 0, 0), (1, 0, 0), (3, 0, 0), (0, 1, 0), (0, 0, 1)
FAR = (2, 0, 0)
KINDS = {
    "next0": (OWN, PREV, 0),
    "next1": (OWN, PREV, 1),
    "prev1": (OWN, NEXT, 1),
    "prev0": (OWN, NEXT, 0),
    "across": (OWN, ACROSS, None),
    "partner": (OWN, PARTNER, None),
    "far0": (NEXT, PREV, 0),
    "far1": (PREV, NEXT, 1),
    "next_across": (ACROSS, PREV, None),
    "prev_across": (ACROSS, NEXT, None),
    "far_across0": (FAR, ACROSS, 0),
    "far_across1": (FAR, ACROSS, 1),
}
GOT = {
    "next0": NEXT,
    "next1": NEXT,
    "prev1": PREV,
    "prev0": PREV,
    "across": ACROSS,
    "partner": PARTNER,
    "far0": FAR,
    "far1": FAR,
    "next_across": (1, 1, 0),
    "prev_across": (3, 1, 0),
    "far_across0": (2, 1, 0),
    "far_across1": (2, 1, 0),
}
for name in list(GOT):
    if name != "partner":
        KINDS["twin_" + name] = (GOT[name], PARTNER, KINDS[name][2])
        GOT["twin_" + name] = GOT[name][:2] + (1,)
ORDER = {name: k for k, name in enumerate(KINDS)}
NEAR_TWINS = [
    "twin_" + name for name in ("next0", "next1", "prev1", "prev0", "across", "far0", "far1")
]


def seq_at(offset):
    place = lax.axis_index("seq")
    y = lax.rem(lax.div(place, 4) + offset[0], 4)
    z = lax.rem(lax.div(place, 2) + offset[1], 2)
    core = lax.rem(place + offset[2], 2)
    return y * 4 + z * 2 + core


class Gather:
    def __init__(self, blocks, send_sem, recv_sem, first=0, last=None):
        self.refs = blocks, send_sem, recv_sem
        self.first, self.size = first, (last or blocks.shape[2]) - first

    def copy(self, name, arrival):
        blocks, send_sem, recv_sem = self.refs
        block, target, half = KINDS[name]
        rows = blocks.shape[1]
        cut = pl.ds(0, rows) if half is None else pl.ds(half * (rows // 2), rows // 2)
        where = blocks.at[
            seq_at(GOT[name] if arrival else block), cut, pl.ds(self.first, self.size)
        ]
        k = ORDER[name]
        return pltpu.make_async_remote_copy(
            src_ref=where,
            dst_ref=where,
            send_sem=send_sem.at[k],
            recv_sem=recv_sem.at[k],
            device_id={"seq": seq_at(target)},
            device_id_type=MESH,
        )

    def start(self, *names):
        for name in names:
            self.copy(name, False).start()

    def arrived(self, *names):
        for name in names:
            self.copy(name, True).wait_recv()

    def start_own(self):
        self.start("next0", "prev1", "across", "next1", "prev0", "partner")

    def forward_near(self):
        self.arrived("next0")
        self.start("far0", "twin_next0")
        self.arrived("prev1")
        self.start("far1", "twin_prev1")
        self.arrived("across")
        self.start("next_across", "prev_across", "twin_across")
        self.arrived("next1")
        self.start("twin_next1")
        self.arrived("prev0")
        self.start("twin_prev0")

    def forward_far(self):
        self.arrived("far0")
        self.start("far_across0", "twin_far0")
        self.arrived("far1")
        self.start("far_across1", "twin_far1")

    def forward_beside(self):
        self.arrived("next_across")
        self.start("twin_next_across")
        self.arrived("prev_across")
        self.start("twin_prev_across")

    def forward_last(self):
        self.arrived("far_across0")
        self.start("twin_far_across0")
        self.arrived("far_across1")
        self.start("twin_far_across1")

    def near_here(self):
        self.arrived("partner", *[name for name in KINDS if name in NEAR_TWINS])

    def beside_here(self):
        self.arrived("twin_next_across", "twin_prev_across")

    def last_here(self):
        self.arrived("twin_far_across0", "twin_far_across1")

    def finish(self):
        for name in KINDS:
            self.copy(name, False).wait_send()


def seq_peers():
    return [{"seq": seq_at(offset)} for offset in (NEXT, PREV, ACROSS, PARTNER)]


GATHER_SEMAPHORES = [
    pltpu.SemaphoreType.DMA((len(KINDS),)),
    pltpu.SemaphoreType.DMA((len(KINDS),)),
]


PASSES = (0, 1, 3, 5)


def mix_kernel(
    start_ref,
    count_ref,
    hidden_ref,
    w_ref,
    text_ref,
    gain_ref,
    out_ref,
    square_ref,
    act,
    weights,
    blocks,
    text,
    weight_sem,
    text_send,
    text_recv,
    own_sem,
    gather_send,
    gather_recv,
    *scratch,
):
    me, right, opposite, left = neighbours()
    group = lax.axis_index("group")
    place = lax.axis_index("seq")
    pieces = Pieces(*scratch)
    chunks, wide = pieces.chunks, pieces.wide
    local = text_ref.shape[0]
    sequences, rows, width = text.shape
    part_rows = blocks.shape[1] // sequences
    spans = [(a * wide, b * wide) for a, b in zip(PASSES, PASSES[1:])]
    gathers = [
        Gather(blocks, gather_send.at[p], gather_recv.at[p], *span)
        for p, span in enumerate(spans)
    ]

    def load(k, dest, c):
        column = pl.multiple_of(dest * width + c * wide, 128)
        return pltpu.make_async_copy(
            w_ref.at[:, pl.ds(column, wide)], weights.at[k, c], weight_sem.at[k, c]
        )

    for c in range(chunks):
        for k, dest in ((2, opposite), (1, right), (3, left), (0, me)):
            load(k, dest, c).start()
    own_text = pltpu.make_async_copy(
        text_ref.at[:, :, pl.ds(pl.multiple_of(me * width, 128), width)],
        text.at[pl.ds(me * local, local)],
        own_sem,
    )
    own_text.start()
    greet([{"tensoror": peer} for peer in (right, opposite, left)] + seq_peers())

    def exchange(k, peer, b, p):
        first, last = spans[p]
        source = pl.ds(pl.multiple_of(peer * width + first, 128), last - first)
        return pltpu.make_async_remote_copy(
            src_ref=text_ref.at[b, :, source],
            dst_ref=text.at[me * local + b, :, pl.ds(first, last - first)],
            send_sem=text_send.at[k, b, p],
            recv_sem=text_recv.at[k, b, p],
            device_id={"tensoror": peer},
            device_id_type=MESH,
        )

    peers = ((2, opposite), (1, right), (3, left))
    hidden = hidden_ref[...].astype(jnp.float32)
    act[...] = (0.5 * hidden * (1.0 + lax.erf(hidden * math.sqrt(0.5)))).astype(jnp.bfloat16)

    def first(c):
        def part(k, dest):
            load(k, dest, c).wait()
            return jnp.dot(act[...], weights[k, c], preferred_element_type=jnp.float32)

        pieces.first(c, part)

    def last(c):
        column = pl.ds(pl.multiple_of(c * wide, 128), wide)
        half = pieces.rows // 2
        for side, sums in enumerate(pieces.last(c)):
            blocks[place, side * half : (side + 1) * half, column] = sums.astype(jnp.bfloat16)

    diagonal = lax.broadcasted_iota(jnp.int32, (rows, rows), 0) == lax.broadcasted_iota(
        jnp.int32, (rows, rows), 1
    )

    def mix_columns(p):
        low, high = spans[p]
        gain = gain_ref[:, pl.ds(pl.multiple_of(me * width + low, 128), high - low)]

        def one(i):
            start = start_ref[group * sequences + i]
            slots = TILE * count_ref[group * sequences + i]
            visual = blocks[
                :, pl.ds(pl.multiple_of(i * part_rows, part_rows), part_rows), low:high
            ].reshape(-1, high - low)
            total = visual.shape[0]
            shift = place * rows - start
            slot = shift + lax.broadcasted_iota(jnp.int32, (rows, total), 0)
            column = lax.broadcasted_iota(jnp.int32, (rows, total), 1)
            pick = jnp.where((slot == column) & (column < slots), 1.0, 0.0).astype(jnp.bfloat16)
            placed = jnp.dot(pick, visual, preferred_element_type=jnp.float32)
            own = shift + lax.broadcasted_iota(jnp.int32, placed.shape, 0)
            inside = (own >= 0) & (own < slots)
            mixed = jnp.where(inside, placed, text[i, :, low:high].astype(jnp.float32))
            squares = jnp.sum(mixed * mixed, axis=1, keepdims=True)
            line = jnp.sum(jnp.where(diagonal, squares, 0.0), axis=0, keepdims=True)
            if p == 0:
                square_ref[pl.ds(i, 1), :] = line
            else:
                square_ref[pl.ds(i, 1), :] += line
            out_ref[pl.ds(pl.multiple_of(i * rows, rows), rows), low:high] = (
                mixed * gain
            ).astype(jnp.bfloat16)

        each(0, sequences, one)

    def own_start(p):
        each(PASSES[p], PASSES[p + 1], last)
        gathers[p].start_own()

    def text_here(p):
        for b in range(local):
            for k, peer in peers:
                exchange(k, peer, b, p).wait()

    each(0, 1, first)
    each(1, 2, first)
    each(0, 1, pieces.pass_on)
    each(2, 3, first)
    each(1, 2, pieces.pass_on)
    own_start(0)
    each(3, 4, first)
    each(2, 3, pieces.pass_on)
    each(4, 5, first)
    each(3, 4, pieces.pass_on)
    gathers[0].forward_near()
    own_start(1)
    each(4, 5, pieces.pass_on)
    for b, p in ((0, 0), (1, 0), (0, 1), (1, 1), (0, 2), (1, 2)):
        for k, peer in peers:
            exchange(k, peer, b, p).start()
    gathers[0].forward_far()
    gathers[0].forward_beside()
    gathers[0].forward_last()
    gathers[1].forward_near()
    own_start(2)
    own_text.wait()
    gathers[0].near_here()
    gathers[0].beside_here()
    gathers[0].last_here()
    gathers[1].forward_far()
    text_here(0)
    mix_columns(0)
    gathers[1].forward_beside()
    gathers[1].forward_last()
    gathers[2].forward_near()
    gathers[1].near_here()
    gathers[1].beside_here()
    gathers[1].last_here()
    gathers[2].forward_far()
    text_here(1)
    mix_columns(1)
    gathers[2].forward_beside()
    gathers[2].forward_last()
    text_here(2)
    gathers[2].near_here()
    gathers[2].beside_here()
    gathers[2].last_here()
    mix_columns(2)
    for gather in gathers:
        gather.finish()
    pieces.finish()


def mix(starts, counts, hidden, weight, text, gain):
    devices = lax.axis_size("seq")
    count = lax.axis_size("tensoror")
    local, rows, full = text.shape
    width = full // count
    sequences = local * count
    wide = 256
    chunks = width // wide
    smem = pl.BlockSpec(memory_space=pltpu.SMEM)
    vmem = pl.BlockSpec(memory_space=pltpu.VMEM)
    hbm = pl.BlockSpec(memory_space=pl.ANY)
    return pl.pallas_call(
        mix_kernel,
        in_specs=[smem, smem, vmem, hbm, hbm, vmem],
        out_specs=[vmem, vmem],
        out_shape=[
            jax.ShapeDtypeStruct((sequences * rows, width), jnp.bfloat16),
            jax.ShapeDtypeStruct((sequences, rows), jnp.float32),
        ],
        scratch_shapes=[
            pltpu.VMEM(hidden.shape, jnp.bfloat16),
            pltpu.VMEM((count, chunks, width, wide), jnp.bfloat16),
            pltpu.VMEM((devices, hidden.shape[0], width), jnp.bfloat16),
            pltpu.VMEM((sequences, rows, width), jnp.bfloat16),
            pltpu.SemaphoreType.DMA((count, chunks)),
            pltpu.SemaphoreType.DMA((count, local, len(PASSES) - 1)),
            pltpu.SemaphoreType.DMA((count, local, len(PASSES) - 1)),
            pltpu.SemaphoreType.DMA,
            pltpu.SemaphoreType.DMA((len(PASSES) - 1, len(KINDS))),
            pltpu.SemaphoreType.DMA((len(PASSES) - 1, len(KINDS))),
        ]
        + piece_scratch(chunks, hidden.shape[0], wide),
        compiler_params=pltpu.CompilerParams(
            collective_id=0, has_side_effects=True, vmem_limit_bytes=VMEM
        ),
    )(starts, counts, hidden, weight, text, gain)


def attend_kernel(
    x_ref,
    square_ref,
    wkv_ref,
    wq_ref,
    out_ref,
    kv_weights,
    q_weights,
    squares,
    total_squares,
    scale,
    blocks,
    queries,
    totals,
    top,
    low,
    kv_weight_sem,
    q_weight_sem,
    square_send,
    square_recv,
    gather_send,
    gather_recv,
    *scratch,
    width,
):
    me, right, opposite, left = neighbours()
    place = lax.axis_index("seq")
    chip = lax.div(place, 2)
    kv_pieces, q_pieces = Pieces(*scratch[:6]), Pieces(*scratch[6:])
    rows = HEAD_SIZE
    local = kv_pieces.rows // rows
    factor = math.log2(math.e) / math.sqrt(HEAD_SIZE)
    gather = Gather(blocks, gather_send, gather_recv)

    def weight_copy(source, c, wide, weights, sem):
        column = pl.ds(pl.multiple_of(c * wide, 128), wide)
        return pltpu.make_async_copy(source.at[:, column], weights.at[c], sem.at[c])

    def kv_copy(c):
        return weight_copy(wkv_ref, c, kv_pieces.wide, kv_weights, kv_weight_sem)

    def q_copy(c):
        return weight_copy(wq_ref, c, q_pieces.wide, q_weights, q_weight_sem)

    for c in range(kv_pieces.chunks):
        kv_copy(c).start()
    for c in range(q_pieces.chunks):
        q_copy(c).start()
    greet([{"tensoror": peer} for peer in (right, opposite, left)] + seq_peers())

    def square_copy(k, peer):
        return pltpu.make_async_remote_copy(
            src_ref=square_ref,
            dst_ref=squares.at[k],
            send_sem=square_send.at[k],
            recv_sem=square_recv.at[k],
            device_id={"tensoror": peer},
            device_id_type=MESH,
        )

    peers = ((1, right), (2, opposite), (3, left))
    for k, peer in peers:
        square_copy(k, peer).start()

    def part_of(weights, c):
        def part(k, dest):
            span = pl.ds(pl.multiple_of(dest * local * rows, rows), local * rows)
            return jnp.dot(x_ref[span, :], weights[c], preferred_element_type=jnp.float32)

        return part

    def first_kv(c):
        kv_copy(c).wait()
        kv_pieces.first(c, part_of(kv_weights, c))

    def first_q(c):
        q_copy(c).wait()
        q_pieces.first(c, part_of(q_weights, c))

    each(0, kv_pieces.chunks, first_kv)
    for k, peer in peers:
        square_copy(k, peer).wait()
    total_squares[...] = square_ref[...] + squares[1] + squares[2] + squares[3]
    diagonal = lax.broadcasted_iota(jnp.int32, (rows, rows), 0) == lax.broadcasted_iota(
        jnp.int32, (rows, rows), 1
    )
    for b in range(local):
        row = jnp.broadcast_to(total_squares[pl.ds(me * local + b, 1), :], (rows, rows))
        column = jnp.sum(jnp.where(diagonal, row, 0.0), axis=1, keepdims=True)
        scale[b * rows : (b + 1) * rows, :] = lax.rsqrt(column / width + epsilon)
    each(0, kv_pieces.chunks, kv_pieces.pass_on)
    each(0, 2, first_q)

    def last_kv(c):
        column = pl.ds(pl.multiple_of(c * kv_pieces.wide, 128), kv_pieces.wide)
        for b, sums in enumerate(kv_pieces.last(c)):
            span = slice(b * rows, (b + 1) * rows)
            blocks[place, span, column] = (sums * scale[span, :]).astype(jnp.bfloat16)

    each(0, kv_pieces.chunks, last_kv)
    gather.start_own()

    def second_q(c):
        first_q(c)
        q_pieces.pass_on(c - 2)

    def absorb(b, h, other, masked):
        unit = b * KEY_VALUE_HEADS + h
        span = slice(b * rows, (b + 1) * rows)
        pair = pl.ds(2 * other, 2)
        key_column = pl.multiple_of(h * HEAD_SIZE, 128)
        value_column = pl.multiple_of((h + KEY_VALUE_HEADS) * HEAD_SIZE, 128)
        keys = blocks[pair, span, pl.ds(key_column, HEAD_SIZE)]
        values = blocks[pair, span, pl.ds(value_column, HEAD_SIZE)]
        scores = lax.dot_general(
            keys.reshape(2 * rows, HEAD_SIZE),
            queries[unit],
            (((1,), (1,)), ((), ())),
            preferred_element_type=jnp.float32,
        )
        if masked:
            key = lax.broadcasted_iota(jnp.int32, scores.shape, 0)
            query = (
                lax.rem(lax.broadcasted_iota(jnp.int32, scores.shape, 1), rows)
                + lax.rem(place, 2) * rows
            )
            scores = jnp.where(key <= query, scores, masked_score)
        best = jnp.max(scores, axis=0, keepdims=True)
        new = best if masked else jnp.maximum(top[unit], best)
        expo = jnp.exp2((scores - new) * factor)
        summed = jnp.sum(expo, axis=0, keepdims=True)
        added = lax.dot_general(
            values.reshape(2 * rows, HEAD_SIZE),
            expo.astype(jnp.bfloat16),
            (((0,), (0,)), ((), ())),
            preferred_element_type=jnp.float32,
        )
        if masked:
            totals[unit] = added
            low[unit] = summed
        else:
            keep = jnp.exp2((top[unit] - new) * factor)
            totals[unit] = totals[unit] * keep + added
            low[unit] = low[unit] * keep + summed
        top[unit] = new

    def absorb_other(h, steps, across):
        other = lax.div(seq_at((steps, across, 0)), 2)

        @pl.when(other < chip)
        def _():
            for b in range(local):
                absorb(b, h, other, False)

    def group_near(h):
        for b, sums in enumerate(q_pieces.last(h)):
            unit = b * KEY_VALUE_HEADS + h
            scaled = (sums * scale[b * rows : (b + 1) * rows, :]).astype(jnp.bfloat16)
            for j in range(GROUP_HEADS):
                queries[unit, j * rows : (j + 1) * rows, :] = scaled[
                    :, j * HEAD_SIZE : (j + 1) * HEAD_SIZE
                ]
        for b in range(local):
            absorb(b, h, chip, True)
        each(0, 4, lambda steps: absorb_other(h, steps, jnp.where(steps == 0, 1, 0)))

    def group_beside(h):
        each(0, 2, lambda side: absorb_other(h, 1 + 2 * side, 1))

    def group_last(h):
        absorb_other(h, 2, 1)
        for b in range(local):
            unit = b * KEY_VALUE_HEADS + h
            result = totals[unit] / low[unit]
            for j in range(GROUP_HEADS):
                column = pl.multiple_of((h * GROUP_HEADS + j) * HEAD_SIZE, 128)
                out_ref[b * rows : (b + 1) * rows, pl.ds(column, HEAD_SIZE)] = jnp.transpose(
                    result[:, j * rows : (j + 1) * rows]
                ).astype(jnp.bfloat16)

    each(0, 2, q_pieces.pass_on)
    gather.forward_near()
    each(2, 3, first_q)
    gather.forward_far()
    each(3, 4, first_q)
    q_pieces.pass_on(2)
    gather.near_here()
    each(0, 1, group_near)
    gather.forward_beside()
    each(1, 2, group_near)
    q_pieces.pass_on(3)
    gather.beside_here()
    each(0, 2, group_beside)
    each(2, 3, group_near)
    gather.forward_last()
    each(2, 3, group_beside)
    each(3, 4, group_near)
    each(3, 4, group_beside)
    gather.last_here()
    each(0, KEY_VALUE_HEADS, group_last)
    gather.finish()
    kv_pieces.finish()
    q_pieces.finish()


def attend(mixed, squares, kv_weight, q_weight, full_width):
    count = lax.axis_size("tensoror")
    devices = lax.axis_size("seq")
    total, width = mixed.shape
    rows = total // count
    kv_cols = kv_weight.shape[1]
    q_cols = q_weight.shape[1]
    kv_wide, q_wide = 512, GROUP_HEADS * HEAD_SIZE
    kv_chunks, q_chunks = kv_cols // kv_wide, q_cols // q_wide
    local = rows // HEAD_SIZE
    vmem = pl.BlockSpec(memory_space=pltpu.VMEM)
    hbm = pl.BlockSpec(memory_space=pl.ANY)
    return pl.pallas_call(
        functools.partial(attend_kernel, width=full_width),
        in_specs=[vmem, vmem, hbm, hbm],
        out_specs=vmem,
        out_shape=jax.ShapeDtypeStruct((rows, q_cols), jnp.bfloat16),
        scratch_shapes=[
            pltpu.VMEM((kv_chunks, width, kv_wide), jnp.bfloat16),
            pltpu.VMEM((q_chunks, width, q_wide), jnp.bfloat16),
            pltpu.VMEM((count,) + squares.shape, jnp.float32),
            pltpu.VMEM(squares.shape, jnp.float32),
            pltpu.VMEM((rows, 1), jnp.float32),
            pltpu.VMEM((devices, rows, kv_cols), jnp.bfloat16),
            pltpu.VMEM((local * KEY_VALUE_HEADS, q_wide, HEAD_SIZE), jnp.bfloat16),
            pltpu.VMEM((local * KEY_VALUE_HEADS, HEAD_SIZE, q_wide), jnp.float32),
            pltpu.VMEM((local * KEY_VALUE_HEADS, 1, q_wide), jnp.float32),
            pltpu.VMEM((local * KEY_VALUE_HEADS, 1, q_wide), jnp.float32),
            pltpu.SemaphoreType.DMA((kv_chunks,)),
            pltpu.SemaphoreType.DMA((q_chunks,)),
            pltpu.SemaphoreType.DMA((count,)),
            pltpu.SemaphoreType.DMA((count,)),
        ]
        + GATHER_SEMAPHORES
        + piece_scratch(kv_chunks, rows, kv_wide)
        + piece_scratch(q_chunks, rows, q_wide),
        compiler_params=pltpu.CompilerParams(
            collective_id=2, has_side_effects=True, vmem_limit_bytes=VMEM
        ),
    )(mixed, squares, kv_weight, q_weight)


def shards(
    visual_hidden,
    projector_weight,
    text_embeddings,
    tile_counts,
    image_start,
    norm_gain,
    query_weight,
    keyvalue_weight,
):
    sequence_local, extent_rows, width = text_embeddings.shape
    sequences, slot_rows, depth = visual_hidden.shape
    mixed, squares = mix(
        image_start,
        tile_counts,
        visual_hidden.reshape(sequences * slot_rows, depth),
        projector_weight,
        text_embeddings,
        norm_gain.reshape(1, width),
    )
    context = attend(mixed, squares, keyvalue_weight, query_weight, width)
    return context.reshape(sequence_local, extent_rows, -1)


def solution(mesh):
    in_specs = (
        P("group", "seq", "tensoror"),
        P("tensoror", None),
        P(("group", "tensoror"), "seq", None),
        P(),
        P(),
        P(),
        P("tensoror", None),
        P("tensoror", None),
    )
    out_specs = P(("group", "tensoror"), "seq", None)
    return jax.shard_map(shards, mesh=mesh, in_specs=in_specs, out_specs=out_specs, check_vma=False)
```
